16 devices in a mesh: dp: 2 (over z), sp: 8 (over y, x, core).
Axes of the slice: x: 2, y: 2, z: 2, core: 2. Of those that a mesh axis runs over, the one named last changes fastest.
Arguments:
- hidden: bfloat16 [2, 4096, 1024], P('dp', 'sp')
- positions: int32 [2, 4096], P('dp', 'sp')
- grad_out: bfloat16 [2, 4096, 1024], P('dp', 'sp')
- gain_attn: bfloat16 [1024], P(('dp', 'sp'))
- gain_mlp: bfloat16 [1024], P(('dp', 'sp'))
- w_query: bfloat16 [1024, 2048], P(('dp', 'sp'))
- w_key: bfloat16 [1024, 1024], P(('dp', 'sp'))
- w_value: bfloat16 [1024, 1024], P(('dp', 'sp'))
- w_out: bfloat16 [2048, 1024], P(('dp', 'sp'))
- w_gate: bfloat16 [1024, 3072], P(('dp', 'sp'))
- w_up: bfloat16 [1024, 3072], P(('dp', 'sp'))
- w_down: bfloat16 [3072, 1024], P(('dp', 'sp'))
Outputs:
- output 1: bfloat16 [2, 4096, 1024], P('dp', 'sp')
- output 2: bfloat16 [2, 4096, 1024], P('dp', 'sp')
- output 3: float32 [1024], P(('dp', 'sp'))
- output 4: float32 [1024], P(('dp', 'sp'))
- output 5: float32 [1024, 2048], P(('dp', 'sp'))
- output 6: float32 [1024, 1024], P(('dp', 'sp'))
- output 7: float32 [1024, 1024], P(('dp', 'sp'))
- output 8: float32 [2048, 1024], P(('dp', 'sp'))
- output 9: float32 [1024, 3072], P(('dp', 'sp'))
- output 10: float32 [1024, 3072], P(('dp', 'sp'))
- output 11: float32 [3072, 1024], P(('dp', 'sp'))
All inputs are finite; a program needn't handle non-finite values.
Results may differ from the reference program's by a relative error of at most 0.0153369.
Values are sent between devices in bfloat16 or wider.
A program may use at most 1 GiB of HBM per device.

```python
import math
import jax
import jax.numpy as jnp
from jax import lax

BATCH = 2
SEQ = 4096
DIM = 1024
HEADS = 16
KV_HEADS = 8
FFN = 3072
HEAD_DIM = 128
ROPE_BASE = 10000.0
NORM_EPS = 1e-5
Q_PER_KV = HEADS // KV_HEADS


def setup_inputs(seed: int = 0) -> dict:
    rand_keys = jax.random.split(jax.random.key(seed), 13)
    qk_boost = (0.65 * math.log(SEQ)) ** 0.25

    def draw_normal(key_idx, arr_shape, spread):
        return (jax.random.normal(rand_keys[key_idx], arr_shape, jnp.float32) * spread).astype(jnp.bfloat16)

    def draw_gain(key_idx):
        return (1.0 + 0.3 * jax.random.normal(rand_keys[key_idx], (DIM,), jnp.float32)).astype(jnp.bfloat16)

    steps_up = jax.random.randint(rand_keys[1], (BATCH, SEQ), 1, 4)
    start_pos = jax.random.randint(rand_keys[2], (BATCH, 1), 0, SEQ)
    return {
        'hidden': draw_normal(0, (BATCH, SEQ, DIM), 1.0),
        'positions': (start_pos + jnp.cumsum(steps_up, axis=1)).astype(jnp.int32),
        'grad_out': draw_normal(3, (BATCH, SEQ, DIM), 1.0),
        'gain_attn': draw_gain(4),
        'gain_mlp': draw_gain(5),
        'w_query': draw_normal(6, (DIM, HEADS * HEAD_DIM), qk_boost / math.sqrt(DIM)),
        'w_key': draw_normal(7, (DIM, KV_HEADS * HEAD_DIM), qk_boost / math.sqrt(DIM)),
        'w_value': draw_normal(8, (DIM, KV_HEADS * HEAD_DIM), 1.0 / math.sqrt(DIM)),
        'w_out': draw_normal(9, (HEADS * HEAD_DIM, DIM), 1.0 / math.sqrt(HEADS * HEAD_DIM)),
        'w_gate': draw_normal(10, (DIM, FFN), 1.0 / math.sqrt(DIM)),
        'w_up': draw_normal(11, (DIM, FFN), 1.0 / math.sqrt(DIM)),
        'w_down': draw_normal(12, (FFN, DIM), 1.0 / math.sqrt(FFN)),
    }


def rope_tables(pos_ids):
    inv_freq = ROPE_BASE ** (-(jnp.arange(HEAD_DIM // 2, dtype=jnp.float32) * (2.0 / HEAD_DIM)))
    angles = pos_ids.astype(jnp.float32)[..., None] * inv_freq
    return jnp.cos(angles), jnp.sin(angles)


def apply_rope(values, cos_tab, sin_tab):
    half_dim = values.shape[-1] // 2
    low_half = values[..., :half_dim]
    high_half = values[..., half_dim:]
    cos_wide = cos_tab[..., None, :]
    sin_wide = sin_tab[..., None, :]
    return jnp.concatenate([low_half * cos_wide - high_half * sin_wide, high_half * cos_wide + low_half * sin_wide], axis=-1)


def rope_grad(grads_in, cos_tab, sin_tab):
    half_dim = grads_in.shape[-1] // 2
    low_half = grads_in[..., :half_dim]
    high_half = grads_in[..., half_dim:]
    cos_wide = cos_tab[..., None, :]
    sin_wide = sin_tab[..., None, :]
    return jnp.concatenate([low_half * cos_wide + high_half * sin_wide, high_half * cos_wide - low_half * sin_wide], axis=-1)


def rms_norm(values, gain_vec):
    vals32 = values.astype(jnp.float32)
    inv_rms = lax.rsqrt(jnp.mean(vals32 * vals32, axis=-1, keepdims=True) + NORM_EPS)
    normed = vals32 * inv_rms
    return (normed * gain_vec.astype(jnp.float32)).astype(jnp.bfloat16), normed, inv_rms


def rms_norm_grad(d_out, normed, inv_rms, gain_vec):
    d_normed = d_out * gain_vec.astype(jnp.float32)
    grad_gain = jnp.sum(d_out * normed, axis=0)
    grad_in = inv_rms * (d_normed - normed * jnp.mean(d_normed * normed, axis=-1, keepdims=True))
    return grad_in, grad_gain


def head_probs(q_one, k_one):
    scores = jnp.einsum('qgd,kd->gqk', q_one.astype(jnp.float32), k_one.astype(jnp.float32)) * (HEAD_DIM ** -0.5)
    causal = jnp.arange(SEQ)[:, None] >= jnp.arange(SEQ)[None, :]
    scores = jnp.where(causal, scores, -jnp.inf)
    row_max = jnp.max(scores, axis=-1, keepdims=True)
    exp_scores = jnp.exp(scores - row_max)
    return exp_scores / jnp.sum(exp_scores, axis=-1, keepdims=True)


def attention_forward(q_heads, k_heads, v_heads):
    q_major = q_heads.reshape(SEQ, KV_HEADS, Q_PER_KV, HEAD_DIM).transpose(1, 0, 2, 3)

    def one_head(operands):
        q_one, k_one, v_one = operands
        probs_bf = head_probs(q_one, k_one).astype(jnp.bfloat16)
        return jnp.einsum('gqk,kd->qgd', probs_bf.astype(jnp.float32), v_one.astype(jnp.float32))

    per_head = lax.map(one_head, (q_major, k_heads.transpose(1, 0, 2), v_heads.transpose(1, 0, 2)))
    return per_head.transpose(1, 0, 2, 3).astype(jnp.bfloat16).reshape(SEQ, HEADS * HEAD_DIM)


def attention_backward(q_heads, k_heads, v_heads, d_heads):
    q_major = q_heads.reshape(SEQ, KV_HEADS, Q_PER_KV, HEAD_DIM).transpose(1, 0, 2, 3)
    d_major = d_heads.reshape(SEQ, KV_HEADS, Q_PER_KV, HEAD_DIM).transpose(1, 0, 2, 3)

    def one_head(operands):
        q_one, k_one, v_one, d_one = operands
        attn_probs = head_probs(q_one, k_one)
        probs32 = attn_probs.astype(jnp.bfloat16).astype(jnp.float32)
        d_f32 = d_one.astype(jnp.float32)
        d_probs = jnp.einsum('qgd,kd->gqk', d_f32, v_one.astype(jnp.float32))
        grad_v = jnp.einsum('gqk,qgd->kd', probs32, d_f32)
        row_dot = jnp.sum(attn_probs * d_probs, axis=-1, keepdims=True)
        d_scores = (attn_probs * (d_probs - row_dot) * (HEAD_DIM ** -0.5)).astype(jnp.bfloat16).astype(jnp.float32)
        grad_q = jnp.einsum('gqk,kd->qgd', d_scores, k_one.astype(jnp.float32))
        grad_k = jnp.einsum('gqk,qgd->kd', d_scores, q_one.astype(jnp.float32))
        return grad_q.astype(jnp.bfloat16), grad_k.astype(jnp.bfloat16), grad_v.astype(jnp.bfloat16)

    grad_q, grad_k, grad_v = lax.map(one_head, (q_major, k_heads.transpose(1, 0, 2), v_heads.transpose(1, 0, 2), d_major))
    return grad_q.transpose(1, 0, 2, 3).reshape(SEQ, HEADS, HEAD_DIM), grad_k.transpose(1, 0, 2), grad_v.transpose(1, 0, 2)


def sequence_step(tokens, pos_ids, d_layer, gain_attn, gain_mlp, w_query, w_key, w_value, w_out, w_gate, w_up, w_down):
    cos_tab, sin_tab = rope_tables(pos_ids)
    u_attn, normed1, inv_rms1 = rms_norm(tokens, gain_attn)
    q_heads = apply_rope(jnp.dot(u_attn, w_query, preferred_element_type=jnp.float32).reshape(SEQ, HEADS, HEAD_DIM), cos_tab, sin_tab).astype(jnp.bfloat16)
    k_heads = apply_rope(jnp.dot(u_attn, w_key, preferred_element_type=jnp.float32).reshape(SEQ, KV_HEADS, HEAD_DIM), cos_tab, sin_tab).astype(jnp.bfloat16)
    v_heads = jnp.dot(u_attn, w_value, preferred_element_type=jnp.float32).astype(jnp.bfloat16).reshape(SEQ, KV_HEADS, HEAD_DIM)
    attn_out = attention_forward(q_heads, k_heads, v_heads)
    residual = (tokens.astype(jnp.float32) + jnp.dot(attn_out, w_out, preferred_element_type=jnp.float32)).astype(jnp.bfloat16)
    u_mlp, normed2, inv_rms2 = rms_norm(residual, gain_mlp)
    gate_pre = jnp.dot(u_mlp, w_gate, preferred_element_type=jnp.float32)
    up_pre = jnp.dot(u_mlp, w_up, preferred_element_type=jnp.float32)
    sig_gate = jax.nn.sigmoid(gate_pre)
    silu_gate = gate_pre * sig_gate
    mlp_act = (silu_gate * up_pre).astype(jnp.bfloat16)
    layer_out = (residual.astype(jnp.float32) + jnp.dot(mlp_act, w_down, preferred_element_type=jnp.float32)).astype(jnp.bfloat16)

    grad_w_down = jnp.dot(mlp_act.T, d_layer, preferred_element_type=jnp.float32)
    d_act = jnp.dot(d_layer, w_down.T, preferred_element_type=jnp.float32)
    d_gate = (d_act * up_pre * sig_gate * (1.0 + gate_pre * (1.0 - sig_gate))).astype(jnp.bfloat16)
    d_up = (d_act * silu_gate).astype(jnp.bfloat16)
    grad_w_gate = jnp.dot(u_mlp.T, d_gate, preferred_element_type=jnp.float32)
    grad_w_up = jnp.dot(u_mlp.T, d_up, preferred_element_type=jnp.float32)
    d_umlp = jnp.dot(d_gate, w_gate.T, preferred_element_type=jnp.float32) + jnp.dot(d_up, w_up.T, preferred_element_type=jnp.float32)
    d_res_norm, grad_gain_mlp = rms_norm_grad(d_umlp, normed2, inv_rms2, gain_mlp)
    d_resid = d_layer.astype(jnp.float32) + d_res_norm
    d_resid_bf = d_resid.astype(jnp.bfloat16)
    grad_w_out = jnp.dot(attn_out.T, d_resid_bf, preferred_element_type=jnp.float32)
    d_attn = jnp.dot(d_resid_bf, w_out.T, preferred_element_type=jnp.float32).astype(jnp.bfloat16).reshape(SEQ, HEADS, HEAD_DIM)
    grad_q, grad_k, grad_v = attention_backward(q_heads, k_heads, v_heads, d_attn)
    dq_pre = rope_grad(grad_q.astype(jnp.float32), cos_tab, sin_tab).astype(jnp.bfloat16).reshape(SEQ, HEADS * HEAD_DIM)
    dk_pre = rope_grad(grad_k.astype(jnp.float32), cos_tab, sin_tab).astype(jnp.bfloat16).reshape(SEQ, KV_HEADS * HEAD_DIM)
    dv_flat = grad_v.reshape(SEQ, KV_HEADS * HEAD_DIM)
    grad_w_query = jnp.dot(u_attn.T, dq_pre, preferred_element_type=jnp.float32)
    grad_w_key = jnp.dot(u_attn.T, dk_pre, preferred_element_type=jnp.float32)
    grad_w_value = jnp.dot(u_attn.T, dv_flat, preferred_element_type=jnp.float32)
    d_uattn = (jnp.dot(dq_pre, w_query.T, preferred_element_type=jnp.float32)
               + jnp.dot(dk_pre, w_key.T, preferred_element_type=jnp.float32)
               + jnp.dot(dv_flat, w_value.T, preferred_element_type=jnp.float32))
    d_tok_norm, grad_gain_attn = rms_norm_grad(d_uattn, normed1, inv_rms1, gain_attn)
    grad_hidden = (d_resid + d_tok_norm).astype(jnp.bfloat16)
    seq_grads = (grad_gain_attn, grad_gain_mlp, grad_w_query, grad_w_key, grad_w_value, grad_w_out, grad_w_gate, grad_w_up, grad_w_down)
    return layer_out, grad_hidden, seq_grads


def reference(hidden, positions, grad_out, gain_attn, gain_mlp, w_query, w_key, w_value, w_out, w_gate, w_up, w_down):
    weights = (gain_attn, gain_mlp, w_query, w_key, w_value, w_out, w_gate, w_up, w_down)
    zero_grads = tuple(jnp.zeros(weight.shape, jnp.float32) for weight in weights)

    def scan_body(grad_sums, seq_in):
        tokens, pos_ids, d_layer = seq_in
        layer_out, grad_hidden, seq_grads = sequence_step(tokens, pos_ids, d_layer, *weights)
        new_sums = tuple(acc_sum + seq_grad for acc_sum, seq_grad in zip(grad_sums, seq_grads))
        return new_sums, (layer_out, grad_hidden)

    grad_sums, outs_pair = lax.scan(scan_body, zero_grads, (hidden, positions, grad_out))
    return (outs_pair[0], outs_pair[1], grad_sums[0], grad_sums[1], grad_sums[2], grad_sums[3], grad_sums[4], grad_sums[5], grad_sums[6], grad_sums[7], grad_sums[8])
```

```python
import functools
import math

import jax
import jax.numpy as jnp
from jax import lax
from jax.experimental import pallas as pl
from jax.experimental.pallas import tpu as pltpu
from jax.sharding import PartitionSpec as P

HEAD_DIM = 128
ROPE_BASE = 10000.0
NORM_EPS = 1e-5
ATTN_SCALE = HEAD_DIM ** -0.5
ALL_AXES = ('dp', 'sp')


def rope_tables(pos_ids):
    inv_freq = ROPE_BASE ** (-(jnp.arange(HEAD_DIM // 2, dtype=jnp.float32) * (2.0 / HEAD_DIM)))
    angles = pos_ids.astype(jnp.float32)[..., None] * inv_freq
    return jnp.cos(angles), jnp.sin(angles)


def apply_rope(values, cos_tab, sin_tab):
    half_dim = values.shape[-1] // 2
    low_half = values[..., :half_dim]
    high_half = values[..., half_dim:]
    cos_wide = cos_tab[..., None, :]
    sin_wide = sin_tab[..., None, :]
    return jnp.concatenate([low_half * cos_wide - high_half * sin_wide, high_half * cos_wide + low_half * sin_wide], axis=-1)


def rope_grad(grads_in, cos_tab, sin_tab):
    half_dim = grads_in.shape[-1] // 2
    low_half = grads_in[..., :half_dim]
    high_half = grads_in[..., half_dim:]
    cos_wide = cos_tab[..., None, :]
    sin_wide = sin_tab[..., None, :]
    return jnp.concatenate([low_half * cos_wide + high_half * sin_wide, high_half * cos_wide - low_half * sin_wide], axis=-1)


def rms_norm(values, gain_vec):
    vals32 = values.astype(jnp.float32)
    inv_rms = lax.rsqrt(jnp.mean(vals32 * vals32, axis=-1, keepdims=True) + NORM_EPS)
    normed = vals32 * inv_rms
    return (normed * gain_vec.astype(jnp.float32)).astype(jnp.bfloat16), normed, inv_rms


def rms_norm_grad(d_out, normed, inv_rms, gain_vec):
    d_normed = d_out * gain_vec.astype(jnp.float32)
    grad_gain = jnp.sum(d_out * normed, axis=0)
    grad_in = inv_rms * (d_normed - normed * jnp.mean(d_normed * normed, axis=-1, keepdims=True))
    return grad_in, grad_gain


LOG2E = math.log2(math.e)
SCALE2 = ATTN_SCALE * LOG2E
NT = (((1,), (1,)), ((), ()))
NN = (((1,), (0,)), ((), ()))
BIG = -1e30


def fwd_kernel(bq, bk, q_ref, k_ref, vt_ref, o_ref, lse_ref):
    i = pl.program_id(0)
    heads = q_ref.shape[1] // HEAD_DIM
    qs = [q_ref[:, h * HEAD_DIM:(h + 1) * HEAD_DIM] for h in range(heads)]

    def block(j, carry, masked):
        rows = pl.ds(pl.multiple_of(j * bk, bk), bk)
        k = k_ref[rows, :]
        vt = vt_ref[:, rows]
        out = []
        for h in range(heads):
            m, l, acc = carry[h]
            s = lax.dot_general(k, qs[h], NT, preferred_element_type=jnp.float32)
            if masked:
                kpos = j * bk + lax.broadcasted_iota(jnp.int32, (bk, bq), 0)
                qpos = i * bq + lax.broadcasted_iota(jnp.int32, (bk, bq), 1)
                s = jnp.where(qpos >= kpos, s, BIG)
            m_new = jnp.maximum(m, jnp.max(s, axis=0, keepdims=True))
            p = jnp.exp2((s - m_new) * SCALE2)
            alpha = jnp.exp2((m - m_new) * SCALE2)
            l = l * alpha + jnp.sum(p, axis=0, keepdims=True)
            acc = acc * alpha + lax.dot_general(vt, p.astype(jnp.bfloat16), NN, preferred_element_type=jnp.float32)
            out.append((m_new, l, acc))
        return tuple(out)

    init = tuple((jnp.full((1, bq), BIG, jnp.float32), jnp.zeros((1, bq), jnp.float32), jnp.zeros((HEAD_DIM, bq), jnp.float32)) for _ in range(heads))
    full = i * bq // bk
    carry = lax.fori_loop(0, full, lambda j, c: block(j, c, False), init)
    for d in range(max(1, bq // bk)):
        carry = block(full + d, carry, True)
    for h in range(heads):
        m, l, acc = carry[h]
        o = acc / l
        o_ref[:, h * HEAD_DIM:(h + 1) * HEAD_DIM] = o.T.astype(jnp.bfloat16)
        lse_ref[h:h + 1, :] = m * SCALE2 + jnp.log2(l)


def flash_fwd(q, k, vt, bq=512, bk=512):
    seq, width = q.shape
    heads = width // HEAD_DIM
    return pl.pallas_call(
        functools.partial(fwd_kernel, bq, bk),
        grid=(seq // bq,),
        in_specs=[pl.BlockSpec((bq, width), lambda i: (i, 0)),
                  pl.BlockSpec((seq, HEAD_DIM), lambda i: (0, 0)),
                  pl.BlockSpec((HEAD_DIM, seq), lambda i: (0, 0))],
        out_specs=[pl.BlockSpec((bq, width), lambda i: (i, 0)),
                   pl.BlockSpec((heads, bq), lambda i: (0, i))],
        out_shape=[jax.ShapeDtypeStruct((seq, width), jnp.bfloat16), jax.ShapeDtypeStruct((heads, seq), jnp.float32)],
        cost_estimate=pl.CostEstimate(flops=2 * seq * seq * width * 2, bytes_accessed=8 << 20, transcendentals=seq * seq),
        compiler_params=pltpu.CompilerParams(vmem_limit_bytes=56 << 20),
        name="flash_fwd",
    )(q, k, vt)


def bwd_kernel(bq, bk, q_ref, d_ref, k_ref, kt_ref, v_ref, lse_ref, rd_ref, dq_ref, dk_ref, dv_ref, dqt, dka, dva):
    j = pl.program_id(0)
    nk = pl.num_programs(0)
    seq, width = q_ref.shape
    heads = width // HEAD_DIM
    nq = seq // bq
    k = k_ref[...]
    v = v_ref[...]
    kt = kt_ref[...]

    @pl.when(j == 0)
    def _():
        dqt[...] = jnp.zeros_like(dqt)

    dka[...] = jnp.zeros_like(dka)
    dva[...] = jnp.zeros_like(dva)

    def block(i, masked):
        rows = pl.ds(pl.multiple_of(i * bq, bq), bq)
        for h in range(heads):
            cols = slice(h * HEAD_DIM, (h + 1) * HEAD_DIM)
            q = q_ref[rows, cols]
            d = d_ref[rows, cols]
            s = lax.dot_general(k, q, NT, preferred_element_type=jnp.float32)
            dp = lax.dot_general(v, d, NT, preferred_element_type=jnp.float32)
            p = jnp.exp2(s * SCALE2 - lse_ref[h:h + 1, rows])
            if masked:
                kpos = j * bk + lax.broadcasted_iota(jnp.int32, (bk, bq), 0)
                qpos = i * bq + lax.broadcasted_iota(jnp.int32, (bk, bq), 1)
                p = jnp.where(qpos >= kpos, p, 0.0)
            ds = (p * (dp - rd_ref[h:h + 1, rows]) * ATTN_SCALE).astype(jnp.bfloat16)
            dva[...] += lax.dot_general(p.astype(jnp.bfloat16), d, NN, preferred_element_type=jnp.float32)
            dka[...] += lax.dot_general(ds, q, NN, preferred_element_type=jnp.float32)
            dqt[cols, rows] += lax.dot_general(kt, ds, NN, preferred_element_type=jnp.float32)

    first = j * bk // bq
    ndiag = max(1, bk // bq)
    for t in range(ndiag):
        block(first + t, True)
    lax.fori_loop(first + ndiag, nq, lambda i, c: (block(i, False), c)[1], 0)
    dk_ref[...] = dka[...].astype(jnp.bfloat16)
    dv_ref[...] = dva[...].astype(jnp.bfloat16)

    @pl.when(j == nk - 1)
    def _():
        def fin(i, c):
            rows = pl.ds(pl.multiple_of(i * bq, bq), bq)
            for h in range(heads):
                cols = slice(h * HEAD_DIM, (h + 1) * HEAD_DIM)
                dq_ref[rows, cols] = dqt[cols, rows].T.astype(jnp.bfloat16)
            return c
        lax.fori_loop(0, nq, fin, 0)


def flash_bwd(q, d, k, kt, v, lse, rd, bq=512, bk=512):
    seq, width = q.shape
    heads = width // HEAD_DIM
    whole = lambda j: (0, 0)
    return pl.pallas_call(
        functools.partial(bwd_kernel, bq, bk),
        grid=(seq // bk,),
        in_specs=[pl.BlockSpec((seq, width), whole), pl.BlockSpec((seq, width), whole),
                  pl.BlockSpec((bk, HEAD_DIM), lambda j: (j, 0)), pl.BlockSpec((HEAD_DIM, bk), lambda j: (0, j)),
                  pl.BlockSpec((bk, HEAD_DIM), lambda j: (j, 0)),
                  pl.BlockSpec((heads, seq), whole), pl.BlockSpec((heads, seq), whole)],
        out_specs=[pl.BlockSpec((seq, width), whole), pl.BlockSpec((bk, HEAD_DIM), lambda j: (j, 0)), pl.BlockSpec((bk, HEAD_DIM), lambda j: (j, 0))],
        out_shape=[jax.ShapeDtypeStruct((seq, width), jnp.bfloat16), jax.ShapeDtypeStruct((seq, HEAD_DIM), jnp.bfloat16), jax.ShapeDtypeStruct((seq, HEAD_DIM), jnp.bfloat16)],
        scratch_shapes=[pltpu.VMEM((width, seq), jnp.float32), pltpu.VMEM((bk, HEAD_DIM), jnp.float32), pltpu.VMEM((bk, HEAD_DIM), jnp.float32)],
        cost_estimate=pl.CostEstimate(flops=5 * seq * seq * width * 2 // 2, bytes_accessed=16 << 20, transcendentals=seq * seq),
        compiler_params=pltpu.CompilerParams(vmem_limit_bytes=56 << 20),
        name="flash_bwd",
    )(q, d, k, kt, v, lse, rd)


def gather_full(local_shard):
    return lax.all_gather(local_shard, ALL_AXES, axis=0, tiled=True)


def scatter_sum(partial_sum):
    return lax.psum_scatter(partial_sum, ALL_AXES, scatter_dimension=0, tiled=True)


def to_heads(tok_major):
    return lax.all_to_all(tok_major, 'sp', 1, 0, tiled=True)


def to_tokens(head_major):
    return lax.all_to_all(head_major, 'sp', 0, 1, tiled=True)


def dot_tokens(left_op, right_op):
    return lax.dot_general(left_op, right_op, (((0,), (0,)), ((), ())), preferred_element_type=jnp.float32)


def dot_back(left_op, weight):
    return lax.dot_general(left_op, weight, (((1,), (1,)), ((), ())), preferred_element_type=jnp.float32)


def layer_step(hidden, positions, grad_out, gain_attn, gain_mlp, w_query, w_key, w_value, w_out, w_gate, w_up, w_down):
    tokens = hidden[0]
    d_layer = grad_out[0]
    tok_count = tokens.shape[0]
    cos_tab, sin_tab = rope_tables(positions[0])

    gain1_full = gather_full(gain_attn)
    u_attn, normed1, inv_rms1 = rms_norm(tokens, gain1_full)
    wq_full = gather_full(w_query)
    wk_full = gather_full(w_key)
    wv_full = gather_full(w_value)
    num_heads = wq_full.shape[1] // HEAD_DIM
    kv_heads = wk_full.shape[1] // HEAD_DIM
    q_tok = apply_rope(jnp.dot(u_attn, wq_full, preferred_element_type=jnp.float32).reshape(tok_count, num_heads, HEAD_DIM), cos_tab, sin_tab).astype(jnp.bfloat16)
    k_tok = apply_rope(jnp.dot(u_attn, wk_full, preferred_element_type=jnp.float32).reshape(tok_count, kv_heads, HEAD_DIM), cos_tab, sin_tab).astype(jnp.bfloat16)
    v_tok = jnp.dot(u_attn, wv_full, preferred_element_type=jnp.float32).astype(jnp.bfloat16).reshape(tok_count, kv_heads, HEAD_DIM)
    q_heads = to_heads(q_tok)
    k_heads = to_heads(k_tok)
    v_heads = to_heads(v_tok)
    seq_len, kv_local = k_heads.shape[0], k_heads.shape[1]
    q_flat = q_heads.reshape(seq_len, -1)
    k_flat = k_heads.reshape(seq_len, HEAD_DIM)
    v_flat = v_heads.reshape(seq_len, HEAD_DIM)
    o_flat, lse = flash_fwd(q_flat, k_flat, v_flat.T, 1024, 512)
    o_heads = o_flat.reshape(seq_len, -1, HEAD_DIM)
    attn_out = to_tokens(o_heads).reshape(tok_count, num_heads * HEAD_DIM)
    wo_full = gather_full(w_out)
    residual = (tokens.astype(jnp.float32) + jnp.dot(attn_out, wo_full, preferred_element_type=jnp.float32)).astype(jnp.bfloat16)
    gain2_full = gather_full(gain_mlp)
    u_mlp, normed2, inv_rms2 = rms_norm(residual, gain2_full)
    wg_full = gather_full(w_gate)
    wu_full = gather_full(w_up)
    wd_full = gather_full(w_down)
    gate_pre = jnp.dot(u_mlp, wg_full, preferred_element_type=jnp.float32)
    up_pre = jnp.dot(u_mlp, wu_full, preferred_element_type=jnp.float32)
    sig_gate = jax.nn.sigmoid(gate_pre)
    silu_gate = gate_pre * sig_gate
    mlp_act = (silu_gate * up_pre).astype(jnp.bfloat16)
    layer_out = (residual.astype(jnp.float32) + jnp.dot(mlp_act, wd_full, preferred_element_type=jnp.float32)).astype(jnp.bfloat16)

    wd_back = gather_full(w_down)
    grad_w_down = scatter_sum(dot_tokens(mlp_act, d_layer))
    d_act = dot_back(d_layer, wd_back)
    d_gate = (d_act * up_pre * sig_gate * (1.0 + gate_pre * (1.0 - sig_gate))).astype(jnp.bfloat16)
    d_up = (d_act * silu_gate).astype(jnp.bfloat16)
    grad_w_gate = scatter_sum(dot_tokens(u_mlp, d_gate))
    grad_w_up = scatter_sum(dot_tokens(u_mlp, d_up))
    wg_back = gather_full(w_gate)
    wu_back = gather_full(w_up)
    d_umlp = dot_back(d_gate, wg_back) + dot_back(d_up, wu_back)
    gain2_back = gather_full(gain_mlp)
    d_res_norm, d_gain2 = rms_norm_grad(d_umlp, normed2, inv_rms2, gain2_back)
    grad_gain_mlp = scatter_sum(d_gain2)
    d_resid = d_layer.astype(jnp.float32) + d_res_norm
    d_resid_bf = d_resid.astype(jnp.bfloat16)
    grad_w_out = scatter_sum(dot_tokens(attn_out, d_resid_bf))
    wo_back = gather_full(w_out)
    d_attn = dot_back(d_resid_bf, wo_back).astype(jnp.bfloat16).reshape(tok_count, num_heads, HEAD_DIM)
    d_heads = to_heads(d_attn)
    d_flat = d_heads.reshape(seq_len, -1)
    row_dot = jnp.sum((o_flat.astype(jnp.float32) * d_flat.astype(jnp.float32)).reshape(seq_len, -1, HEAD_DIM), axis=-1).T
    dq_flat, dk_flat, dv_flat = flash_bwd(q_flat, d_flat, k_flat, k_flat.T, v_flat, lse, row_dot, 512, 512)
    grad_q = dq_flat.reshape(seq_len, -1, HEAD_DIM)
    grad_k = dk_flat.reshape(seq_len, kv_local, HEAD_DIM)
    grad_v = dv_flat.reshape(seq_len, kv_local, HEAD_DIM)
    dq_tok = to_tokens(grad_q)
    dk_tok = to_tokens(grad_k)
    dv_tok = to_tokens(grad_v).reshape(tok_count, kv_heads * HEAD_DIM)
    dq_pre = rope_grad(dq_tok.astype(jnp.float32), cos_tab, sin_tab).astype(jnp.bfloat16).reshape(tok_count, num_heads * HEAD_DIM)
    dk_pre = rope_grad(dk_tok.astype(jnp.float32), cos_tab, sin_tab).astype(jnp.bfloat16).reshape(tok_count, kv_heads * HEAD_DIM)
    grad_w_query = scatter_sum(dot_tokens(u_attn, dq_pre))
    grad_w_key = scatter_sum(dot_tokens(u_attn, dk_pre))
    grad_w_value = scatter_sum(dot_tokens(u_attn, dv_tok))
    wq_back = gather_full(w_query)
    wk_back = gather_full(w_key)
    wv_back = gather_full(w_value)
    d_uattn = dot_back(dq_pre, wq_back) + dot_back(dk_pre, wk_back) + dot_back(dv_tok, wv_back)
    gain1_back = gather_full(gain_attn)
    d_tok_norm, d_gain1 = rms_norm_grad(d_uattn, normed1, inv_rms1, gain1_back)
    grad_gain_attn = scatter_sum(d_gain1)
    grad_hidden = (d_resid + d_tok_norm).astype(jnp.bfloat16)
    return (layer_out[None], grad_hidden[None], grad_gain_attn, grad_gain_mlp, grad_w_query, grad_w_key, grad_w_value, grad_w_out, grad_w_gate, grad_w_up, grad_w_down)


def solution(mesh):
    act_spec = P('dp', 'sp', None)
    pos_spec = P('dp', 'sp')
    vec_spec = P(ALL_AXES)
    mat_spec = P(ALL_AXES, None)
    in_specs = (act_spec, pos_spec, act_spec, vec_spec, vec_spec) + (mat_spec,) * 7
    out_specs = (act_spec, act_spec, vec_spec, vec_spec) + (mat_spec,) * 7
    return jax.shard_map(layer_step, mesh=mesh, in_specs=in_specs, out_specs=out_specs, check_vma=False)
```

```python
import functools
import math

import jax
import jax.numpy as jnp
from jax import lax
from jax.experimental import pallas as pl
from jax.experimental.pallas import tpu as pltpu
from jax.sharding import PartitionSpec as P

HEAD_DIM = 128
ROPE_BASE = 10000.0
NORM_EPS = 1e-5
ATTN_SCALE = HEAD_DIM ** -0.5
ALL_AXES = ('dp', 'sp')


def rope_tables(pos_ids):
    inv_freq = ROPE_BASE ** (-(jnp.arange(HEAD_DIM // 2, dtype=jnp.float32) * (2.0 / HEAD_DIM)))
    angles = pos_ids.astype(jnp.float32)[..., None] * inv_freq
    return jnp.cos(angles), jnp.sin(angles)


def apply_rope(values, cos_tab, sin_tab):
    half_dim = values.shape[-1] // 2
    low_half = values[..., :half_dim]
    high_half = values[..., half_dim:]
    cos_wide = cos_tab[..., None, :]
    sin_wide = sin_tab[..., None, :]
    return jnp.concatenate([low_half * cos_wide - high_half * sin_wide, high_half * cos_wide + low_half * sin_wide], axis=-1)


def rope_grad(grads_in, cos_tab, sin_tab):
    half_dim = grads_in.shape[-1] // 2
    low_half = grads_in[..., :half_dim]
    high_half = grads_in[..., half_dim:]
    cos_wide = cos_tab[..., None, :]
    sin_wide = sin_tab[..., None, :]
    return jnp.concatenate([low_half * cos_wide + high_half * sin_wide, high_half * cos_wide - low_half * sin_wide], axis=-1)


def rms_norm(values, gain_vec):
    vals32 = values.astype(jnp.float32)
    inv_rms = lax.rsqrt(jnp.mean(vals32 * vals32, axis=-1, keepdims=True) + NORM_EPS)
    normed = vals32 * inv_rms
    return (normed * gain_vec.astype(jnp.float32)).astype(jnp.bfloat16), normed, inv_rms


def rms_norm_grad(d_out, normed, inv_rms, gain_vec):
    d_normed = d_out * gain_vec.astype(jnp.float32)
    grad_gain = jnp.sum(d_out * normed, axis=0)
    grad_in = inv_rms * (d_normed - normed * jnp.mean(d_normed * normed, axis=-1, keepdims=True))
    return grad_in, grad_gain


LOG2E = math.log2(math.e)
SCALE2 = ATTN_SCALE * LOG2E
NT = (((1,), (1,)), ((), ()))
NN = (((1,), (0,)), ((), ()))
BIG = -1e30


def fwd_kernel(bq, bk, q_ref, k_ref, vt_ref, o_ref, lse_ref):
    i = pl.program_id(0)
    heads = q_ref.shape[1] // HEAD_DIM
    qs = [q_ref[:, h * HEAD_DIM:(h + 1) * HEAD_DIM] for h in range(heads)]

    def block(j, carry, masked):
        rows = pl.ds(pl.multiple_of(j * bk, bk), bk)
        k = k_ref[rows, :]
        vt = vt_ref[:, rows]
        out = []
        for h in range(heads):
            m, l, acc = carry[h]
            s = lax.dot_general(k, qs[h], NT, preferred_element_type=jnp.float32)
            if masked:
                kpos = j * bk + lax.broadcasted_iota(jnp.int32, (bk, bq), 0)
                qpos = i * bq + lax.broadcasted_iota(jnp.int32, (bk, bq), 1)
                s = jnp.where(qpos >= kpos, s, BIG)
            m_new = jnp.maximum(m, jnp.max(s, axis=0, keepdims=True))
            p = jnp.exp2((s - m_new) * SCALE2)
            alpha = jnp.exp2((m - m_new) * SCALE2)
            l = l * alpha + jnp.sum(p, axis=0, keepdims=True)
            acc = acc * alpha + lax.dot_general(vt, p.astype(jnp.bfloat16), NN, preferred_element_type=jnp.float32)
            out.append((m_new, l, acc))
        return tuple(out)

    init = tuple((jnp.full((1, bq), BIG, jnp.float32), jnp.zeros((1, bq), jnp.float32), jnp.zeros((HEAD_DIM, bq), jnp.float32)) for _ in range(heads))
    full = i * bq // bk
    carry = lax.fori_loop(0, full, lambda j, c: block(j, c, False), init)
    for d in range(max(1, bq // bk)):
        carry = block(full + d, carry, True)
    for h in range(heads):
        m, l, acc = carry[h]
        o = acc / l
        o_ref[:, h * HEAD_DIM:(h + 1) * HEAD_DIM] = o.T.astype(jnp.bfloat16)
        lse_ref[h:h + 1, :] = m * SCALE2 + jnp.log2(l)


def flash_fwd(q, k, vt, bq=512, bk=512):
    seq, width = q.shape
    heads = width // HEAD_DIM
    return pl.pallas_call(
        functools.partial(fwd_kernel, bq, bk),
        grid=(seq // bq,),
        in_specs=[pl.BlockSpec((bq, width), lambda i: (i, 0)),
                  pl.BlockSpec((seq, HEAD_DIM), lambda i: (0, 0)),
                  pl.BlockSpec((HEAD_DIM, seq), lambda i: (0, 0))],
        out_specs=[pl.BlockSpec((bq, width), lambda i: (i, 0)),
                   pl.BlockSpec((heads, bq), lambda i: (0, i))],
        out_shape=[jax.ShapeDtypeStruct((seq, width), jnp.bfloat16), jax.ShapeDtypeStruct((heads, seq), jnp.float32)],
        cost_estimate=pl.CostEstimate(flops=2 * seq * seq * width * 2, bytes_accessed=8 << 20, transcendentals=seq * seq),
        compiler_params=pltpu.CompilerParams(vmem_limit_bytes=56 << 20),
        name="flash_fwd",
    )(q, k, vt)


def bwd_kernel(bq, bk, q_ref, o_ref, d_ref, k_ref, kt_ref, v_ref, lse_ref, out_ref, dqt, dka, dva, rd):
    j = pl.program_id(0)
    nk = pl.num_programs(0)
    seq, width = q_ref.shape
    heads = width // HEAD_DIM
    nq = seq // bq
    k = k_ref[...]
    v = v_ref[...]
    kt = kt_ref[...]

    @pl.when(j == 0)
    def _():
        dqt[...] = jnp.zeros_like(dqt)

        def prep(i, c):
            rows = pl.ds(pl.multiple_of(i * bq, bq), bq)
            for h in range(heads):
                cols = slice(h * HEAD_DIM, (h + 1) * HEAD_DIM)
                prod = o_ref[rows, cols].astype(jnp.float32) * d_ref[rows, cols].astype(jnp.float32)
                rd[h:h + 1, rows] = jnp.sum(prod.T, axis=0, keepdims=True)
            return c
        lax.fori_loop(0, nq, prep, 0)

    dka[...] = jnp.zeros_like(dka)
    dva[...] = jnp.zeros_like(dva)

    def block(i, masked):
        rows = pl.ds(pl.multiple_of(i * bq, bq), bq)
        for h in range(heads):
            cols = slice(h * HEAD_DIM, (h + 1) * HEAD_DIM)
            q = q_ref[rows, cols]
            d = d_ref[rows, cols]
            s = lax.dot_general(k, q, NT, preferred_element_type=jnp.float32)
            dp = lax.dot_general(v, d, NT, preferred_element_type=jnp.float32)
            p = jnp.exp2(s * SCALE2 - lse_ref[h:h + 1, rows])
            if masked:
                kpos = j * bk + lax.broadcasted_iota(jnp.int32, (bk, bq), 0)
                qpos = i * bq + lax.broadcasted_iota(jnp.int32, (bk, bq), 1)
                p = jnp.where(qpos >= kpos, p, 0.0)
            ds = (p * (dp - rd[h:h + 1, rows]) * ATTN_SCALE).astype(jnp.bfloat16)
            dva[...] += lax.dot_general(p.astype(jnp.bfloat16), d, NN, preferred_element_type=jnp.float32)
            dka[...] += lax.dot_general(ds, q, NN, preferred_element_type=jnp.float32)
            dqt[cols, rows] += lax.dot_general(kt, ds, NN, preferred_element_type=jnp.float32)

    first = j * bk // bq
    ndiag = max(1, bk // bq)
    for t in range(ndiag):
        block(first + t, True)
    lax.fori_loop(first + ndiag, nq, lambda i, c: (block(i, False), c)[1], 0)
    own = pl.ds(pl.multiple_of(j * bk, bk), bk)
    out_ref[own, width:width + HEAD_DIM] = dka[...].astype(jnp.bfloat16)
    out_ref[own, width + HEAD_DIM:] = dva[...].astype(jnp.bfloat16)

    @pl.when(j == nk - 1)
    def _():
        def fin(i, c):
            rows = pl.ds(pl.multiple_of(i * bq, bq), bq)
            for h in range(heads):
                cols = slice(h * HEAD_DIM, (h + 1) * HEAD_DIM)
                out_ref[rows, cols] = dqt[cols, rows].T.astype(jnp.bfloat16)
            return c
        lax.fori_loop(0, nq, fin, 0)


def flash_bwd(q, o, d, k, kt, v, lse, bq=512, bk=512):
    seq, width = q.shape
    heads = width // HEAD_DIM
    whole = lambda j: (0, 0)
    return pl.pallas_call(
        functools.partial(bwd_kernel, bq, bk),
        grid=(seq // bk,),
        in_specs=[pl.BlockSpec((seq, width), whole), pl.BlockSpec((seq, width), whole), pl.BlockSpec((seq, width), whole),
                  pl.BlockSpec((bk, HEAD_DIM), lambda j: (j, 0)), pl.BlockSpec((HEAD_DIM, bk), lambda j: (0, j)),
                  pl.BlockSpec((bk, HEAD_DIM), lambda j: (j, 0)),
                  pl.BlockSpec((heads, seq), whole)],
        out_specs=pl.BlockSpec((seq, width + 2 * HEAD_DIM), whole),
        out_shape=jax.ShapeDtypeStruct((seq, width + 2 * HEAD_DIM), jnp.bfloat16),
        scratch_shapes=[pltpu.VMEM((width, seq), jnp.float32), pltpu.VMEM((bk, HEAD_DIM), jnp.float32), pltpu.VMEM((bk, HEAD_DIM), jnp.float32),
                        pltpu.VMEM((heads, seq), jnp.float32)],
        cost_estimate=pl.CostEstimate(flops=5 * seq * seq * width * 2 // 2, bytes_accessed=16 << 20, transcendentals=seq * seq),
        compiler_params=pltpu.CompilerParams(vmem_limit_bytes=56 << 20),
        name="flash_bwd",
    )(q, o, d, k, kt, v, lse)


MESH = pl.DeviceIdType.MESH
ORDERS = ('xyz', 'yzx', 'zxy')


class Spot:
    def __init__(self):
        self.z = lax.axis_index('dp')
        self.s = lax.axis_index('sp')
        self.y = self.s // 4
        self.x = (self.s // 2) % 2
        self.c = self.s % 2
        self.bits = {'z': self.z, 'y': self.y, 'x': self.x}

    def peer(self, dim):
        if dim == 'z':
            return (1 - self.z, self.s)
        if dim == 'y':
            return (self.z, self.s + 4 - 8 * self.y)
        if dim == 'x':
            return (self.z, self.s + 2 - 4 * self.x)
        return (self.z, self.s + 1 - 2 * self.c)

    def others(self):
        return [(self.z, (self.s + t) % 8) for t in range(1, 8)]

    def region(self, freed, flipped=''):
        return tuple(slice(None) if d in freed else (1 - self.bits[d] if d in flipped else self.bits[d]) for d in 'zyx')


def greet(targets):
    bar = pltpu.get_barrier_semaphore()
    for t in targets:
        pl.semaphore_signal(bar, inc=1, device_id=t, device_id_type=MESH)
    pl.semaphore_wait(bar, len(targets))


class Wires:
    def __init__(self, send_sem, recv_sem):
        self.send_sem, self.recv_sem, self.n = send_sem, recv_sem, 0

    def copy(self, src, dst, target):
        i = self.n
        self.n += 1
        return pltpu.make_async_remote_copy(src_ref=src, dst_ref=dst, send_sem=self.send_sem.at[i], recv_sem=self.recv_sem.at[i], device_id=target, device_id_type=MESH)


class PlaneGather:
    N = 13

    def __init__(self, here, wires, src, out, local_sem):
        h = src.shape[0] // 2
        A, B = slice(0, h), slice(h, 2 * h)
        s = here.s
        sx, sy, sc = here.peer('x')[1], here.peer('y')[1], here.peer('c')[1]
        sd = here.s + 2 - 4 * here.x + 4 - 8 * here.y
        nx, ny, nc = here.peer('x'), here.peer('y'), here.peer('c')
        self.local = pltpu.make_async_copy(src, out.at[s], local_sem)
        mk = wires.copy
        self.x1 = {k: mk(src.at[r], out.at[s, r], nx) for k, r in (('A', A), ('B', B))}
        self.y1 = {k: mk(src.at[r], out.at[s, r], ny) for k, r in (('B', B), ('A', A))}
        self.c1 = mk(src, out.at[s], nc)
        self.fy = mk(out.at[sx, A], out.at[sx, A], ny)
        self.fx = mk(out.at[sy, B], out.at[sy, B], nx)
        self.cc = {}
        for name, idx in (('x', sx), ('y', sy), ('d', sd)):
            for k, r in (('A', A), ('B', B)):
                self.cc[name + k] = mk(out.at[idx, r], out.at[idx, r], nc)

    def start(self):
        self.x1['A'].start(); self.y1['B'].start(); self.x1['B'].start(); self.y1['A'].start()
        self.c1.start(); self.local.start()

    def finish(self):
        self.x1['A'].wait_recv(); self.fy.start(); self.cc['xA'].start()
        self.y1['B'].wait_recv(); self.fx.start(); self.cc['yB'].start()
        self.x1['B'].wait_recv(); self.cc['xB'].start()
        self.y1['A'].wait_recv(); self.cc['yA'].start()
        self.fy.wait_recv(); self.cc['dA'].start()
        self.fx.wait_recv(); self.cc['dB'].start()
        self.c1.wait_recv()
        for k in self.cc:
            self.cc[k].wait_recv()
        for c in (*self.x1.values(), *self.y1.values(), self.c1, self.fy, self.fx, *self.cc.values()):
            c.wait_send()
        self.local.wait()


def plane_targets(here):
    return [here.peer('x'), here.peer('y'), here.peer('c')]


def plane_gather_kernel(src, out, send_sem, recv_sem, local_sem):
    here = Spot()
    greet(plane_targets(here))
    g = PlaneGather(here, Wires(send_sem, recv_sem), src, out, local_sem)
    g.start()
    g.finish()


def plane_gather(src, cid, name):
    rows, cols = src.shape
    n = PlaneGather.N
    return pl.pallas_call(
        plane_gather_kernel,
        in_specs=[pl.BlockSpec(memory_space=pltpu.VMEM)],
        out_specs=pl.BlockSpec(memory_space=pl.ANY),
        out_shape=jax.ShapeDtypeStruct((8, rows, cols), src.dtype),
        scratch_shapes=[pltpu.SemaphoreType.DMA((n,)), pltpu.SemaphoreType.DMA((n,)), pltpu.SemaphoreType.DMA],
        compiler_params=pltpu.CompilerParams(collective_id=cid, has_side_effects=True),
        name=name,
    )(src)


def entry_kernel(x_ref, w_ref, meta_ref, pos_ref, xa, wa, ma, pa, send_sem, recv_sem, local_sem):
    here = Spot()
    z, s = here.z, here.s
    peers = here.others()
    nz = here.peer('z')
    greet(peers + [nz])
    wires = Wires(send_sem, recv_sem)
    first = []
    for t in peers:
        for src, dst in ((w_ref.at[t[1]], wa.at[z, s]), (meta_ref, ma.at[z, s]), (pos_ref, pa.at[s])):
            first.append(wires.copy(src, dst, t))
    locals_ = [pltpu.make_async_copy(w_ref.at[s], wa.at[z, s], local_sem.at[1]),
               pltpu.make_async_copy(meta_ref, ma.at[z, s], local_sem.at[2]),
               pltpu.make_async_copy(pos_ref, pa.at[s], local_sem.at[3])]
    g = PlaneGather(here, wires, x_ref, xa, local_sem.at[0])
    cross = [wires.copy(wa.at[z], wa.at[z], nz), wires.copy(ma.at[z], ma.at[z], nz)]
    for c in first:
        c.start()
    for c in locals_:
        c.start()
    g.start()
    for c in first:
        c.wait_recv()
    for c in locals_:
        c.wait()
    for c in cross:
        c.start()
    g.finish()
    for c in cross:
        c.wait()
    for c in first:
        c.wait_send()


def entry(x, w, meta, pos, cid):
    n = PlaneGather.N + 21 + 2
    vm = pl.BlockSpec(memory_space=pltpu.VMEM)
    an = pl.BlockSpec(memory_space=pl.ANY)
    return pl.pallas_call(
        entry_kernel,
        in_specs=[vm] * 4, out_specs=[an] * 4,
        out_shape=[jax.ShapeDtypeStruct((8, *x.shape), x.dtype), jax.ShapeDtypeStruct((2, 8, *w.shape[1:]), w.dtype),
                   jax.ShapeDtypeStruct((2, 8, *meta.shape), meta.dtype), jax.ShapeDtypeStruct((8, *pos.shape), pos.dtype)],
        scratch_shapes=[pltpu.SemaphoreType.DMA((n,)), pltpu.SemaphoreType.DMA((n,)), pltpu.SemaphoreType.DMA((4,))],
        compiler_params=pltpu.CompilerParams(collective_id=cid, has_side_effects=True),
        name="entry",
    )(x, w, meta, pos)


def regroup_kernel(src, out, send_sem, recv_sem, local_sem, stage):
    here = Spot()
    s = here.s
    rows, width = out.shape[0], src.shape[1]
    peers = here.others()
    greet(peers)
    wires = Wires(send_sem, recv_sem)
    piece = lambda i: pl.ds(pl.multiple_of(i * rows, rows), rows)
    mine = pl.ds(pl.multiple_of(s * width, width), width)
    cs = [wires.copy(src.at[piece(t[1])], out.at[:, mine], t) for t in peers]
    for c in cs:
        c.start()
    a = pltpu.make_async_copy(src.at[piece(s)], stage, local_sem.at[0])
    a.start(); a.wait()
    b = pltpu.make_async_copy(stage, out.at[:, mine], local_sem.at[1])
    b.start(); b.wait()
    for c in cs:
        c.wait()


def regroup(src, cid, name):
    seq, width = src.shape
    rows = seq // 8
    an = pl.BlockSpec(memory_space=pl.ANY)
    return pl.pallas_call(
        regroup_kernel, in_specs=[an], out_specs=an,
        out_shape=jax.ShapeDtypeStruct((rows, 8 * width), src.dtype),
        scratch_shapes=[pltpu.SemaphoreType.DMA((7,)), pltpu.SemaphoreType.DMA((7,)), pltpu.SemaphoreType.DMA((2,)), pltpu.VMEM((rows, width), src.dtype)],
        compiler_params=pltpu.CompilerParams(collective_id=cid, has_side_effects=True),
        name=name,
    )(src)


class CubeGather:
    def __init__(self, here, wires, jobs):
        self.steps = []
        for i in range(3):
            cs = []
            for out, suffix, order in jobs:
                reg = here.region(order[:i]) + suffix
                cs.append(wires.copy(out.at[reg], out.at[reg], here.peer(order[i])))
            self.steps.append(cs)

    def start(self, i):
        for c in self.steps[i]:
            c.start()

    def arrive(self, i):
        for c in self.steps[i]:
            c.wait_recv()

    def drain(self):
        for cs in self.steps:
            for c in cs:
                c.wait_send()


def col_chunks(cols):
    n = cols // 128
    a = -(-n // 3)
    b = -(-(n - a) // 2)
    return [(0, a * 128), (a * 128, b * 128), ((a + b) * 128, (n - a - b) * 128)]


def cube_targets(here):
    return [here.peer(d) for d in 'xyzc']


def wgather_plan(here, wires, local_sem, ins, outs):
    w1, w3, w2, wo = ins
    o1, o3, o2, oo = outs
    c = here.c
    zyx = here.region('')
    nc = here.peer('c')
    pre = [wires.copy(w1.at[1 - c], o1.at[zyx + (c,)], nc), wires.copy(w3.at[1 - c], o3.at[zyx + (c,)], nc)]
    loc = [pltpu.make_async_copy(w1.at[c], o1.at[zyx + (c,)], local_sem.at[0]),
           pltpu.make_async_copy(w3.at[c], o3.at[zyx + (c,)], local_sem.at[1]),
           pltpu.make_async_copy(w2, o2.at[zyx], local_sem.at[2]),
           pltpu.make_async_copy(wo, oo.at[zyx + (c,)], local_sem.at[3])]
    jobs = [(o1, (), ORDERS[0]), (o3, (), ORDERS[1]), (o2, (), ORDERS[2])]
    for (off, n), order in zip(col_chunks(wo.shape[1]), ORDERS):
        jobs.append((oo, (c, slice(None), slice(off, off + n)), order))
    cube = CubeGather(here, wires, jobs)
    post = [wires.copy(oo.at[:, :, :, c], oo.at[:, :, :, c], nc)]
    return pre, loc, cube, post

NW = 2 + 6 * 3 + 1

def wgather_kernel(w1, w3, w2, wo, o1, o3, o2, oo, send_sem, recv_sem, local_sem):
    here = Spot()
    greet(cube_targets(here))
    pre, loc, cube, post = wgather_plan(here, Wires(send_sem, recv_sem), local_sem, (w1, w3, w2, wo), (o1, o3, o2, oo))
    for c in pre + loc: c.start()
    for c in loc: c.wait()
    for c in pre: c.wait()
    for i in range(3):
        cube.start(i)
        cube.arrive(i)
    for c in post: c.start()
    for c in post: c.wait()
    cube.drain()

def wgather_shapes(w1, w3, w2, wo):
    return [jax.ShapeDtypeStruct((2, 2, 2, *w.shape), w.dtype) if k < 3 else jax.ShapeDtypeStruct((2, 2, 2, 2, *w.shape), w.dtype) for k, w in enumerate((w1, w3, w2, wo))]

def wgather(w1, w3, w2, wo, cid):
    vm = pl.BlockSpec(memory_space=pltpu.VMEM); an = pl.BlockSpec(memory_space=pl.ANY)
    return pl.pallas_call(
        wgather_kernel, in_specs=[vm] * 4, out_specs=[an] * 4, out_shape=wgather_shapes(w1, w3, w2, wo),
        scratch_shapes=[pltpu.SemaphoreType.DMA((NW,)), pltpu.SemaphoreType.DMA((NW,)), pltpu.SemaphoreType.DMA((4,))],
        compiler_params=pltpu.CompilerParams(collective_id=cid, has_side_effects=True), name="wgather",
    )(w1, w3, w2, wo)

def halve_kernel(nd, n, *refs):
    ins, outs = refs[:n], refs[n:2 * n]
    send_sem, recv_sem = refs[2 * n:]
    here = Spot()
    greet([here.peer(d) for d in 'xyz'])
    wires = Wires(send_sem, recv_sem)
    cs = []
    for k in range(n):
        order = ORDERS[k % 3]
        live = [d for d in 'zyx' if d in order[:nd]]
        d = order[nd - 1]
        reg = tuple(1 - here.bits[d] if e == d else slice(None) for e in live)
        cs.append(wires.copy(ins[k].at[reg], outs[k], here.peer(d)))
    for c in cs: c.start()
    for c in cs: c.wait()

def halve(arrs, nd, cid, name):
    n = len(arrs)
    outs = [jax.ShapeDtypeStruct((*((2,) * (nd - 1)), *a.shape[nd:]), a.dtype) for a in arrs]
    an = pl.BlockSpec(memory_space=pl.ANY)
    return pl.pallas_call(
        functools.partial(halve_kernel, nd, n), in_specs=[an] * n, out_specs=[an] * n, out_shape=outs,
        scratch_shapes=[pltpu.SemaphoreType.DMA((n,)), pltpu.SemaphoreType.DMA((n,))],
        compiler_params=pltpu.CompilerParams(collective_id=cid, has_side_effects=True), name=name,
    )(*arrs)


def ggather_kernel(wg, og, send_sem, recv_sem, local_sem):
    here = Spot()
    greet(cube_targets(here))
    c = here.c
    wires = Wires(send_sem, recv_sem)
    loc = pltpu.make_async_copy(wg, og.at[here.region('') + (c,)], local_sem)
    jobs = [(og, (c, slice(None), slice(off, off + n)), order) for (off, n), order in zip(col_chunks(wg.shape[1]), ORDERS)]
    cube = CubeGather(here, wires, jobs)
    post = wires.copy(og.at[:, :, :, c], og.at[:, :, :, c], here.peer('c'))
    loc.start()
    loc.wait()
    for i in range(3):
        cube.start(i)
        cube.arrive(i)
    post.start()
    post.wait()
    cube.drain()


def ggather(wg, cid):
    return pl.pallas_call(
        ggather_kernel, in_specs=[pl.BlockSpec(memory_space=pltpu.VMEM)], out_specs=pl.BlockSpec(memory_space=pl.ANY),
        out_shape=jax.ShapeDtypeStruct((2, 2, 2, 2, *wg.shape), wg.dtype),
        scratch_shapes=[pltpu.SemaphoreType.DMA((10,)), pltpu.SemaphoreType.DMA((10,)), pltpu.SemaphoreType.DMA],
        compiler_params=pltpu.CompilerParams(collective_id=cid, has_side_effects=True), name="ggather",
    )(wg)


def owner_kernel(a, b, oa, ob, send_sem, recv_sem, local_sem):
    here = Spot()
    peers = here.others()
    greet(peers)
    wires = Wires(send_sem, recv_sem)
    s = here.s
    cs = [wires.copy(r.at[t[1]], o.at[s], t) for t in peers for r, o in ((a, oa), (b, ob))]
    loc = [pltpu.make_async_copy(a.at[s], oa.at[s], local_sem.at[0]), pltpu.make_async_copy(b.at[s], ob.at[s], local_sem.at[1])]
    for c in cs + loc:
        c.start()
    for c in cs + loc:
        c.wait()


def owner(a, b, cid):
    vm = pl.BlockSpec(memory_space=pltpu.VMEM)
    return pl.pallas_call(
        owner_kernel, in_specs=[vm] * 2, out_specs=[vm] * 2,
        out_shape=[jax.ShapeDtypeStruct(t.shape, t.dtype) for t in (a, b)],
        scratch_shapes=[pltpu.SemaphoreType.DMA((14,)), pltpu.SemaphoreType.DMA((14,)), pltpu.SemaphoreType.DMA((2,))],
        compiler_params=pltpu.CompilerParams(collective_id=cid, has_side_effects=True), name="owner",
    )(a, b)


def dot_tokens(left_op, right_op):
    return lax.dot_general(left_op, right_op, (((0,), (0,)), ((), ())), preferred_element_type=jnp.float32)


def dot_back(left_op, weight):
    return lax.dot_general(left_op, weight, (((1,), (1,)), ((), ())), preferred_element_type=jnp.float32)


def dot_on(left_op, weight):
    return jnp.dot(left_op, weight, preferred_element_type=jnp.float32)


def swap_core(t):
    return lax.ppermute(t, 'sp', [(i, i ^ 1) for i in range(8)])


def swap_z(t):
    return lax.ppermute(t, 'dp', [(0, 1), (1, 0)])


def halve_sum(arrs, nd, cid, name):
    here = Spot()
    got = halve(arrs, nd, cid, name)
    out = []
    for i, (g, r) in enumerate(zip(arrs, got)):
        order = ORDERS[i % 3]
        live = [d for d in 'zyx' if d in order[:nd]]
        d = order[nd - 1]
        out.append(lax.dynamic_index_in_dim(g, here.bits[d], live.index(d), False) + r)
    return out


def split_cols(w):
    rows, cols = w.shape
    return w.reshape(rows, 8, 2, cols // 16).transpose(2, 0, 1, 3).reshape(2, rows, cols // 2)


def join_cols(mine, other, c):
    rows, half = mine.shape
    m, o = mine.reshape(rows, 8, 1, half // 8), other.reshape(rows, 8, 1, half // 8)
    first = jnp.where(c == 0, m, o)
    second = jnp.where(c == 0, o, m)
    return jnp.concatenate([first, second], axis=2).reshape(rows, 2 * half)


def layer_step(hidden, positions, grad_out, gain_attn, gain_mlp, w_query, w_key, w_value, w_out, w_gate, w_up, w_down):
    tokens = hidden[0]
    d_layer = grad_out[0]
    tok, dim = tokens.shape
    here = Spot()
    z, s, c = here.z, here.s, here.c
    rows = w_query.shape[0]
    grp_q = w_query.shape[1] // 8
    grp_k = w_key.shape[1] // 8
    grp = grp_q + 2 * grp_k
    seq = 8 * tok

    w_grp = jnp.concatenate([w_query.reshape(rows, 8, grp_q), w_key.reshape(rows, 8, grp_k), w_value.reshape(rows, 8, grp_k)], axis=2)
    w_flat = w_grp.reshape(rows, 8 * grp)
    pad = HEAD_DIM - gain_attn.shape[0]
    meta = jnp.pad(jnp.stack([jnp.pad(gain_attn, (0, pad)), jnp.pad(gain_mlp, (0, pad))]), ((0, 14), (0, 0)))
    x_all, w_own, meta_all, pos_all = entry(tokens, w_grp.transpose(1, 0, 2), meta, positions[0].reshape(-1, 128), 1)
    x_all = x_all.reshape(seq, dim)
    w_own = w_own.reshape(dim, grp)
    gain1 = meta_all[:, :, 0, :rows].reshape(dim)
    gain2 = meta_all[:, :, 1, :rows].reshape(dim)
    cos_tab, sin_tab = rope_tables(pos_all.reshape(seq))

    u_all = rms_norm(x_all, gain1)[0]
    qkv = dot_on(u_all, w_own)
    heads = (grp_q + grp_k) // HEAD_DIM
    qk = apply_rope(qkv[:, :grp_q + grp_k].reshape(seq, heads, HEAD_DIM), cos_tab, sin_tab).astype(jnp.bfloat16).reshape(seq, grp_q + grp_k)
    q_own, k_own = qk[:, :grp_q], qk[:, grp_q:]
    v_own = qkv[:, grp_q + grp_k:].astype(jnp.bfloat16)
    k_t, v_t = k_own.T, v_own.T
    o_own, lse = flash_fwd(q_own, k_own, v_t, 1024, 512)

    w1, w3, w2, wo = wgather(split_cols(w_gate), split_cols(w_up), w_down, w_out, 2)
    ffn_half = w1.shape[-1]
    w1, w3 = w1.reshape(dim, ffn_half), w3.reshape(dim, ffn_half)
    w2 = w2.reshape(ffn_half, dim)
    wo = wo.reshape(-1, dim)
    attn_out = regroup(o_own, 3, 'regroup_o')
    residual = (tokens.astype(jnp.float32) + dot_on(attn_out, wo)).astype(jnp.bfloat16)
    u_mlp, normed2, inv_rms2 = rms_norm(residual, gain2)
    u_pair = jnp.concatenate([u_mlp, swap_core(u_mlp)], axis=0)
    d_pair = jnp.concatenate([d_layer, swap_core(d_layer)], axis=0)
    gate_pre = dot_on(u_pair, w1)
    up_pre = dot_on(u_pair, w3)
    sig_gate = jax.nn.sigmoid(gate_pre)
    silu_gate = gate_pre * sig_gate
    mlp_act = (silu_gate * up_pre).astype(jnp.bfloat16)
    y_part = dot_on(mlp_act, w2)
    layer_out = (residual.astype(jnp.float32) + (y_part[:tok] + swap_core(y_part[tok:]))).astype(jnp.bfloat16)

    d_act = dot_back(d_pair, w2)
    d_gate = (d_act * up_pre * sig_gate * (1.0 + gate_pre * (1.0 - sig_gate))).astype(jnp.bfloat16)
    d_up = (d_act * silu_gate).astype(jnp.bfloat16)
    d_part = dot_back(d_gate, w1) + dot_back(d_up, w3)
    d_umlp = d_part[:tok] + swap_core(d_part[tok:])
    d_res_norm, d_gain2 = rms_norm_grad(d_umlp, normed2, inv_rms2, gain2)
    d_resid = d_layer.astype(jnp.float32) + d_res_norm
    d_resid_bf = d_resid.astype(jnp.bfloat16)
    g1 = dot_tokens(u_pair, d_gate).reshape(2, 2, 2, dim // 8, ffn_half)
    g3 = dot_tokens(u_pair, d_up).reshape(2, 2, 2, dim // 8, ffn_half)
    g2 = dot_tokens(mlp_act, d_pair).reshape(2, 2, 2, ffn_half // 8, dim)

    dh_all = plane_gather(d_resid_bf, 4, 'gather_dh').reshape(seq, dim)
    wo_own = lax.dynamic_slice_in_dim(wo, s * grp_q, grp_q, 0)
    d_own = dot_back(dh_all, wo_own).astype(jnp.bfloat16)
    go = dot_tokens(o_own, dh_all).reshape(2, grp_q // 2, dim)
    g_mlp = halve_sum([g1, g3, g2], 3, 6, 'halve3')
    dqkv = flash_bwd(q_own, o_own, d_own, k_own, k_t, v_own, lse, 512, 512)
    back = rope_grad(dqkv[:, :grp_q + grp_k].astype(jnp.float32).reshape(seq, heads, HEAD_DIM), cos_tab, sin_tab).astype(jnp.bfloat16)
    dqkv_pre = jnp.concatenate([back.reshape(seq, grp_q + grp_k), dqkv[:, grp_q + grp_k:]], axis=1)

    go_mine = lax.dynamic_index_in_dim(go, z, 0, False) + swap_z(lax.dynamic_index_in_dim(go, 1 - z, 0, False))
    grad_w_out = lax.ppermute(go_mine, ALL_AXES, [(zz * 8 + ss, 2 * ss + zz) for zz in range(2) for ss in range(8)])
    dqkv_tok = regroup(dqkv_pre, 5, 'regroup_dqkv')
    g_mlp = halve_sum(g_mlp, 2, 7, 'halve2')
    gq = dot_tokens(u_all, dqkv_pre).reshape(2, dim // 2, grp)
    gq_mine = lax.dynamic_index_in_dim(gq, z, 0, False) + swap_z(lax.dynamic_index_in_dim(gq, 1 - z, 0, False))
    wg = ggather(w_flat, 9).reshape(dim, 8 * grp)
    d_uattn = dot_back(dqkv_tok, wg)
    _, normed1, inv_rms1 = rms_norm(tokens, gain1)
    d_tok_norm, d_gain1 = rms_norm_grad(d_uattn, normed1, inv_rms1, gain1)
    grad_hidden = (d_resid + d_tok_norm).astype(jnp.bfloat16)

    gains = jnp.concatenate([d_gain1.reshape(2, 8, rows), d_gain2.reshape(2, 8, rows)], axis=2)
    gains_mine = lax.dynamic_index_in_dim(gains, z, 0, False) + swap_z(lax.dynamic_index_in_dim(gains, 1 - z, 0, False))
    gains_mine = jnp.broadcast_to(gains_mine[:, None, :], (8, 8, 2 * rows))
    got_q, got_g = owner(gq_mine.reshape(8, rows, grp), gains_mine, 10)
    got_q = got_q.transpose(1, 0, 2)
    grad_w_query = got_q[:, :, :grp_q].reshape(rows, 8 * grp_q)
    grad_w_key = got_q[:, :, grp_q:grp_q + grp_k].reshape(rows, 8 * grp_k)
    grad_w_value = got_q[:, :, grp_q + grp_k:].reshape(rows, 8 * grp_k)
    grad_gains = jnp.sum(got_g[:, 0, :], axis=0)
    grad_gain_attn, grad_gain_mlp = grad_gains[:rows], grad_gains[rows:]

    m1, m3, grad_w_down = halve_sum(g_mlp, 1, 8, 'halve1')
    pair = jnp.stack([m1.reshape(2, rows, ffn_half), m3.reshape(2, rows, ffn_half)], axis=1)
    keep = lax.dynamic_index_in_dim(pair, c, 0, False)
    other = swap_core(lax.dynamic_index_in_dim(pair, 1 - c, 0, False))
    grad_w_gate = join_cols(keep[0], other[0], c)
    grad_w_up = join_cols(keep[1], other[1], c)
    return (layer_out[None], grad_hidden[None], grad_gain_attn, grad_gain_mlp, grad_w_query, grad_w_key, grad_w_value, grad_w_out, grad_w_gate, grad_w_up, grad_w_down)


def solution(mesh):
    act_spec = P('dp', 'sp', None)
    pos_spec = P('dp', 'sp')
    vec_spec = P(ALL_AXES)
    mat_spec = P(ALL_AXES, None)
    in_specs = (act_spec, pos_spec, act_spec, vec_spec, vec_spec) + (mat_spec,) * 7
    out_specs = (act_spec, act_spec, vec_spec, vec_spec) + (mat_spec,) * 7
    return jax.shard_map(layer_step, mesh=mesh, in_specs=in_specs, out_specs=out_specs, check_vma=False)
```

```python
import functools
import math

import jax
import jax.numpy as jnp
from jax import lax
from jax.experimental import pallas as pl
from jax.experimental.pallas import tpu as pltpu
from jax.sharding import PartitionSpec as P

HEAD_DIM = 128
ROPE_BASE = 10000.0
NORM_EPS = 1e-5
ATTN_SCALE = HEAD_DIM ** -0.5
ALL_AXES = ('dp', 'sp')


def rope_tables(pos_ids):
    inv_freq = ROPE_BASE ** (-(jnp.arange(HEAD_DIM // 2, dtype=jnp.float32) * (2.0 / HEAD_DIM)))
    angles = pos_ids.astype(jnp.float32)[..., None] * inv_freq
    return jnp.cos(angles), jnp.sin(angles)


def rms_norm(values, gain_vec):
    vals32 = values.astype(jnp.float32)
    inv_rms = lax.rsqrt(jnp.mean(vals32 * vals32, axis=-1, keepdims=True) + NORM_EPS)
    normed = vals32 * inv_rms
    return (normed * gain_vec.astype(jnp.float32)).astype(jnp.bfloat16), normed, inv_rms


def rms_norm_grad(d_out, normed, inv_rms, gain_vec):
    d_normed = d_out * gain_vec.astype(jnp.float32)
    grad_gain = jnp.sum(d_out * normed, axis=0)
    grad_in = inv_rms * (d_normed - normed * jnp.mean(d_normed * normed, axis=-1, keepdims=True))
    return grad_in, grad_gain


MESH = pl.DeviceIdType.MESH
ORDERS = ('xyz', 'yzx', 'zxy')


class Spot:
    def __init__(self):
        self.z = lax.axis_index('dp')
        self.s = lax.axis_index('sp')
        self.y = self.s // 4
        self.x = (self.s // 2) % 2
        self.c = self.s % 2
        self.bits = {'z': self.z, 'y': self.y, 'x': self.x}

    def peer(self, dim):
        if dim == 'z':
            return (1 - self.z, self.s)
        if dim == 'y':
            return (self.z, self.s + 4 - 8 * self.y)
        if dim == 'x':
            return (self.z, self.s + 2 - 4 * self.x)
        return (self.z, self.s + 1 - 2 * self.c)

    def others(self):
        return [(self.z, (self.s + t) % 8) for t in range(1, 8)]

    def region(self, freed, flipped=''):
        return tuple(slice(None) if d in freed else (1 - self.bits[d] if d in flipped else self.bits[d]) for d in 'zyx')


def greet(targets):
    bar = pltpu.get_barrier_semaphore()
    for t in targets:
        pl.semaphore_signal(bar, inc=1, device_id=t, device_id_type=MESH)
    pl.semaphore_wait(bar, len(targets))


class Wires:
    def __init__(self, send_sem, recv_sem):
        self.send_sem, self.recv_sem, self.n = send_sem, recv_sem, 0

    def copy(self, src, dst, target):
        i = self.n
        self.n += 1
        return pltpu.make_async_remote_copy(src_ref=src, dst_ref=dst, send_sem=self.send_sem.at[i], recv_sem=self.recv_sem.at[i], device_id=target, device_id_type=MESH)


class CubeGather:
    def __init__(self, here, wires, jobs):
        self.stages = [[], [], []]
        self.need = [[], []]
        self.rest = []
        for out, suffix, (a, b, e) in jobs:
            def mk(freed, flipped, d):
                reg = here.region(freed, flipped) + suffix
                return wires.copy(out.at[reg], out.at[reg], here.peer(d))
            first = [mk('', '', d) for d in (a, b, e)]
            second = [mk('', a, d) for d in (b, e)]
            third = [mk(a, b, e)]
            self.stages[0] += first
            self.stages[1] += second
            self.stages[2] += third
            self.need[0].append(first[0])
            self.need[1] += [first[1], second[0]]
            self.rest += [first[2], second[1]] + third

    def start(self, i):
        for c in self.need[i - 1] if i else ():
            c.wait_recv()
        for c in self.stages[i]:
            c.start()

    def arrive(self):
        for c in self.rest:
            c.wait_recv()

    def drain(self):
        for st in self.stages:
            for c in st:
                c.wait_send()


def col_chunks(cols, parts):
    n, out, off = cols // 128, [], 0
    for p in range(parts, 0, -1):
        w = -(-n // p)
        out.append((off, w * 128))
        off += w * 128
        n -= w
    return out


def cube_targets(here):
    return [here.peer(d) for d in 'xyzc']


def comm_params(cid, **kw):
    return pltpu.CompilerParams(collective_id=cid, has_side_effects=True, **kw)


def busy(us):
    return pl.CostEstimate(flops=int(us * 1e8), bytes_accessed=1 << 20, transcendentals=0)


NW = 2 + 6 * 6 + 1


class WeightGather:
    def __init__(self, here, wires, local_sem, ins, outs):
        w1, w3, w2, wo = ins
        o1, o3, o2, oo = outs
        c, zyx, nc = here.c, here.region(''), here.peer('c')
        self.pre = [wires.copy(w1.at[1 - c], o1.at[zyx + (c,)], nc), wires.copy(w3.at[1 - c], o3.at[zyx + (c,)], nc)]
        self.loc = [pltpu.make_async_copy(w1.at[c], o1.at[zyx + (c,)], local_sem.at[0]),
                    pltpu.make_async_copy(w3.at[c], o3.at[zyx + (c,)], local_sem.at[1]),
                    pltpu.make_async_copy(w2, o2.at[zyx], local_sem.at[2]),
                    pltpu.make_async_copy(wo, oo.at[zyx + (c,)], local_sem.at[3])]
        jobs = [(o1, (), ORDERS[0]), (o3, (), ORDERS[1]), (o2, (), ORDERS[2])]
        for (off, n), order in zip(col_chunks(wo.shape[1], 3), ORDERS):
            jobs.append((oo, (c, slice(None), slice(off, off + n)), order))
        self.cube = CubeGather(here, wires, jobs)
        self.post = wires.copy(oo.at[:, :, :, c], oo.at[:, :, :, c], nc)

    def begin(self):
        for c in self.pre + self.loc:
            c.start()
        for c in self.loc:
            c.wait()
        for c in self.pre:
            c.wait()
        self.cube.start(0)

    def end(self):
        self.cube.arrive()
        self.post.start()
        self.post.wait()
        self.cube.drain()


def gathered(ws):
    return [jax.ShapeDtypeStruct((2, 2, 2, *w.shape), w.dtype) if k < 3 else jax.ShapeDtypeStruct((2, 2, 2, 2, *w.shape), w.dtype) for k, w in enumerate(ws)]


def halve_copies(here, wires, nd, ins, outs):
    cs = []
    for i, (a, o) in enumerate(zip(ins, outs)):
        order = ORDERS[i % 3]
        d = order[nd - 1]
        reg = tuple(1 - here.bits[d] if e == d else slice(None) for e in 'zyx' if e in order[:nd])
        cs.append(wires.copy(a.at[reg], o, here.peer(d)))
    return cs


def halve_shapes(arrs, nd):
    return [jax.ShapeDtypeStruct((*((2,) * (nd - 1)), *a.shape[nd:]), a.dtype) for a in arrs]


def halve_add(arrs, got, nd):
    here = Spot()
    out = []
    for i, (g, r) in enumerate(zip(arrs, got)):
        order = ORDERS[i % 3]
        live = [d for d in 'zyx' if d in order[:nd]]
        d = order[nd - 1]
        out.append(lax.dynamic_index_in_dim(g, here.bits[d], live.index(d), False) + r)
    return out


def proj_kernel(nrot, x_ref, g_ref, w_ref, cos_ref, sin_ref, u_ref, q_ref, k_ref, v_ref, kt_ref, vt_ref):
    x = x_ref[...].astype(jnp.float32)
    inv = lax.rsqrt(jnp.mean(x * x, axis=-1, keepdims=True) + NORM_EPS)
    u = (x * inv * g_ref[0:1, :].astype(jnp.float32)).astype(jnp.bfloat16)
    u_ref[...] = u
    cos, sin = cos_ref[...], sin_ref[...]
    for h in range(nrot + 2):
        t = jnp.dot(u, w_ref[:, h * HEAD_DIM:(h + 1) * HEAD_DIM], preferred_element_type=jnp.float32)
        if h <= nrot:
            t = t * cos + pltpu.roll(t, HEAD_DIM // 2, 1) * sin
        if h < nrot:
            q_ref[:, h * HEAD_DIM:(h + 1) * HEAD_DIM] = t.astype(jnp.bfloat16)
        else:
            n_ref, t_ref = (k_ref, kt_ref) if h == nrot else (v_ref, vt_ref)
            n_ref[...] = t.astype(jnp.bfloat16)
            t_ref[...] = t.T.astype(jnp.bfloat16)


def project(x, gain, w, cosw, sinw, bt=512):
    seq, dim = x.shape
    grp = w.shape[1]
    nq = grp // HEAD_DIM - 2
    row = lambda i: (i, 0)
    whole = lambda i: (0, 0)
    bf = jnp.bfloat16
    return pl.pallas_call(
        functools.partial(proj_kernel, nq), grid=(seq // bt,),
        in_specs=[pl.BlockSpec((bt, dim), row), pl.BlockSpec((16, dim), whole), pl.BlockSpec((dim, grp), whole),
                  pl.BlockSpec((bt, HEAD_DIM), row), pl.BlockSpec((bt, HEAD_DIM), row)],
        out_specs=[pl.BlockSpec((bt, dim), row), pl.BlockSpec((bt, nq * HEAD_DIM), row), pl.BlockSpec((bt, HEAD_DIM), row), pl.BlockSpec((bt, HEAD_DIM), row),
                   pl.BlockSpec((HEAD_DIM, bt), lambda i: (0, i)), pl.BlockSpec((HEAD_DIM, bt), lambda i: (0, i))],
        out_shape=[jax.ShapeDtypeStruct((seq, dim), bf), jax.ShapeDtypeStruct((seq, nq * HEAD_DIM), bf), jax.ShapeDtypeStruct((seq, HEAD_DIM), bf),
                   jax.ShapeDtypeStruct((seq, HEAD_DIM), bf), jax.ShapeDtypeStruct((HEAD_DIM, seq), bf), jax.ShapeDtypeStruct((HEAD_DIM, seq), bf)],
        cost_estimate=pl.CostEstimate(flops=2 * seq * dim * grp, bytes_accessed=32 << 20, transcendentals=0),
        compiler_params=pltpu.CompilerParams(vmem_limit_bytes=48 << 20), name="project",
    )(x, gain, w, cosw, sinw)


LOG2E = math.log2(math.e)
SCALE2 = ATTN_SCALE * LOG2E
NT = (((1,), (1,)), ((), ()))
NN = (((1,), (0,)), ((), ()))
BIG = -1e30


def fwd_kernel(bq, bk, q_ref, k_ref, vt_ref, w1, w3, w2, wo, o_ref, lse_ref, o1, o3, o2, oo, send_sem, recv_sem, local_sem):
    i = pl.program_id(0)
    last = pl.num_programs(0) - 1
    here = Spot()
    carry_over = WeightGather(here, Wires(send_sem, recv_sem), local_sem, (w1, w3, w2, wo), (o1, o3, o2, oo))

    @pl.when(i == 0)
    def _():
        greet(cube_targets(here))
        carry_over.begin()

    @pl.when(i == 2)
    def _():
        carry_over.cube.start(1)

    heads = q_ref.shape[1] // HEAD_DIM
    qs = [q_ref[:, h * HEAD_DIM:(h + 1) * HEAD_DIM] for h in range(heads)]

    def block(j, carry, masked):
        rows = pl.ds(pl.multiple_of(j * bk, bk), bk)
        k = k_ref[rows, :]
        vt = vt_ref[:, rows]
        out = []
        for h in range(heads):
            m, l, acc = carry[h]
            s = lax.dot_general(k, qs[h], NT, preferred_element_type=jnp.float32)
            if masked:
                kpos = j * bk + lax.broadcasted_iota(jnp.int32, (bk, bq), 0)
                qpos = i * bq + lax.broadcasted_iota(jnp.int32, (bk, bq), 1)
                s = jnp.where(qpos >= kpos, s, BIG)
            m_new = jnp.maximum(m, jnp.max(s, axis=0, keepdims=True))
            p = jnp.exp2((s - m_new) * SCALE2)
            alpha = jnp.exp2((m - m_new) * SCALE2)
            l = l * alpha + jnp.sum(p, axis=0, keepdims=True)
            acc = acc * alpha + lax.dot_general(vt, p.astype(jnp.bfloat16), NN, preferred_element_type=jnp.float32)
            out.append((m_new, l, acc))
        return tuple(out)

    init = tuple((jnp.full((1, bq), BIG, jnp.float32), jnp.zeros((1, bq), jnp.float32), jnp.zeros((HEAD_DIM, bq), jnp.float32)) for _ in range(heads))
    full = i * bq // bk
    carry = lax.fori_loop(0, full, lambda j, c: block(j, c, False), init)
    for d in range(max(1, bq // bk)):
        carry = block(full + d, carry, True)
    for h in range(heads):
        m, l, acc = carry[h]
        o = acc / l
        o_ref[:, h * HEAD_DIM:(h + 1) * HEAD_DIM] = o.T.astype(jnp.bfloat16)
        lse_ref[h:h + 1, :] = m * SCALE2 + jnp.log2(l)

    @pl.when(i == last)
    def _():
        carry_over.cube.start(2)
        carry_over.end()


def flash_fwd(q, k, vt, ws, cid, bq=1024, bk=512):
    seq, width = q.shape
    heads = width // HEAD_DIM
    vm = pl.BlockSpec(memory_space=pltpu.VMEM)
    an = pl.BlockSpec(memory_space=pl.ANY)
    return pl.pallas_call(
        functools.partial(fwd_kernel, bq, bk),
        grid=(seq // bq,),
        in_specs=[pl.BlockSpec((bq, width), lambda i: (i, 0)),
                  pl.BlockSpec((seq, HEAD_DIM), lambda i: (0, 0)),
                  pl.BlockSpec((HEAD_DIM, seq), lambda i: (0, 0))] + [vm] * 4,
        out_specs=[pl.BlockSpec((bq, width), lambda i: (i, 0)),
                   pl.BlockSpec((heads, bq), lambda i: (0, i))] + [an] * 4,
        out_shape=[jax.ShapeDtypeStruct((seq, width), jnp.bfloat16), jax.ShapeDtypeStruct((heads, seq), jnp.float32)] + gathered(ws),
        scratch_shapes=[pltpu.SemaphoreType.DMA((NW,)), pltpu.SemaphoreType.DMA((NW,)), pltpu.SemaphoreType.DMA((4,))],
        cost_estimate=pl.CostEstimate(flops=2 * seq * seq * width * 2, bytes_accessed=8 << 20, transcendentals=seq * seq),
        compiler_params=comm_params(cid, vmem_limit_bytes=56 << 20),
        name="flash_fwd",
    )(q, k, vt, *ws)


def bwd_kernel(bq, bk, q_ref, o_ref, d_ref, k_ref, kt_ref, v_ref, lse_ref, cos_ref, sin_ref, g1, g3, g2, out_ref, r1, r3, r2, dqt, dka, dva, rd, send_sem, recv_sem):
    j = pl.program_id(0)
    nk = pl.num_programs(0)
    seq, width = q_ref.shape
    heads = width // HEAD_DIM
    nq = seq // bq
    k = k_ref[...]
    v = v_ref[...]
    kt = kt_ref[...]
    here = Spot()
    carry_over = halve_copies(here, Wires(send_sem, recv_sem), 3, (g1, g3, g2), (r1, r3, r2))

    def turned(t, rows):
        t = t.astype(jnp.bfloat16).astype(jnp.float32)
        return (t * cos_ref[rows, :] - pltpu.roll(t, HEAD_DIM // 2, 1) * sin_ref[rows, :]).astype(jnp.bfloat16)

    @pl.when(j == 0)
    def _():
        greet([here.peer(d) for d in 'xyz'])
        for cp in carry_over:
            cp.start()
        dqt[...] = jnp.zeros_like(dqt)

        def prep(i, c):
            rows = pl.ds(pl.multiple_of(i * bq, bq), bq)
            for h in range(heads):
                cols = slice(h * HEAD_DIM, (h + 1) * HEAD_DIM)
                prod = o_ref[rows, cols].astype(jnp.float32) * d_ref[rows, cols].astype(jnp.float32)
                rd[h:h + 1, rows] = jnp.sum(prod.T, axis=0, keepdims=True)
            return c
        lax.fori_loop(0, nq, prep, 0)

    dka[...] = jnp.zeros_like(dka)
    dva[...] = jnp.zeros_like(dva)

    def block(i, masked):
        rows = pl.ds(pl.multiple_of(i * bq, bq), bq)
        for h in range(heads):
            cols = slice(h * HEAD_DIM, (h + 1) * HEAD_DIM)
            q = q_ref[rows, cols]
            d = d_ref[rows, cols]
            s = lax.dot_general(k, q, NT, preferred_element_type=jnp.float32)
            dp = lax.dot_general(v, d, NT, preferred_element_type=jnp.float32)
            p = jnp.exp2(s * SCALE2 - lse_ref[h:h + 1, rows])
            if masked:
                kpos = j * bk + lax.broadcasted_iota(jnp.int32, (bk, bq), 0)
                qpos = i * bq + lax.broadcasted_iota(jnp.int32, (bk, bq), 1)
                p = jnp.where(qpos >= kpos, p, 0.0)
            ds = (p * (dp - rd[h:h + 1, rows]) * ATTN_SCALE).astype(jnp.bfloat16)
            dva[...] += lax.dot_general(p.astype(jnp.bfloat16), d, NN, preferred_element_type=jnp.float32)
            dka[...] += lax.dot_general(ds, q, NN, preferred_element_type=jnp.float32)
            dqt[cols, rows] += lax.dot_general(kt, ds, NN, preferred_element_type=jnp.float32)

    first = j * bk // bq
    ndiag = max(1, bk // bq)
    for t in range(ndiag):
        block(first + t, True)
    lax.fori_loop(first + ndiag, nq, lambda i, c: (block(i, False), c)[1], 0)
    own = pl.ds(pl.multiple_of(j * bk, bk), bk)
    out_ref[own, width:width + HEAD_DIM] = turned(dka[...], own)
    out_ref[own, width + HEAD_DIM:] = dva[...].astype(jnp.bfloat16)

    @pl.when(j == nk - 1)
    def _():
        def fin(i, c):
            rows = pl.ds(pl.multiple_of(i * bq, bq), bq)
            for h in range(heads):
                cols = slice(h * HEAD_DIM, (h + 1) * HEAD_DIM)
                out_ref[rows, cols] = turned(dqt[cols, rows].T, rows)
            return c
        lax.fori_loop(0, nq, fin, 0)
        for cp in carry_over:
            cp.wait()


def flash_bwd(q, o, d, k, kt, v, lse, cosw, sinw, gs, cid, bq=512, bk=512):
    seq, width = q.shape
    heads = width // HEAD_DIM
    whole = lambda j: (0, 0)
    an = pl.BlockSpec(memory_space=pl.ANY)
    return pl.pallas_call(
        functools.partial(bwd_kernel, bq, bk),
        grid=(seq // bk,),
        in_specs=[pl.BlockSpec((seq, width), whole), pl.BlockSpec((seq, width), whole), pl.BlockSpec((seq, width), whole),
                  pl.BlockSpec((bk, HEAD_DIM), lambda j: (j, 0)), pl.BlockSpec((HEAD_DIM, bk), lambda j: (0, j)),
                  pl.BlockSpec((bk, HEAD_DIM), lambda j: (j, 0)),
                  pl.BlockSpec((heads, seq), whole), pl.BlockSpec((seq, HEAD_DIM), whole), pl.BlockSpec((seq, HEAD_DIM), whole)] + [an] * 3,
        out_specs=[pl.BlockSpec((seq, width + 2 * HEAD_DIM), whole)] + [an] * 3,
        out_shape=[jax.ShapeDtypeStruct((seq, width + 2 * HEAD_DIM), jnp.bfloat16)] + halve_shapes(gs, 3),
        scratch_shapes=[pltpu.VMEM((width, seq), jnp.float32), pltpu.VMEM((bk, HEAD_DIM), jnp.float32), pltpu.VMEM((bk, HEAD_DIM), jnp.float32),
                        pltpu.VMEM((heads, seq), jnp.float32), pltpu.SemaphoreType.DMA((3,)), pltpu.SemaphoreType.DMA((3,))],
        cost_estimate=pl.CostEstimate(flops=5 * seq * seq * width * 2 // 2, bytes_accessed=16 << 20, transcendentals=seq * seq),
        compiler_params=comm_params(cid, vmem_limit_bytes=58 << 20),
        name="flash_bwd",
    )(q, o, d, k, kt, v, lse, cosw, sinw, *gs)


class PlaneGather:
    N = 13

    def __init__(self, here, wires, src, out, local_sem):
        h = src.shape[0] // 2
        A, B = slice(0, h), slice(h, 2 * h)
        s = here.s
        sx, sy, sc = here.peer('x')[1], here.peer('y')[1], here.peer('c')[1]
        sd = here.s + 2 - 4 * here.x + 4 - 8 * here.y
        nx, ny, nc = here.peer('x'), here.peer('y'), here.peer('c')
        self.local = pltpu.make_async_copy(src, out.at[s], local_sem)
        mk = wires.copy
        self.x1 = {k: mk(src.at[r], out.at[s, r], nx) for k, r in (('A', A), ('B', B))}
        self.y1 = {k: mk(src.at[r], out.at[s, r], ny) for k, r in (('B', B), ('A', A))}
        self.c1 = mk(src, out.at[s], nc)
        self.fy = mk(out.at[sx, A], out.at[sx, A], ny)
        self.fx = mk(out.at[sy, B], out.at[sy, B], nx)
        self.cc = {}
        for name, idx in (('x', sx), ('y', sy), ('d', sd)):
            for k, r in (('A', A), ('B', B)):
                self.cc[name + k] = mk(out.at[idx, r], out.at[idx, r], nc)

    def start_first(self):
        self.x1['A'].start()
        self.y1['B'].start()
        self.c1.start()
        self.local.start()

    def start_second(self):
        self.x1['B'].start()
        self.y1['A'].start()

    def relay(self):
        self.x1['A'].wait_recv()
        self.fy.start()
        self.cc['xA'].start()
        self.y1['B'].wait_recv()
        self.fx.start()
        self.cc['yB'].start()
        self.x1['B'].wait_recv()
        self.cc['xB'].start()
        self.y1['A'].wait_recv()
        self.cc['yA'].start()

    def finish(self):
        self.fy.wait_recv()
        self.cc['dA'].start()
        self.fx.wait_recv()
        self.cc['dB'].start()
        self.c1.wait_recv()
        for k in self.cc:
            self.cc[k].wait_recv()
        for c in (*self.x1.values(), *self.y1.values(), self.c1, self.fy, self.fx, *self.cc.values()):
            c.wait_send()
        self.local.wait()


NG = PlaneGather.N + 2 * 6 + 1


def dh_kernel(src, wg, out, og, send_sem, recv_sem, local_sem):
    here = Spot()
    greet(cube_targets(here))
    wires = Wires(send_sem, recv_sem)
    c = here.c
    loc = pltpu.make_async_copy(wg, og.at[here.region('') + (c,)], local_sem.at[1])
    g = PlaneGather(here, wires, src, out, local_sem.at[0])
    jobs = [(og, (c, slice(None), slice(off, off + n)), order) for (off, n), order in zip(col_chunks(wg.shape[1], 2), ('xyz', 'yxz'))]
    cube = CubeGather(here, wires, jobs)
    post = wires.copy(og.at[:, :, :, c], og.at[:, :, :, c], here.peer('c'))
    loc.start()
    loc.wait()
    cube.start(0)
    g.start_first()
    cube.start(1)
    g.start_second()
    g.relay()
    cube.start(2)
    g.finish()
    cube.arrive()
    post.start()
    post.wait()
    cube.drain()


def gather_dh(src, wg, cid):
    rows, cols = src.shape
    vm = pl.BlockSpec(memory_space=pltpu.VMEM)
    an = pl.BlockSpec(memory_space=pl.ANY)
    return pl.pallas_call(
        dh_kernel, in_specs=[vm] * 2, out_specs=[an] * 2,
        out_shape=[jax.ShapeDtypeStruct((8, rows, cols), src.dtype), jax.ShapeDtypeStruct((2, 2, 2, 2, *wg.shape), wg.dtype)],
        scratch_shapes=[pltpu.SemaphoreType.DMA((NG,)), pltpu.SemaphoreType.DMA((NG,)), pltpu.SemaphoreType.DMA((2,))],
        cost_estimate=busy(50), compiler_params=comm_params(cid), name="gather_dh",
    )(src, wg)


def entry_kernel(x_ref, w_ref, meta_ref, pos_ref, xa, wa, ma, pa, send_sem, recv_sem, local_sem):
    here = Spot()
    z, s = here.z, here.s
    peers = here.others()
    nz = here.peer('z')
    greet(peers + [nz])
    wires = Wires(send_sem, recv_sem)
    first = []
    for t in peers:
        for src, dst in ((w_ref.at[t[1]], wa.at[z, s]), (meta_ref, ma.at[z, s]), (pos_ref, pa.at[s])):
            first.append(wires.copy(src, dst, t))
    locals_ = [pltpu.make_async_copy(w_ref.at[s], wa.at[z, s], local_sem.at[1]),
               pltpu.make_async_copy(meta_ref, ma.at[z, s], local_sem.at[2]),
               pltpu.make_async_copy(pos_ref, pa.at[s], local_sem.at[3])]
    g = PlaneGather(here, wires, x_ref, xa, local_sem.at[0])
    cross = [wires.copy(wa.at[z], wa.at[z], nz), wires.copy(ma.at[z], ma.at[z], nz)]
    for c in first:
        c.start()
    for c in locals_:
        c.start()
    g.start_first()
    g.start_second()
    for c in first:
        c.wait_recv()
    for c in locals_:
        c.wait()
    for c in cross:
        c.start()
    g.relay()
    g.finish()
    for c in cross:
        c.wait()
    for c in first:
        c.wait_send()


def entry(x, w, meta, pos, cid):
    n = PlaneGather.N + 21 + 2
    vm = pl.BlockSpec(memory_space=pltpu.VMEM)
    an = pl.BlockSpec(memory_space=pl.ANY)
    return pl.pallas_call(
        entry_kernel,
        in_specs=[vm] * 4, out_specs=[an] * 4,
        out_shape=[jax.ShapeDtypeStruct((8, *x.shape), x.dtype), jax.ShapeDtypeStruct((2, 8, *w.shape[1:]), w.dtype),
                   jax.ShapeDtypeStruct((2, 8, *meta.shape), meta.dtype), jax.ShapeDtypeStruct((8, *pos.shape), pos.dtype)],
        scratch_shapes=[pltpu.SemaphoreType.DMA((n,)), pltpu.SemaphoreType.DMA((n,)), pltpu.SemaphoreType.DMA((4,))],
        cost_estimate=busy(45), compiler_params=comm_params(cid),
        name="entry",
    )(x, w, meta, pos)


def regroup_kernel(n, *refs):
    src, gs, out, rs = refs[0], refs[1:1 + n], refs[1 + n], refs[2 + n:2 + 2 * n]
    send_sem, recv_sem, local_sem, stage = refs[2 + 2 * n:]
    here = Spot()
    s = here.s
    rows, width = out.shape[0], src.shape[1]
    peers = here.others()
    greet(peers + ([here.peer('z')] if n else []))
    wires = Wires(send_sem, recv_sem)
    piece = lambda i: pl.ds(pl.multiple_of(i * rows, rows), rows)
    mine = pl.ds(pl.multiple_of(s * width, width), width)
    cs = [wires.copy(src.at[piece(t[1])], out.at[:, mine], t) for t in peers]
    cs += halve_copies(here, wires, 2, gs, rs)
    for c in cs:
        c.start()
    a = pltpu.make_async_copy(src.at[piece(s)], stage, local_sem.at[0])
    a.start()
    a.wait()
    b = pltpu.make_async_copy(stage, out.at[:, mine], local_sem.at[1])
    b.start()
    b.wait()
    for c in cs:
        c.wait()


def regroup(src, gs, cid, name):
    seq, width = src.shape
    rows, n = seq // 8, len(gs)
    an = pl.BlockSpec(memory_space=pl.ANY)
    out = pl.pallas_call(
        functools.partial(regroup_kernel, n), in_specs=[an] * (1 + n), out_specs=[an] * (1 + n),
        out_shape=[jax.ShapeDtypeStruct((rows, 8 * width), src.dtype)] + halve_shapes(gs, 2),
        scratch_shapes=[pltpu.SemaphoreType.DMA((7 + n,)), pltpu.SemaphoreType.DMA((7 + n,)), pltpu.SemaphoreType.DMA((2,)), pltpu.VMEM((rows, width), src.dtype)],
        cost_estimate=busy(70 if n else 25), compiler_params=comm_params(cid), name=name,
    )(src, *gs)
    return out[0], out[1:]


def owner_kernel(n, *refs):
    a, b, gs, oa, ob, rs = refs[0], refs[1], refs[2:2 + n], refs[2 + n], refs[3 + n], refs[4 + n:4 + 2 * n]
    send_sem, recv_sem, local_sem = refs[4 + 2 * n:]
    here = Spot()
    peers = here.others()
    greet(peers + [here.peer('z')])
    wires = Wires(send_sem, recv_sem)
    s = here.s
    cs = halve_copies(here, wires, 1, gs, rs)
    cs += [wires.copy(r.at[t[1]], o.at[s], t) for t in peers for r, o in ((a, oa), (b, ob))]
    loc = [pltpu.make_async_copy(a.at[s], oa.at[s], local_sem.at[0]), pltpu.make_async_copy(b.at[s], ob.at[s], local_sem.at[1])]
    for c in cs + loc:
        c.start()
    for c in cs + loc:
        c.wait()


def owner(a, b, gs, cid):
    n = len(gs)
    vm = pl.BlockSpec(memory_space=pltpu.VMEM)
    an = pl.BlockSpec(memory_space=pl.ANY)
    out = pl.pallas_call(
        functools.partial(owner_kernel, n), in_specs=[vm] * 2 + [an] * n, out_specs=[vm] * 2 + [an] * n,
        out_shape=[jax.ShapeDtypeStruct(t.shape, t.dtype) for t in (a, b)] + halve_shapes(gs, 1),
        scratch_shapes=[pltpu.SemaphoreType.DMA((14 + n,)), pltpu.SemaphoreType.DMA((14 + n,)), pltpu.SemaphoreType.DMA((2,))],
        cost_estimate=busy(30), compiler_params=comm_params(cid), name="owner",
    )(a, b, *gs)
    return out[0], out[1], out[2:]


def dot_tokens(left_op, right_op):
    return lax.dot_general(left_op, right_op, (((0,), (0,)), ((), ())), preferred_element_type=jnp.float32)


def dot_back(left_op, weight):
    return lax.dot_general(left_op, weight, (((1,), (1,)), ((), ())), preferred_element_type=jnp.float32)


def dot_on(left_op, weight):
    return jnp.dot(left_op, weight, preferred_element_type=jnp.float32)


def swap_core(t):
    return lax.ppermute(t, 'sp', [(i, i ^ 1) for i in range(8)])


def swap_z(t):
    return lax.ppermute(t, 'dp', [(0, 1), (1, 0)])


def split_cols(w):
    rows, cols = w.shape
    return w.reshape(rows, 8, 2, cols // 16).transpose(2, 0, 1, 3).reshape(2, rows, cols // 2)


def join_cols(mine, other, c):
    rows, half = mine.shape
    m, o = mine.reshape(rows, 8, 1, half // 8), other.reshape(rows, 8, 1, half // 8)
    first = jnp.where(c == 0, m, o)
    second = jnp.where(c == 0, o, m)
    return jnp.concatenate([first, second], axis=2).reshape(rows, 2 * half)


def layer_step(hidden, positions, grad_out, gain_attn, gain_mlp, w_query, w_key, w_value, w_out, w_gate, w_up, w_down):
    tokens = hidden[0]
    d_layer = grad_out[0]
    tok, dim = tokens.shape
    here = Spot()
    z, s, c = here.z, here.s, here.c
    rows = w_query.shape[0]
    grp_q = w_query.shape[1] // 8
    grp_k = w_key.shape[1] // 8
    grp = grp_q + 2 * grp_k
    seq = 8 * tok

    w_grp = jnp.concatenate([w_query.reshape(rows, 8, grp_q), w_key.reshape(rows, 8, grp_k), w_value.reshape(rows, 8, grp_k)], axis=2)
    w_flat = w_grp.reshape(rows, 8 * grp)
    pad = HEAD_DIM - gain_attn.shape[0]
    meta = jnp.pad(jnp.stack([jnp.pad(gain_attn, (0, pad)), jnp.pad(gain_mlp, (0, pad))]), ((0, 14), (0, 0)))
    x_all, w_own, meta_all, pos_all = entry(tokens, w_grp.transpose(1, 0, 2), meta, positions[0].reshape(-1, 128), 1)
    x_all = x_all.reshape(seq, dim)
    w_own = w_own.reshape(dim, grp)
    gain1 = meta_all[:, :, 0, :rows].reshape(dim)
    gain2 = meta_all[:, :, 1, :rows].reshape(dim)
    cos_tab, sin_tab = rope_tables(pos_all.reshape(seq))

    cosw = jnp.concatenate([cos_tab, cos_tab], axis=1)
    sinw = jnp.concatenate([-sin_tab, sin_tab], axis=1)
    u_all, q_own, k_own, v_own, k_t, v_t = project(x_all, jnp.broadcast_to(gain1[None], (16, dim)), w_own, cosw, sinw)
    o_own, lse, w1, w3, w2, wo = flash_fwd(q_own, k_own, v_t, (split_cols(w_gate), split_cols(w_up), w_down, w_out), 2)
    ffn_half = w1.shape[-1]
    w1, w3 = w1.reshape(dim, ffn_half), w3.reshape(dim, ffn_half)
    w2 = w2.reshape(ffn_half, dim)
    wo = wo.reshape(-1, dim)
    attn_out, _ = regroup(o_own, (), 3, 'regroup_o')
    residual = (tokens.astype(jnp.float32) + dot_on(attn_out, wo)).astype(jnp.bfloat16)
    u_mlp, normed2, inv_rms2 = rms_norm(residual, gain2)
    u_pair = jnp.concatenate([u_mlp, swap_core(u_mlp)], axis=0)
    d_pair = jnp.concatenate([d_layer, swap_core(d_layer)], axis=0)
    gate_pre = dot_on(u_pair, w1)
    up_pre = dot_on(u_pair, w3)
    sig_gate = jax.nn.sigmoid(gate_pre)
    silu_gate = gate_pre * sig_gate
    mlp_act = (silu_gate * up_pre).astype(jnp.bfloat16)
    y_part = dot_on(mlp_act, w2)
    layer_out = (residual.astype(jnp.float32) + (y_part[:tok] + swap_core(y_part[tok:]))).astype(jnp.bfloat16)

    d_act = dot_back(d_pair, w2)
    d_gate = (d_act * up_pre * sig_gate * (1.0 + gate_pre * (1.0 - sig_gate))).astype(jnp.bfloat16)
    d_up = (d_act * silu_gate).astype(jnp.bfloat16)
    d_part = dot_back(d_gate, w1) + dot_back(d_up, w3)
    d_umlp = d_part[:tok] + swap_core(d_part[tok:])
    d_res_norm, d_gain2 = rms_norm_grad(d_umlp, normed2, inv_rms2, gain2)
    d_resid = d_layer.astype(jnp.float32) + d_res_norm
    d_resid_bf = d_resid.astype(jnp.bfloat16)
    g1 = dot_tokens(u_pair, d_gate).reshape(2, 2, 2, dim // 8, ffn_half)
    g3 = dot_tokens(u_pair, d_up).reshape(2, 2, 2, dim // 8, ffn_half)
    g2 = dot_tokens(mlp_act, d_pair).reshape(2, 2, 2, ffn_half // 8, dim)

    dh_all, wg = gather_dh(d_resid_bf, w_flat, 4)
    dh_all = dh_all.reshape(seq, dim)
    wg = wg.reshape(dim, 8 * grp)
    wo_own = lax.dynamic_slice_in_dim(wo, s * grp_q, grp_q, 0)
    d_own = dot_back(dh_all, wo_own).astype(jnp.bfloat16)
    go = dot_tokens(o_own, dh_all).reshape(2, grp_q // 2, dim)
    dqkv_pre, *got = flash_bwd(q_own, o_own, d_own, k_own, k_t, v_own, lse, cosw, sinw, (g1, g3, g2), 6)
    g_mlp = halve_add((g1, g3, g2), got, 3)

    go_mine = lax.dynamic_index_in_dim(go, z, 0, False) + swap_z(lax.dynamic_index_in_dim(go, 1 - z, 0, False))
    grad_w_out = lax.ppermute(go_mine, ALL_AXES, [(zz * 8 + ss, 2 * ss + zz) for zz in range(2) for ss in range(8)])
    dqkv_tok, got = regroup(dqkv_pre, g_mlp, 5, 'regroup_dqkv')
    g_mlp = halve_add(g_mlp, got, 2)
    gq = dot_tokens(u_all, dqkv_pre).reshape(2, dim // 2, grp)
    gq_mine = lax.dynamic_index_in_dim(gq, z, 0, False) + swap_z(lax.dynamic_index_in_dim(gq, 1 - z, 0, False))
    d_uattn = dot_back(dqkv_tok, wg)
    _, normed1, inv_rms1 = rms_norm(tokens, gain1)
    d_tok_norm, d_gain1 = rms_norm_grad(d_uattn, normed1, inv_rms1, gain1)
    grad_hidden = (d_resid + d_tok_norm).astype(jnp.bfloat16)

    gains = jnp.concatenate([d_gain1.reshape(2, 8, rows), d_gain2.reshape(2, 8, rows)], axis=2)
    gains_mine = lax.dynamic_index_in_dim(gains, z, 0, False) + swap_z(lax.dynamic_index_in_dim(gains, 1 - z, 0, False))
    gains_mine = jnp.broadcast_to(gains_mine[:, None, :], (8, 8, 2 * rows))
    got_q, got_g, got = owner(gq_mine.reshape(8, rows, grp), gains_mine, g_mlp, 10)
    got_q = got_q.transpose(1, 0, 2)
    grad_w_query = got_q[:, :, :grp_q].reshape(rows, 8 * grp_q)
    grad_w_key = got_q[:, :, grp_q:grp_q + grp_k].reshape(rows, 8 * grp_k)
    grad_w_value = got_q[:, :, grp_q + grp_k:].reshape(rows, 8 * grp_k)
    grad_gains = jnp.sum(got_g[:, 0, :], axis=0)
    grad_gain_attn, grad_gain_mlp = grad_gains[:rows], grad_gains[rows:]

    m1, m3, grad_w_down = halve_add(g_mlp, got, 1)
    pair = jnp.stack([m1.reshape(2, rows, ffn_half), m3.reshape(2, rows, ffn_half)], axis=1)
    keep = lax.dynamic_index_in_dim(pair, c, 0, False)
    other = swap_core(lax.dynamic_index_in_dim(pair, 1 - c, 0, False))
    grad_w_gate = join_cols(keep[0], other[0], c)
    grad_w_up = join_cols(keep[1], other[1], c)
    return (layer_out[None], grad_hidden[None], grad_gain_attn, grad_gain_mlp, grad_w_query, grad_w_key, grad_w_value, grad_w_out, grad_w_gate, grad_w_up, grad_w_down)


def solution(mesh):
    act_spec = P('dp', 'sp', None)
    pos_spec = P('dp', 'sp')
    vec_spec = P(ALL_AXES)
    mat_spec = P(ALL_AXES, None)
    in_specs = (act_spec, pos_spec, act_spec, vec_spec, vec_spec) + (mat_spec,) * 7
    out_specs = (act_spec, act_spec, vec_spec, vec_spec) + (mat_spec,) * 7
    return jax.shard_map(layer_step, mesh=mesh, in_specs=in_specs, out_specs=out_specs, check_vma=False)
```

```python
import functools
import math

import jax
import jax.numpy as jnp
from jax import lax
from jax.experimental import pallas as pl
from jax.experimental.pallas import tpu as pltpu
from jax.sharding import PartitionSpec as P

HEAD_DIM = 128
ROPE_BASE = 10000.0
NORM_EPS = 1e-5
ATTN_SCALE = HEAD_DIM ** -0.5
ALL_AXES = ('dp', 'sp')


def rope_tables(pos_ids):
    inv_freq = ROPE_BASE ** (-(jnp.arange(HEAD_DIM // 2, dtype=jnp.float32) * (2.0 / HEAD_DIM)))
    angles = pos_ids.astype(jnp.float32)[None, :] * inv_freq[:, None]
    return jnp.cos(angles), jnp.sin(angles)


def rms_norm(values, gain_vec):
    vals32 = values.astype(jnp.float32)
    inv_rms = lax.rsqrt(jnp.mean(vals32 * vals32, axis=-1, keepdims=True) + NORM_EPS)
    normed = vals32 * inv_rms
    return (normed * gain_vec.astype(jnp.float32)).astype(jnp.bfloat16), normed, inv_rms


def rms_norm_grad(d_out, normed, inv_rms, gain_vec):
    d_normed = d_out * gain_vec.astype(jnp.float32)
    grad_gain = jnp.sum(d_out * normed, axis=0)
    grad_in = inv_rms * (d_normed - normed * jnp.mean(d_normed * normed, axis=-1, keepdims=True))
    return grad_in, grad_gain


MESH = pl.DeviceIdType.MESH


def by_rows(i):
    return i, 0


def by_cols(i):
    return 0, i


def whole(i):
    return 0, 0


def head(h):
    return slice(h * HEAD_DIM, (h + 1) * HEAD_DIM)


def pick(t, i):
    return lax.dynamic_index_in_dim(t, i, 0, False)


ORDERS = ('xyz', 'yzx', 'zxy')


class Spot:
    def __init__(self):
        self.z = lax.axis_index('dp')
        self.s = lax.axis_index('sp')
        self.y = self.s // 4
        self.x = (self.s // 2) % 2
        self.c = self.s % 2
        self.bits = {'z': self.z, 'y': self.y, 'x': self.x}

    def peer(self, dim):
        if dim == 'z':
            return (1 - self.z, self.s)
        if dim == 'y':
            return (self.z, self.s + 4 - 8 * self.y)
        if dim == 'x':
            return (self.z, self.s + 2 - 4 * self.x)
        return (self.z, self.s + 1 - 2 * self.c)

    def others(self):
        return [(self.z, (self.s + t) % 8) for t in range(1, 8)]

    def region(self, freed, flipped=''):
        return tuple(slice(None) if d in freed else (1 - self.bits[d] if d in flipped else self.bits[d]) for d in 'zyx')


def greet(targets):
    bar = pltpu.get_barrier_semaphore()
    for t in targets:
        pl.semaphore_signal(bar, inc=1, device_id=t, device_id_type=MESH)
    pl.semaphore_wait(bar, len(targets))


class Wires:
    def __init__(self, send_sem, recv_sem):
        self.send_sem, self.recv_sem, self.n = send_sem, recv_sem, 0

    def copy(self, src, dst, target):
        i = self.n
        self.n += 1
        return pltpu.make_async_remote_copy(src_ref=src, dst_ref=dst, send_sem=self.send_sem.at[i], recv_sem=self.recv_sem.at[i], device_id=target, device_id_type=MESH)


class CubeGather:
    def __init__(self, here, wires, jobs):
        firsts, seconds, thirds = [], [], []
        for out, suffix, (a, b, e) in jobs:
            def mk(freed, flipped, d):
                reg = here.region(freed, flipped) + suffix
                return wires.copy(out.at[reg], out.at[reg], here.peer(d))
            firsts.append([mk('', '', d) for d in (a, b, e)])
            seconds.append([mk('', a, d) for d in (b, e)])
            thirds.append(mk(a, b, e))
        self.stages = [[f[i] for i in range(3) for f in firsts], [t[i] for i in range(2) for t in seconds], thirds]
        self.need = [[f[0] for f in firsts], [f[1] for f in firsts] + [t[0] for t in seconds]]
        self.rest = [[f[2], t[1], e] for f, t, e in zip(firsts, seconds, thirds)]

    def start(self, i):
        for c in self.need[i - 1] if i else ():
            c.wait_recv()
        for c in self.stages[i]:
            c.start()

    def arrive(self, lo=0, hi=None):
        for job in self.rest[lo:hi]:
            for c in job:
                c.wait_recv()

    def drain(self):
        for st in self.stages:
            for c in st:
                c.wait_send()


def col_chunks(cols, parts):
    n, out, off = cols // 128, [], 0
    for p in range(parts, 0, -1):
        w = -(-n // p)
        out.append((off, w * 128))
        off += w * 128
        n -= w
    return out


def cube_targets(here):
    return [here.peer(d) for d in 'xyzc']


def comm_params(cid, **kw):
    return pltpu.CompilerParams(collective_id=cid, has_side_effects=True, **kw)


def busy(us):
    return pl.CostEstimate(flops=int(us * 1e8), bytes_accessed=1 << 20, transcendentals=0)


NW = 2 + 6 * 6 + 1


class WeightGather:
    def __init__(self, here, wires, local_sem, ins, outs):
        w1, w3, w2, wo = ins
        o1, o3, o2, oo = outs
        c, zyx, nc = here.c, here.region(''), here.peer('c')
        self.pre = [wires.copy(w1.at[1 - c], o1.at[zyx + (c,)], nc), wires.copy(w3.at[1 - c], o3.at[zyx + (c,)], nc)]
        self.loc = [pltpu.make_async_copy(w1.at[c], o1.at[zyx + (c,)], local_sem.at[0]),
                    pltpu.make_async_copy(w3.at[c], o3.at[zyx + (c,)], local_sem.at[1]),
                    pltpu.make_async_copy(w2, o2.at[zyx], local_sem.at[2]),
                    pltpu.make_async_copy(wo, oo.at[zyx + (c,)], local_sem.at[3])]
        jobs = [(oo, (c, slice(None), slice(off, off + n)), order) for (off, n), order in zip(col_chunks(wo.shape[1], 3), ORDERS)]
        jobs += [(o1, (), ORDERS[0]), (o3, (), ORDERS[1]), (o2, (), ORDERS[2])]
        self.cube = CubeGather(here, wires, jobs)
        self.post = wires.copy(oo.at[:, :, :, c], oo.at[:, :, :, c], nc)

    def begin(self):
        for c in self.pre + self.loc:
            c.start()
        for c in self.loc:
            c.wait()
        for c in self.pre:
            c.wait()
        self.cube.start(0)

    def end(self):
        self.cube.arrive(0, 3)
        self.post.start()
        self.cube.arrive(3)
        self.post.wait()
        self.cube.drain()


def gathered(ws):
    return [jax.ShapeDtypeStruct((2, 2, 2, *w.shape), w.dtype) if k < 3 else jax.ShapeDtypeStruct((2, 2, 2, 2, *w.shape), w.dtype) for k, w in enumerate(ws)]


def halve_copies(here, wires, nd, ins, outs):
    cs = []
    for i, (a, o) in enumerate(zip(ins, outs)):
        order = ORDERS[i % 3]
        d = order[nd - 1]
        reg = tuple(1 - here.bits[d] if e == d else slice(None) for e in 'zyx' if e in order[:nd])
        cs.append(wires.copy(a.at[reg], o, here.peer(d)))
    return cs


def halve_shapes(arrs, nd):
    return [jax.ShapeDtypeStruct((*((2,) * (nd - 1)), *a.shape[nd:]), a.dtype) for a in arrs]


def part_of(here, t, order, nd, flip):
    live = [d for d in 'zyx' if d in order[:nd]]
    d = order[nd - 1]
    bit = here.bits[d]
    return lax.dynamic_index_in_dim(t, 1 - bit if flip else bit, live.index(d), False)


def total(terms):
    out = terms[0]
    for t in terms[1:]:
        out = out + t
    return out


def to_send(here, terms, nd):
    return [total([part_of(here, t, ORDERS[i % 3], nd, True) for t in ts]) for i, ts in enumerate(terms)]


def after(here, terms, got, nd):
    return [[part_of(here, t, ORDERS[i % 3], nd, False) for t in ts] + [r] for i, (ts, r) in enumerate(zip(terms, got))]


def wide_tables(cos_t, sin_t):
    return jnp.concatenate([cos_t, cos_t], axis=0).T, jnp.concatenate([-sin_t, sin_t], axis=0).T


def proj_kernel(nrot, x_ref, g_ref, w_ref, cos_ref, sin_ref, u_ref, q_ref, k_ref, v_ref, kt_ref, vt_ref):
    x = x_ref[...].astype(jnp.float32)
    inv = lax.rsqrt(jnp.mean(x * x, axis=-1, keepdims=True) + NORM_EPS)
    u = (x * inv * g_ref[0:1, :].astype(jnp.float32)).astype(jnp.bfloat16)
    u_ref[...] = u
    cos, sin = wide_tables(cos_ref[...], sin_ref[...])
    for h in range(nrot + 2):
        t = jnp.dot(u, w_ref[:, head(h)], preferred_element_type=jnp.float32)
        if h <= nrot:
            t = t * cos + pltpu.roll(t, HEAD_DIM // 2, 1) * sin
        if h < nrot:
            q_ref[:, head(h)] = t.astype(jnp.bfloat16)
        else:
            n_ref, t_ref = (k_ref, kt_ref) if h == nrot else (v_ref, vt_ref)
            n_ref[...] = t.astype(jnp.bfloat16)
            t_ref[...] = t.T.astype(jnp.bfloat16)


def project(x, gain, w, cos_t, sin_t, bt=512):
    seq, dim = x.shape
    grp = w.shape[1]
    nq = grp // HEAD_DIM - 2
    bf = jnp.bfloat16
    return pl.pallas_call(
        functools.partial(proj_kernel, nq), grid=(seq // bt,),
        in_specs=[pl.BlockSpec((bt, dim), by_rows), pl.BlockSpec((16, dim), whole), pl.BlockSpec((dim, grp), whole),
                  pl.BlockSpec((cos_t.shape[0], bt), by_cols), pl.BlockSpec((cos_t.shape[0], bt), by_cols)],
        out_specs=[pl.BlockSpec((bt, dim), by_rows), pl.BlockSpec((bt, nq * HEAD_DIM), by_rows), pl.BlockSpec((bt, HEAD_DIM), by_rows), pl.BlockSpec((bt, HEAD_DIM), by_rows),
                   pl.BlockSpec((HEAD_DIM, bt), by_cols), pl.BlockSpec((HEAD_DIM, bt), by_cols)],
        out_shape=[jax.ShapeDtypeStruct((seq, dim), bf), jax.ShapeDtypeStruct((seq, nq * HEAD_DIM), bf), jax.ShapeDtypeStruct((seq, HEAD_DIM), bf),
                   jax.ShapeDtypeStruct((seq, HEAD_DIM), bf), jax.ShapeDtypeStruct((HEAD_DIM, seq), bf), jax.ShapeDtypeStruct((HEAD_DIM, seq), bf)],
        cost_estimate=pl.CostEstimate(flops=2 * seq * dim * grp, bytes_accessed=32 << 20, transcendentals=0),
        compiler_params=pltpu.CompilerParams(vmem_limit_bytes=48 << 20), name="project",
    )(x, gain, w, cos_t, sin_t)


LOG2E = math.log2(math.e)
SCALE2 = ATTN_SCALE * LOG2E
NT = (((1,), (1,)), ((), ()))
NN = (((1,), (0,)), ((), ()))
BIG = -1e30


def fwd_kernel(bq, bk, q_ref, k_ref, vt_ref, w1, w3, w2, wo, o_ref, ot_ref, lse_ref, o1, o3, o2, oo, send_sem, recv_sem, local_sem):
    i = pl.program_id(0)
    last = pl.num_programs(0) - 1
    here = Spot()
    carry_over = WeightGather(here, Wires(send_sem, recv_sem), local_sem, (w1, w3, w2, wo), (o1, o3, o2, oo))

    @pl.when(i == 0)
    def _():
        greet(cube_targets(here))
        carry_over.begin()

    @pl.when(i == 2)
    def _():
        carry_over.cube.start(1)

    heads = q_ref.shape[1] // HEAD_DIM
    qs = [q_ref[:, head(h)] for h in range(heads)]

    def block(j, carry, masked):
        rows = pl.ds(pl.multiple_of(j * bk, bk), bk)
        k = k_ref[rows, :]
        vt = vt_ref[:, rows]
        out = []
        for h in range(heads):
            m, l, acc = carry[h]
            s = lax.dot_general(k, qs[h], NT, preferred_element_type=jnp.float32)
            if masked:
                kpos = j * bk + lax.broadcasted_iota(jnp.int32, (bk, bq), 0)
                qpos = i * bq + lax.broadcasted_iota(jnp.int32, (bk, bq), 1)
                s = jnp.where(qpos >= kpos, s, BIG)
            m_new = jnp.maximum(m, jnp.max(s, axis=0, keepdims=True))
            p = jnp.exp2((s - m_new) * SCALE2)
            alpha = jnp.exp2((m - m_new) * SCALE2)
            l = l * alpha + jnp.sum(p, axis=0, keepdims=True)
            acc = acc * alpha + lax.dot_general(vt, p.astype(jnp.bfloat16), NN, preferred_element_type=jnp.float32)
            out.append((m_new, l, acc))
        return tuple(out)

    init = tuple((jnp.full((1, bq), BIG, jnp.float32), jnp.zeros((1, bq), jnp.float32), jnp.zeros((HEAD_DIM, bq), jnp.float32)) for _ in range(heads))
    full = i * bq // bk
    carry = lax.fori_loop(0, full, lambda j, c: block(j, c, False), init)
    for d in range(max(1, bq // bk)):
        carry = block(full + d, carry, True)
    for h in range(heads):
        m, l, acc = carry[h]
        o = acc / l
        o_ref[:, head(h)] = o.T.astype(jnp.bfloat16)
        ot_ref[head(h), :] = o.astype(jnp.bfloat16)
        lse_ref[h:h + 1, :] = m * SCALE2 + jnp.log2(l)

    @pl.when(i == last)
    def _():
        carry_over.cube.start(2)
        carry_over.end()


def flash_fwd(q, k, vt, ws, cid, bq=1024, bk=512):
    seq, width = q.shape
    heads = width // HEAD_DIM
    vm = pl.BlockSpec(memory_space=pltpu.VMEM)
    an = pl.BlockSpec(memory_space=pl.ANY)
    return pl.pallas_call(
        functools.partial(fwd_kernel, bq, bk),
        grid=(seq // bq,),
        in_specs=[pl.BlockSpec((bq, width), by_rows),
                  pl.BlockSpec((seq, HEAD_DIM), whole),
                  pl.BlockSpec((HEAD_DIM, seq), whole)] + [vm] * 4,
        out_specs=[pl.BlockSpec((bq, width), by_rows), pl.BlockSpec((width, bq), by_cols),
                   pl.BlockSpec((heads, bq), by_cols)] + [an] * 4,
        out_shape=[jax.ShapeDtypeStruct((seq, width), jnp.bfloat16), jax.ShapeDtypeStruct((width, seq), jnp.bfloat16), jax.ShapeDtypeStruct((heads, seq), jnp.float32)] + gathered(ws),
        scratch_shapes=[pltpu.SemaphoreType.DMA((NW,)), pltpu.SemaphoreType.DMA((NW,)), pltpu.SemaphoreType.DMA((4,))],
        cost_estimate=pl.CostEstimate(flops=2 * seq * seq * width * 2, bytes_accessed=8 << 20, transcendentals=seq * seq),
        compiler_params=comm_params(cid, vmem_limit_bytes=56 << 20),
        name="flash_fwd",
    )(q, k, vt, *ws)


def bwd_kernel(bq, bk, q_ref, o_ref, d_ref, k_ref, kt_ref, v_ref, lse_ref, cos_ref, sin_ref, g1, g3, g2, out_ref, r1, r3, r2, dqt, dka, dva, rd, send_sem, recv_sem):
    j = pl.program_id(0)
    nk = pl.num_programs(0)
    seq, width = q_ref.shape
    heads = width // HEAD_DIM
    nq = seq // bq
    k = k_ref[...]
    v = v_ref[...]
    kt = kt_ref[...]
    here = Spot()
    wires = Wires(send_sem, recv_sem)
    carry_over = halve_copies(here, wires, 3, (g1, g3, g2), (r1, r3, r2))

    half = HEAD_DIM // 2

    @pl.when(j == 0)
    def _():
        greet([here.peer(d) for d in 'xyz'])
        for cp in carry_over:
            cp.start()
        dqt[...] = jnp.zeros_like(dqt)

        def prep(i, c):
            rows = pl.ds(pl.multiple_of(i * bq, bq), bq)
            for h in range(heads):
                cols = head(h)
                prod = o_ref[rows, cols].astype(jnp.float32) * d_ref[rows, cols].astype(jnp.float32)
                rd[h:h + 1, rows] = jnp.sum(prod.T, axis=0, keepdims=True)
            return c
        lax.fori_loop(0, nq, prep, 0)

    dka[...] = jnp.zeros_like(dka)
    dva[...] = jnp.zeros_like(dva)

    def block(i, masked):
        rows = pl.ds(pl.multiple_of(i * bq, bq), bq)
        for h in range(heads):
            cols = head(h)
            q = q_ref[rows, cols]
            d = d_ref[rows, cols]
            s = lax.dot_general(k, q, NT, preferred_element_type=jnp.float32)
            dp = lax.dot_general(v, d, NT, preferred_element_type=jnp.float32)
            p = jnp.exp2(s * SCALE2 - lse_ref[h:h + 1, rows])
            if masked:
                kpos = j * bk + lax.broadcasted_iota(jnp.int32, (bk, bq), 0)
                qpos = i * bq + lax.broadcasted_iota(jnp.int32, (bk, bq), 1)
                p = jnp.where(qpos >= kpos, p, 0.0)
            ds = (p * (dp - rd[h:h + 1, rows]) * ATTN_SCALE).astype(jnp.bfloat16)
            dva[...] += lax.dot_general(p.astype(jnp.bfloat16), d, NN, preferred_element_type=jnp.float32)
            dka[...] += lax.dot_general(ds, q, NN, preferred_element_type=jnp.float32)
            dqt[cols, rows] += lax.dot_general(kt, ds, NN, preferred_element_type=jnp.float32)

    first = j * bk // bq
    ndiag = max(1, bk // bq)
    for t in range(ndiag):
        block(first + t, True)
    lax.fori_loop(first + ndiag, nq, lambda i, c: (block(i, False), c)[1], 0)
    own = pl.ds(pl.multiple_of(j * bk, bk), bk)
    cosw, sinw = wide_tables(cos_ref[:, own], sin_ref[:, own])
    dk = dka[...].astype(jnp.bfloat16).astype(jnp.float32)
    out_ref[own, width:width + HEAD_DIM] = (dk * cosw - pltpu.roll(dk, half, 1) * sinw).astype(jnp.bfloat16)
    out_ref[own, width + HEAD_DIM:] = dva[...].astype(jnp.bfloat16)

    @pl.when(j == nk - 1)
    def _():
        def fin(i, c):
            rows = pl.ds(pl.multiple_of(i * bq, bq), bq)
            cos, sin = cos_ref[:, rows], sin_ref[:, rows]
            for h in range(heads):
                cols = head(h)
                t = dqt[cols, rows].astype(jnp.bfloat16).astype(jnp.float32)
                lo, hi = t[:half], t[half:]
                out_ref[rows, cols] = jnp.concatenate([lo * cos + hi * sin, hi * cos - lo * sin], axis=0).T.astype(jnp.bfloat16)
            return c
        lax.fori_loop(0, nq, fin, 0)
        for cp in carry_over:
            cp.wait()


def flash_bwd(q, o, d, k, kt, v, lse, cos_t, sin_t, gs, cid, bq=512, bk=512):
    seq, width = q.shape
    heads = width // HEAD_DIM
    an = pl.BlockSpec(memory_space=pl.ANY)
    return pl.pallas_call(
        functools.partial(bwd_kernel, bq, bk),
        grid=(seq // bk,),
        in_specs=[pl.BlockSpec((seq, width), whole), pl.BlockSpec((seq, width), whole), pl.BlockSpec((seq, width), whole),
                  pl.BlockSpec((bk, HEAD_DIM), by_rows), pl.BlockSpec((HEAD_DIM, bk), by_cols),
                  pl.BlockSpec((bk, HEAD_DIM), by_rows),
                  pl.BlockSpec((heads, seq), whole), pl.BlockSpec(cos_t.shape, whole), pl.BlockSpec(cos_t.shape, whole)] + [an] * 3,
        out_specs=[pl.BlockSpec((seq, width + 2 * HEAD_DIM), whole)] + [an] * 3,
        out_shape=[jax.ShapeDtypeStruct((seq, width + 2 * HEAD_DIM), jnp.bfloat16)] + halve_shapes(gs, 3),
        scratch_shapes=[pltpu.VMEM((width, seq), jnp.float32), pltpu.VMEM((bk, HEAD_DIM), jnp.float32), pltpu.VMEM((bk, HEAD_DIM), jnp.float32),
                        pltpu.VMEM((heads, seq), jnp.float32), pltpu.SemaphoreType.DMA((3,)), pltpu.SemaphoreType.DMA((3,))],
        cost_estimate=pl.CostEstimate(flops=5 * seq * seq * width * 2 // 2, bytes_accessed=16 << 20, transcendentals=seq * seq),
        compiler_params=comm_params(cid, vmem_limit_bytes=58 << 20),
        name="flash_bwd",
    )(q, o, d, k, kt, v, lse, cos_t, sin_t, *gs)


class PlaneGather:
    N = 13

    def __init__(self, here, wires, src, out, local_sem):
        h = src.shape[0] // 2
        A, B = slice(h), slice(h, None)
        s = here.s
        sx, sy, sc = here.peer('x')[1], here.peer('y')[1], here.peer('c')[1]
        sd = here.s + 2 - 4 * here.x + 4 - 8 * here.y
        nx, ny, nc = here.peer('x'), here.peer('y'), here.peer('c')
        self.local = pltpu.make_async_copy(src, out.at[s], local_sem)
        mk = wires.copy
        self.x1 = {k: mk(src.at[r], out.at[s, r], nx) for k, r in (('A', A), ('B', B))}
        self.y1 = {k: mk(src.at[r], out.at[s, r], ny) for k, r in (('B', B), ('A', A))}
        self.c1 = mk(src, out.at[s], nc)
        self.fy = mk(out.at[sx, A], out.at[sx, A], ny)
        self.fx = mk(out.at[sy, B], out.at[sy, B], nx)
        self.cc = {}
        for name, idx in (('x', sx), ('y', sy), ('d', sd)):
            for k, r in (('A', A), ('B', B)):
                self.cc[name + k] = mk(out.at[idx, r], out.at[idx, r], nc)

    def start_first(self):
        self.x1['A'].start()
        self.y1['B'].start()
        self.c1.start()
        self.local.start()

    def start_second(self):
        self.x1['B'].start()
        self.y1['A'].start()

    def relay(self):
        self.x1['A'].wait_recv()
        self.fy.start()
        self.cc['xA'].start()
        self.y1['B'].wait_recv()
        self.fx.start()
        self.cc['yB'].start()
        self.x1['B'].wait_recv()
        self.cc['xB'].start()
        self.y1['A'].wait_recv()
        self.cc['yA'].start()

    def finish(self):
        self.fy.wait_recv()
        self.cc['dA'].start()
        self.fx.wait_recv()
        self.cc['dB'].start()
        self.c1.wait_recv()
        for k in self.cc:
            self.cc[k].wait_recv()
        for c in (*self.x1.values(), *self.y1.values(), self.c1, self.fy, self.fx, *self.cc.values()):
            c.wait_send()
        self.local.wait()


def dh_kernel(src, out, send_sem, recv_sem, local_sem):
    here = Spot()
    greet([here.peer(d) for d in 'xyc'])
    g = PlaneGather(here, Wires(send_sem, recv_sem), src, out, local_sem)
    g.start_first()
    g.start_second()
    g.relay()
    g.finish()


def gather_dh(src, cid):
    rows, cols = src.shape
    n = PlaneGather.N
    return pl.pallas_call(
        dh_kernel, in_specs=[pl.BlockSpec(memory_space=pltpu.VMEM)], out_specs=pl.BlockSpec(memory_space=pl.ANY),
        out_shape=jax.ShapeDtypeStruct((8, rows, cols), src.dtype),
        scratch_shapes=[pltpu.SemaphoreType.DMA((n,)), pltpu.SemaphoreType.DMA((n,)), pltpu.SemaphoreType.DMA],
        cost_estimate=busy(40), compiler_params=comm_params(cid), name="gather_dh",
    )(src)


def mlp_kernel(u_ref, d_ref, w1_ref, w3_ref, w2_ref, wg, y_ref, dx_ref, g1_ref, g3_ref, g2_ref, og, ut, send_sem, recv_sem, local_sem):
    j = pl.program_id(0)
    last = pl.num_programs(0) - 1
    here = Spot()
    c = here.c
    wires = Wires(send_sem, recv_sem)
    loc = pltpu.make_async_copy(wg, og.at[here.region('') + (c,)], local_sem)
    jobs = [(og, (c, slice(None), slice(off, off + n)), order) for (off, n), order in zip(col_chunks(wg.shape[1], 3), ORDERS)]
    cube = CubeGather(here, wires, jobs)
    post = wires.copy(og.at[:, :, :, c], og.at[:, :, :, c], here.peer('c'))
    toks = u_ref.shape[0]

    @pl.when(j == 0)
    def _():
        greet(cube_targets(here))
        loc.start()
        loc.wait()
        cube.start(0)
        y_ref[...] = jnp.zeros_like(y_ref)
        dx_ref[...] = jnp.zeros_like(dx_ref)

        def flip(i, carry):
            part = pl.ds(pl.multiple_of(i * 128, 128), 128)
            ut[:, part] = u_ref[part, :].astype(jnp.float32).T.astype(jnp.bfloat16)
            return carry
        lax.fori_loop(0, toks // 128, flip, 0)

    @pl.when(j == 1)
    def _():
        cube.start(1)

    @pl.when(j == 3)
    def _():
        cube.start(2)

    @pl.when(j == last)
    def _():
        cube.arrive()
        post.start()

    f32 = jnp.float32
    u, d = u_ref[...], d_ref[...]
    w1, w3, w2 = w1_ref[...], w3_ref[...], w2_ref[...]
    gate = jnp.dot(u, w1, preferred_element_type=f32)
    up = jnp.dot(u, w3, preferred_element_type=f32)
    act = lax.dot_general(d, w2, NT, preferred_element_type=f32)
    sig = jax.nn.sigmoid(gate)
    silu = gate * sig
    z = (silu * up).astype(jnp.bfloat16)
    da = (act * up * sig * (1.0 + gate * (1.0 - sig))).astype(jnp.bfloat16)
    dc = (act * silu).astype(jnp.bfloat16)
    y_ref[...] += jnp.dot(z, w2, preferred_element_type=f32)
    dx_ref[...] += lax.dot_general(da, w1, NT, preferred_element_type=f32) + lax.dot_general(dc, w3, NT, preferred_element_type=f32)
    g1_ref[...] = jnp.dot(ut[...], da, preferred_element_type=f32)
    g3_ref[...] = jnp.dot(ut[...], dc, preferred_element_type=f32)
    g2_ref[...] = lax.dot_general(z, d, (((0,), (0,)), ((), ())), preferred_element_type=f32)

    @pl.when(j == last)
    def _():
        post.wait()
        cube.drain()


def mlp(u, d, w1, w3, w2, wg, cid, bh=256):
    toks, dim = u.shape
    half = w1.shape[1]
    f32 = jnp.float32
    vm = pl.BlockSpec(memory_space=pltpu.VMEM)
    an = pl.BlockSpec(memory_space=pl.ANY)
    return pl.pallas_call(
        mlp_kernel, grid=(half // bh,),
        in_specs=[vm, vm, pl.BlockSpec((dim, bh), by_cols), pl.BlockSpec((dim, bh), by_cols), pl.BlockSpec((bh, dim), by_rows), vm],
        out_specs=[pl.BlockSpec((toks, dim), whole), pl.BlockSpec((toks, dim), whole), pl.BlockSpec((dim, bh), by_cols), pl.BlockSpec((dim, bh), by_cols),
                   pl.BlockSpec((bh, dim), by_rows), an],
        out_shape=[jax.ShapeDtypeStruct((toks, dim), f32), jax.ShapeDtypeStruct((toks, dim), f32), jax.ShapeDtypeStruct((dim, half), f32),
                   jax.ShapeDtypeStruct((dim, half), f32), jax.ShapeDtypeStruct((half, dim), f32),
                   jax.ShapeDtypeStruct((2, 2, 2, 2, *wg.shape), wg.dtype)],
        scratch_shapes=[pltpu.VMEM((dim, toks), jnp.bfloat16), pltpu.SemaphoreType.DMA((19,)), pltpu.SemaphoreType.DMA((19,)), pltpu.SemaphoreType.DMA],
        cost_estimate=pl.CostEstimate(flops=18 * toks * dim * half, bytes_accessed=48 << 20, transcendentals=toks * half),
        compiler_params=comm_params(cid, vmem_limit_bytes=58 << 20), name="mlp",
    )(u, d, w1, w3, w2, wg)


def entry_kernel(x_ref, w_ref, meta_ref, pos_ref, xa, wa, ma, pa, send_sem, recv_sem, local_sem):
    here = Spot()
    z, s = here.z, here.s
    peers = here.others()
    nz = here.peer('z')
    greet(peers + [nz])
    wires = Wires(send_sem, recv_sem)
    first = []
    for t in peers:
        for src, dst in ((w_ref.at[t[1]], wa.at[z, s]), (meta_ref, ma.at[z, s]), (pos_ref, pa.at[s])):
            first.append(wires.copy(src, dst, t))
    locals_ = [pltpu.make_async_copy(w_ref.at[s], wa.at[z, s], local_sem.at[1]),
               pltpu.make_async_copy(meta_ref, ma.at[z, s], local_sem.at[2]),
               pltpu.make_async_copy(pos_ref, pa.at[s], local_sem.at[3])]
    g = PlaneGather(here, wires, x_ref, xa, local_sem.at[0])
    cross = [wires.copy(wa.at[z], wa.at[z], nz), wires.copy(ma.at[z], ma.at[z], nz)]
    for c in first:
        c.start()
    for c in locals_:
        c.start()
    g.start_first()
    g.start_second()
    for c in first:
        c.wait_recv()
    for c in locals_:
        c.wait()
    for c in cross:
        c.start()
    g.relay()
    g.finish()
    for c in cross:
        c.wait()
    for c in first:
        c.wait_send()


def entry(x, w, meta, pos, cid):
    n = PlaneGather.N + 21 + 2
    vm = pl.BlockSpec(memory_space=pltpu.VMEM)
    an = pl.BlockSpec(memory_space=pl.ANY)
    return pl.pallas_call(
        entry_kernel,
        in_specs=[vm] * 4, out_specs=[an] * 4,
        out_shape=[jax.ShapeDtypeStruct((8, *x.shape), x.dtype), jax.ShapeDtypeStruct((2, 8, *w.shape[1:]), w.dtype),
                   jax.ShapeDtypeStruct((2, 8, *meta.shape), meta.dtype), jax.ShapeDtypeStruct((8, *pos.shape), pos.dtype)],
        scratch_shapes=[pltpu.SemaphoreType.DMA((n,)), pltpu.SemaphoreType.DMA((n,)), pltpu.SemaphoreType.DMA((4,))],
        cost_estimate=busy(45), compiler_params=comm_params(cid),
        name="entry",
    )(x, w, meta, pos)


def regroup_kernel(n, *refs):
    src, gs, out, rs = refs[0], refs[1:1 + n], refs[1 + n], refs[2 + n:2 + 2 * n]
    send_sem, recv_sem, local_sem, stage = refs[2 + 2 * n:]
    here = Spot()
    s = here.s
    rows, width = out.shape[0], src.shape[1]
    peers = here.others()
    greet(peers + ([here.peer('z')] if n else []))
    wires = Wires(send_sem, recv_sem)
    piece = lambda i: pl.ds(pl.multiple_of(i * rows, rows), rows)
    mine = pl.ds(pl.multiple_of(s * width, width), width)
    cs = [wires.copy(src.at[piece(t[1])], out.at[:, mine], t) for t in peers]
    cs += [wires.copy(g, r, here.peer(order[1])) for g, r, order in zip(gs[:3], rs, ORDERS)]
    cs += [wires.copy(g.at[1 - here.z], r, here.peer('z')) for g, r in zip(gs[3:], rs[3:])]
    for c in cs:
        c.start()
    a = pltpu.make_async_copy(src.at[piece(s)], stage, local_sem.at[0])
    a.start()
    a.wait()
    b = pltpu.make_async_copy(stage, out.at[:, mine], local_sem.at[1])
    b.start()
    b.wait()
    for c in cs:
        c.wait()


def regroup(src, gs, cid, name):
    seq, width = src.shape
    rows, n = seq // 8, len(gs)
    an = pl.BlockSpec(memory_space=pl.ANY)
    back = [jax.ShapeDtypeStruct(g.shape if i < 3 else g.shape[1:], g.dtype) for i, g in enumerate(gs)]
    out = pl.pallas_call(
        functools.partial(regroup_kernel, n), in_specs=[an] * (1 + n), out_specs=[an] * (1 + n),
        out_shape=[jax.ShapeDtypeStruct((rows, 8 * width), src.dtype)] + back,
        scratch_shapes=[pltpu.SemaphoreType.DMA((7 + n,)), pltpu.SemaphoreType.DMA((7 + n,)), pltpu.SemaphoreType.DMA((2,)), pltpu.VMEM((rows, width), src.dtype)],
        cost_estimate=busy(70 if n else 25), compiler_params=comm_params(cid), name=name,
    )(src, *gs)
    return out[0], out[1:]


def back_kernel(t_ref, w_ref, x_ref, gain_ref, res_ref, a, g1, g3, g2, dx_ref, gg_ref, oa, r1, r3, r2, acc, send_sem, recv_sem, local_sem):
    j = pl.program_id(0)
    bn = w_ref.shape[0]
    here = Spot()
    peers = here.others()
    wires = Wires(send_sem, recv_sem)
    s = here.s
    cs = [wires.copy(g, r, here.peer(order[0])) for g, r, order in zip((g1, g3, g2), (r1, r3, r2), ORDERS)]
    cs += [wires.copy(a.at[t[1]], oa.at[s], t) for t in peers]
    loc = pltpu.make_async_copy(a.at[s], oa.at[s], local_sem)

    @pl.when(j == 0)
    def _():
        greet(peers + [here.peer('z')])
        for c in cs:
            c.start()
        loc.start()

    acc[:, pl.ds(pl.multiple_of(j * bn, bn), bn)] = lax.dot_general(t_ref[...], w_ref[...], NT, preferred_element_type=jnp.float32)

    @pl.when(j == pl.num_programs(0) - 1)
    def _():
        gg_ref[...] = jnp.zeros_like(gg_ref)
        gain = gain_ref[0:1, :].astype(jnp.float32)

        def rows_of(i, carry):
            part = pl.ds(pl.multiple_of(i * HEAD_DIM, HEAD_DIM), HEAD_DIM)
            x = x_ref[part, :].astype(jnp.float32)
            inv = lax.rsqrt(jnp.mean(x * x, axis=-1, keepdims=True) + NORM_EPS)
            normed = x * inv
            d_out = acc[part, :]
            d_normed = d_out * gain
            gg_ref[...] += jnp.sum(d_out * normed, axis=0, keepdims=True)
            grad_in = inv * (d_normed - normed * jnp.mean(d_normed * normed, axis=-1, keepdims=True))
            dx_ref[part, :] = (res_ref[part, :] + grad_in).astype(jnp.bfloat16)
            return carry
        lax.fori_loop(0, x_ref.shape[0] // HEAD_DIM, rows_of, 0)
        for c in cs:
            c.wait()
        loc.wait()


def back_project(t, w, x, gain, res, a, gs, cid, bn=256):
    toks, inner = t.shape
    dim = w.shape[0]
    vm = pl.BlockSpec(memory_space=pltpu.VMEM)
    an = pl.BlockSpec(memory_space=pl.ANY)
    out = pl.pallas_call(
        back_kernel, grid=(dim // bn,),
        in_specs=[vm, pl.BlockSpec((bn, inner), by_rows)] + [vm] * 4 + [an] * 3,
        out_specs=[pl.BlockSpec((toks, dim), whole), pl.BlockSpec((1, dim), whole)] + [an] * 4,
        out_shape=[jax.ShapeDtypeStruct((toks, dim), jnp.bfloat16), jax.ShapeDtypeStruct((1, dim), jnp.float32), jax.ShapeDtypeStruct(a.shape, a.dtype)]
        + [jax.ShapeDtypeStruct(g.shape, g.dtype) for g in gs],
        scratch_shapes=[pltpu.VMEM((toks, dim), jnp.float32), pltpu.SemaphoreType.DMA((10,)), pltpu.SemaphoreType.DMA((10,)), pltpu.SemaphoreType.DMA],
        cost_estimate=busy(35), compiler_params=comm_params(cid, vmem_limit_bytes=48 << 20), name="back_project",
    )(t, w, x, gain, res, a, *gs)
    return out[0], out[1], out[2], out[3:]


def last_kernel(b, p1, p3, ob, q1, q3, send_sem, recv_sem, local_sem):
    here = Spot()
    peers = here.others()
    greet(peers)
    wires = Wires(send_sem, recv_sem)
    s, nc = here.s, here.peer('c')
    cs = [wires.copy(p.at[1 - here.c], q, nc) for p, q in ((p1, q1), (p3, q3))]
    cs += [wires.copy(b.at[t[1]], ob.at[s], t) for t in peers]
    loc = pltpu.make_async_copy(b.at[s], ob.at[s], local_sem)
    for c in cs + [loc]:
        c.start()
    for c in cs + [loc]:
        c.wait()


def last_exchange(b, p1, p3, cid):
    vm = pl.BlockSpec(memory_space=pltpu.VMEM)
    return pl.pallas_call(
        last_kernel, in_specs=[vm] * 3, out_specs=[vm] * 3,
        out_shape=[jax.ShapeDtypeStruct(b.shape, b.dtype)] + [jax.ShapeDtypeStruct(p.shape[1:], p.dtype) for p in (p1, p3)],
        scratch_shapes=[pltpu.SemaphoreType.DMA((9,)), pltpu.SemaphoreType.DMA((9,)), pltpu.SemaphoreType.DMA],
        cost_estimate=busy(5), compiler_params=comm_params(cid), name="last_exchange",
    )(b, p1, p3)


def dot_tokens(left_op, right_op):
    return lax.dot_general(left_op, right_op, (((0,), (0,)), ((), ())), preferred_element_type=jnp.float32)


def dot_back(left_op, weight):
    return lax.dot_general(left_op, weight, (((1,), (1,)), ((), ())), preferred_element_type=jnp.float32)


def dot_on(left_op, weight):
    return jnp.dot(left_op, weight, preferred_element_type=jnp.float32)


def swap_core(t):
    return lax.ppermute(t, 'sp', [(i, i ^ 1) for i in range(8)])


def swap_z(t):
    return lax.ppermute(t, 'dp', [(0, 1), (1, 0)])


def split_cols(w):
    rows, cols = w.shape
    return w.reshape(rows, 8, 2, cols // 16).transpose(2, 0, 1, 3).reshape(2, rows, cols // 2)


def join_cols(mine, other, c):
    rows, half = mine.shape
    m, o = mine.reshape(rows, 8, 1, half // 8), other.reshape(rows, 8, 1, half // 8)
    first = jnp.where(c == 0, m, o)
    second = jnp.where(c == 0, o, m)
    return jnp.concatenate([first, second], axis=2).reshape(rows, 2 * half)


def layer_step(hidden, positions, grad_out, gain_attn, gain_mlp, w_query, w_key, w_value, w_out, w_gate, w_up, w_down):
    tokens = hidden[0]
    d_layer = grad_out[0]
    tok, dim = tokens.shape
    here = Spot()
    z, s, c = here.z, here.s, here.c
    rows = w_query.shape[0]
    grp_q = w_query.shape[1] // 8
    grp_k = w_key.shape[1] // 8
    grp = grp_q + 2 * grp_k
    seq = 8 * tok

    w_grp = jnp.concatenate([w_query.reshape(rows, 8, grp_q), w_key.reshape(rows, 8, grp_k), w_value.reshape(rows, 8, grp_k)], axis=2)
    w_flat = w_grp.reshape(rows, 8 * grp)
    pad = HEAD_DIM - gain_attn.shape[0]
    meta = jnp.pad(jnp.stack([jnp.pad(gain_attn, (0, pad)), jnp.pad(gain_mlp, (0, pad))]), ((0, 14), (0, 0)))
    x_all, w_own, meta_all, pos_all = entry(tokens, w_grp.transpose(1, 0, 2), meta, positions[0].reshape(-1, 128), 1)
    x_all = x_all.reshape(seq, dim)
    w_own = w_own.reshape(dim, grp)
    gain1 = meta_all[:, :, 0, :rows].reshape(dim)
    gain2 = meta_all[:, :, 1, :rows].reshape(dim)
    cos_t, sin_t = rope_tables(pos_all.reshape(seq))

    gain1_rows = jnp.broadcast_to(gain1[None], (16, dim))
    u_all, q_own, k_own, v_own, k_t, v_t = project(x_all, gain1_rows, w_own, cos_t, sin_t)
    o_own, o_t, lse, w1, w3, w2, wo = flash_fwd(q_own, k_own, v_t, (split_cols(w_gate), split_cols(w_up), w_down, w_out), 2)
    ffn_half = w1.shape[-1]
    w1, w3 = w1.reshape(dim, ffn_half), w3.reshape(dim, ffn_half)
    w2 = w2.reshape(ffn_half, dim)
    wo = wo.reshape(-1, dim)
    attn_out, _ = regroup(o_own, (), 3, 'regroup_o')
    residual = (tokens.astype(jnp.float32) + dot_on(attn_out, wo)).astype(jnp.bfloat16)
    u_mlp, normed2, inv_rms2 = rms_norm(residual, gain2)
    u_pair = jnp.concatenate([u_mlp, swap_core(u_mlp)], axis=0)
    d_pair = jnp.concatenate([d_layer, swap_core(d_layer)], axis=0)
    y_part, d_part, g1, g3, g2, wg = mlp(u_pair, d_pair, w1, w3, w2, w_flat, 7)
    layer_out = (residual.astype(jnp.float32) + (y_part[:tok] + swap_core(y_part[tok:]))).astype(jnp.bfloat16)

    d_umlp = d_part[:tok] + swap_core(d_part[tok:])
    d_res_norm, d_gain2 = rms_norm_grad(d_umlp, normed2, inv_rms2, gain2)
    d_resid = d_layer.astype(jnp.float32) + d_res_norm
    d_resid_bf = d_resid.astype(jnp.bfloat16)
    g1 = g1.reshape(2, 2, 2, dim // 8, ffn_half)
    g3 = g3.reshape(2, 2, 2, dim // 8, ffn_half)
    g2 = g2.reshape(2, 2, 2, ffn_half // 8, dim)

    dh_all = gather_dh(d_resid_bf, 4).reshape(seq, dim)
    wg = wg.reshape(dim, 8 * grp)
    wo_own = lax.dynamic_slice_in_dim(wo, s * grp_q, grp_q, 0)
    d_own = dot_back(dh_all, wo_own).astype(jnp.bfloat16)
    go = dot_on(o_t, dh_all).reshape(2, grp_q // 2, dim)
    dqkv_pre, *got = flash_bwd(q_own, o_own, d_own, k_own, k_t, v_own, lse, cos_t, sin_t, (g1, g3, g2), 6)
    gq = dot_tokens(u_all, dqkv_pre).reshape(2, dim // 2, grp)
    terms = after(here, [[g1], [g3], [g2]], got, 3)
    dqkv_tok, (*got, gq_got, go_got) = regroup(dqkv_pre, (*to_send(here, terms, 2), gq, go), 5, 'regroup_dqkv')
    grad_w_out = lax.ppermute(pick(go, z) + go_got, ALL_AXES, [(zz * 8 + ss, 2 * ss + zz) for zz in range(2) for ss in range(8)])
    terms = after(here, terms, got, 2)
    gq_mine = pick(gq, z) + gq_got
    grad_hidden, d_gain1, got_q, got = back_project(dqkv_tok, wg, tokens, gain1_rows, d_resid, gq_mine.reshape(8, rows, grp), to_send(here, terms, 1), 8)
    m1, m3, grad_w_down = [total(ts) for ts in after(here, terms, got, 1)]

    gains = jnp.concatenate([d_gain1.reshape(2, 8, rows), d_gain2.reshape(2, 8, rows)], axis=2)
    gains_mine = pick(gains, z) + swap_z(pick(gains, 1 - z))
    gains_mine = jnp.broadcast_to(gains_mine[:, None, :], (8, 8, 2 * rows))
    pair1, pair3 = m1.reshape(2, rows, ffn_half), m3.reshape(2, rows, ffn_half)
    got_g, other1, other3 = last_exchange(gains_mine, pair1, pair3, 10)
    got_q = got_q.transpose(1, 0, 2)
    grad_w_query = got_q[:, :, :grp_q].reshape(rows, 8 * grp_q)
    grad_w_key = got_q[:, :, grp_q:grp_q + grp_k].reshape(rows, 8 * grp_k)
    grad_w_value = got_q[:, :, grp_q + grp_k:].reshape(rows, 8 * grp_k)
    grad_gains = jnp.sum(got_g[:, 0, :], axis=0)
    grad_gain_attn, grad_gain_mlp = grad_gains[:rows], grad_gains[rows:]

    grad_w_gate = join_cols(pick(pair1, c), other1, c)
    grad_w_up = join_cols(pick(pair3, c), other3, c)
    return (layer_out[None], grad_hidden[None], grad_gain_attn, grad_gain_mlp, grad_w_query, grad_w_key, grad_w_value, grad_w_out, grad_w_gate, grad_w_up, grad_w_down)


def solution(mesh):
    act_spec = P('dp', 'sp', None)
    pos_spec = P('dp', 'sp')
    vec_spec = P(ALL_AXES)
    mat_spec = P(ALL_AXES, None)
    in_specs = (act_spec, pos_spec, act_spec, vec_spec, vec_spec) + (mat_spec,) * 7
    out_specs = (act_spec, act_spec, vec_spec, vec_spec) + (mat_spec,) * 7
    return jax.shard_map(layer_step, mesh=mesh, in_specs=in_specs, out_specs=out_specs, check_vma=False)
```

```python
import functools
import math

import jax
import jax.numpy as jnp
from jax import lax
from jax.experimental import pallas as pl
from jax.experimental.pallas import tpu as pltpu
from jax.sharding import PartitionSpec as P

HEAD_DIM = 128
ROPE_BASE = 10000.0
NORM_EPS = 1e-5
ATTN_SCALE = HEAD_DIM ** -0.5
ALL_AXES = ('dp', 'sp')


def rope_tables(pos_ids):
    inv_freq = ROPE_BASE ** (-(jnp.arange(HEAD_DIM // 2, dtype=jnp.float32) * (2.0 / HEAD_DIM)))
    angles = pos_ids.astype(jnp.float32)[None, :] * inv_freq[:, None]
    return jnp.cos(angles), jnp.sin(angles)


def rms_norm(values, gain_vec):
    vals32 = values.astype(jnp.float32)
    inv_rms = lax.rsqrt(jnp.mean(vals32 * vals32, axis=-1, keepdims=True) + NORM_EPS)
    normed = vals32 * inv_rms
    return (normed * gain_vec.astype(jnp.float32)).astype(jnp.bfloat16), normed, inv_rms


def rms_norm_grad(d_out, normed, inv_rms, gain_vec):
    d_normed = d_out * gain_vec.astype(jnp.float32)
    grad_gain = jnp.sum(d_out * normed, axis=0)
    grad_in = inv_rms * (d_normed - normed * jnp.mean(d_normed * normed, axis=-1, keepdims=True))
    return grad_in, grad_gain


MESH = pl.DeviceIdType.MESH


def by_rows(i):
    return i, 0


def by_cols(i):
    return 0, i


def whole(i):
    return 0, 0


def head(h):
    return slice(h * HEAD_DIM, (h + 1) * HEAD_DIM)


def pick(t, i):
    return lax.dynamic_index_in_dim(t, i, 0, False)


ORDERS = ('xyz', 'yzx', 'zxy')


class Spot:
    def __init__(self):
        self.z = lax.axis_index('dp')
        self.s = lax.axis_index('sp')
        self.y = self.s // 4
        self.x = (self.s // 2) % 2
        self.c = self.s % 2
        self.bits = {'z': self.z, 'y': self.y, 'x': self.x}

    def peer(self, dim):
        if dim == 'z':
            return (1 - self.z, self.s)
        if dim == 'y':
            return (self.z, self.s + 4 - 8 * self.y)
        if dim == 'x':
            return (self.z, self.s + 2 - 4 * self.x)
        return (self.z, self.s + 1 - 2 * self.c)

    def others(self):
        return [(self.z, (self.s + t) % 8) for t in range(1, 8)]

    def region(self, freed, flipped=''):
        return tuple(slice(None) if d in freed else (1 - self.bits[d] if d in flipped else self.bits[d]) for d in 'zyx')


def greet(targets):
    bar = pltpu.get_barrier_semaphore()
    for t in targets:
        pl.semaphore_signal(bar, inc=1, device_id=t, device_id_type=MESH)
    pl.semaphore_wait(bar, len(targets))


class Wires:
    def __init__(self, send_sem, recv_sem):
        self.send_sem, self.recv_sem, self.n = send_sem, recv_sem, 0

    def copy(self, src, dst, target):
        i = self.n
        self.n += 1
        return pltpu.make_async_remote_copy(src_ref=src, dst_ref=dst, send_sem=self.send_sem.at[i], recv_sem=self.recv_sem.at[i], device_id=target, device_id_type=MESH)


class CubeGather:
    def __init__(self, here, wires, jobs):
        firsts, seconds, thirds = [], [], []
        for out, suffix, (a, b, e) in jobs:
            def mk(freed, flipped, d):
                reg = here.region(freed, flipped) + suffix
                return wires.copy(out.at[reg], out.at[reg], here.peer(d))
            firsts.append([mk('', '', d) for d in (a, b, e)])
            seconds.append([mk('', a, d) for d in (b, e)])
            thirds.append(mk(a, b, e))
        self.stages = [[f[i] for i in range(3) for f in firsts], [t[i] for i in range(2) for t in seconds], thirds]
        self.need = [[f[0] for f in firsts], [f[1] for f in firsts] + [t[0] for t in seconds]]
        self.rest = [[f[2], t[1], e] for f, t, e in zip(firsts, seconds, thirds)]

    def start(self, i):
        for c in self.need[i - 1] if i else ():
            c.wait_recv()
        for c in self.stages[i]:
            c.start()

    def arrive(self, lo=0, hi=None):
        for job in self.rest[lo:hi]:
            for c in job:
                c.wait_recv()

    def drain(self):
        for st in self.stages:
            for c in st:
                c.wait_send()


def col_chunks(cols, parts):
    n, out, off = cols // 128, [], 0
    for p in range(parts, 0, -1):
        w = -(-n // p)
        out.append((off, w * 128))
        off += w * 128
        n -= w
    return out


def cube_targets(here):
    return [here.peer(d) for d in 'xyzc']


def comm_params(cid, **kw):
    return pltpu.CompilerParams(collective_id=cid, has_side_effects=True, **kw)


def busy(us):
    return pl.CostEstimate(flops=int(us * 1e8), bytes_accessed=1 << 20, transcendentals=0)


NW = 2 + 6 * 6 + 1


class WeightGather:
    def __init__(self, here, wires, local_sem, ins, outs):
        w1, w3, w2, wo = ins
        o1, o3, o2, oo = outs
        c, zyx, nc = here.c, here.region(''), here.peer('c')
        self.pre = [wires.copy(w1.at[1 - c], o1.at[zyx + (c,)], nc), wires.copy(w3.at[1 - c], o3.at[zyx + (c,)], nc)]
        self.loc = [pltpu.make_async_copy(w1.at[c], o1.at[zyx + (c,)], local_sem.at[0]),
                    pltpu.make_async_copy(w3.at[c], o3.at[zyx + (c,)], local_sem.at[1]),
                    pltpu.make_async_copy(w2, o2.at[zyx], local_sem.at[2]),
                    pltpu.make_async_copy(wo, oo.at[zyx + (c,)], local_sem.at[3])]
        jobs = [(oo, (c, slice(None), slice(off, off + n)), order) for (off, n), order in zip(col_chunks(wo.shape[1], 3), ORDERS)]
        jobs += [(o1, (), ORDERS[0]), (o3, (), ORDERS[1]), (o2, (), ORDERS[2])]
        self.cube = CubeGather(here, wires, jobs)
        self.post = wires.copy(oo.at[:, :, :, c], oo.at[:, :, :, c], nc)

    def begin(self):
        for c in self.pre + self.loc:
            c.start()
        for c in self.loc:
            c.wait()
        for c in self.pre:
            c.wait()
        self.cube.start(0)

    def end(self):
        self.cube.arrive(0, 3)
        self.post.start()
        self.cube.arrive(3)
        self.post.wait()
        self.cube.drain()


def gathered(ws):
    return [jax.ShapeDtypeStruct((2, 2, 2, *w.shape), w.dtype) if k < 3 else jax.ShapeDtypeStruct((2, 2, 2, 2, *w.shape), w.dtype) for k, w in enumerate(ws)]


def halve_copies(here, wires, nd, ins, outs):
    cs = []
    for i, (a, o) in enumerate(zip(ins, outs)):
        order = ORDERS[i % 3]
        d = order[nd - 1]
        reg = tuple(1 - here.bits[d] if e == d else slice(None) for e in 'zyx' if e in order[:nd])
        cs.append(wires.copy(a.at[reg], o, here.peer(d)))
    return cs


def halve_shapes(arrs, nd):
    return [jax.ShapeDtypeStruct((*((2,) * (nd - 1)), *a.shape[nd:]), a.dtype) for a in arrs]


def part_of(here, t, order, nd, flip):
    live = [d for d in 'zyx' if d in order[:nd]]
    d = order[nd - 1]
    bit = here.bits[d]
    return lax.dynamic_index_in_dim(t, 1 - bit if flip else bit, live.index(d), False)


def total(terms):
    out = terms[0]
    for t in terms[1:]:
        out = out + t
    return out


def to_send(here, terms, nd):
    return [total([part_of(here, t, ORDERS[i % 3], nd, True) for t in ts]) for i, ts in enumerate(terms)]


def after(here, terms, got, nd):
    return [[part_of(here, t, ORDERS[i % 3], nd, False) for t in ts] + [r] for i, (ts, r) in enumerate(zip(terms, got))]


def wide_tables(cos_t, sin_t):
    return jnp.concatenate([cos_t, cos_t], axis=0).T, jnp.concatenate([-sin_t, sin_t], axis=0).T


def proj_kernel(nrot, x_ref, g_ref, w_ref, cos_ref, sin_ref, u_ref, q_ref, k_ref, v_ref, kt_ref, vt_ref):
    x = x_ref[...].astype(jnp.float32)
    inv = lax.rsqrt(jnp.mean(x * x, axis=-1, keepdims=True) + NORM_EPS)
    u = (x * inv * g_ref[0:1, :].astype(jnp.float32)).astype(jnp.bfloat16)
    u_ref[...] = u
    cos, sin = wide_tables(cos_ref[...], sin_ref[...])
    full = jnp.dot(u, w_ref[...], preferred_element_type=jnp.float32)
    for h in range(nrot + 2):
        t = full[:, head(h)]
        if h <= nrot:
            t = t * cos + pltpu.roll(t, HEAD_DIM // 2, 1) * sin
        if h < nrot:
            q_ref[:, head(h)] = t.astype(jnp.bfloat16)
        else:
            n_ref, t_ref = (k_ref, kt_ref) if h == nrot else (v_ref, vt_ref)
            n_ref[...] = t.astype(jnp.bfloat16)
            t_ref[...] = t.T.astype(jnp.bfloat16)


def project(x, gain, w, cos_t, sin_t, bt=512):
    seq, dim = x.shape
    grp = w.shape[1]
    nq = grp // HEAD_DIM - 2
    bf = jnp.bfloat16
    return pl.pallas_call(
        functools.partial(proj_kernel, nq), grid=(seq // bt,),
        in_specs=[pl.BlockSpec((bt, dim), by_rows), pl.BlockSpec((16, dim), whole), pl.BlockSpec((dim, grp), whole),
                  pl.BlockSpec((cos_t.shape[0], bt), by_cols), pl.BlockSpec((cos_t.shape[0], bt), by_cols)],
        out_specs=[pl.BlockSpec((bt, dim), by_rows), pl.BlockSpec((bt, nq * HEAD_DIM), by_rows), pl.BlockSpec((bt, HEAD_DIM), by_rows), pl.BlockSpec((bt, HEAD_DIM), by_rows),
                   pl.BlockSpec((HEAD_DIM, bt), by_cols), pl.BlockSpec((HEAD_DIM, bt), by_cols)],
        out_shape=[jax.ShapeDtypeStruct((seq, dim), bf), jax.ShapeDtypeStruct((seq, nq * HEAD_DIM), bf), jax.ShapeDtypeStruct((seq, HEAD_DIM), bf),
                   jax.ShapeDtypeStruct((seq, HEAD_DIM), bf), jax.ShapeDtypeStruct((HEAD_DIM, seq), bf), jax.ShapeDtypeStruct((HEAD_DIM, seq), bf)],
        cost_estimate=pl.CostEstimate(flops=2 * seq * dim * grp, bytes_accessed=32 << 20, transcendentals=0),
        compiler_params=pltpu.CompilerParams(vmem_limit_bytes=62 << 20), name="project",
    )(x, gain, w, cos_t, sin_t)


LOG2E = math.log2(math.e)
SCALE2 = ATTN_SCALE * LOG2E
NT = (((1,), (1,)), ((), ()))
NN = (((1,), (0,)), ((), ()))
BIG = -1e30


def fwd_kernel(bq, bk, q_ref, k_ref, vt_ref, w1, w3, w2, wo, o_ref, ot_ref, lse_ref, o1, o3, o2, oo, send_sem, recv_sem, local_sem):
    i = pl.program_id(0)
    last = pl.num_programs(0) - 1
    here = Spot()
    carry_over = WeightGather(here, Wires(send_sem, recv_sem), local_sem, (w1, w3, w2, wo), (o1, o3, o2, oo))

    @pl.when(i == 0)
    def _():
        greet(cube_targets(here))
        carry_over.begin()

    @pl.when(i == 2)
    def _():
        carry_over.cube.start(1)

    heads = q_ref.shape[1] // HEAD_DIM
    qs = [q_ref[:, head(h)] for h in range(heads)]

    def block(j, carry, masked):
        rows = pl.ds(pl.multiple_of(j * bk, bk), bk)
        k = k_ref[rows, :]
        vt = vt_ref[:, rows]
        out = []
        for h in range(heads):
            m, l, acc = carry[h]
            s = lax.dot_general(k, qs[h], NT, preferred_element_type=jnp.float32)
            if masked:
                kpos = j * bk + lax.broadcasted_iota(jnp.int32, (bk, bq), 0)
                qpos = i * bq + lax.broadcasted_iota(jnp.int32, (bk, bq), 1)
                s = jnp.where(qpos >= kpos, s, BIG)
            m_new = jnp.maximum(m, jnp.max(s, axis=0, keepdims=True))
            p = jnp.exp2((s - m_new) * SCALE2)
            alpha = jnp.exp2((m - m_new) * SCALE2)
            l = l * alpha + jnp.sum(p, axis=0, keepdims=True)
            acc = acc * alpha + lax.dot_general(vt, p.astype(jnp.bfloat16), NN, preferred_element_type=jnp.float32)
            out.append((m_new, l, acc))
        return tuple(out)

    init = tuple((jnp.full((1, bq), BIG, jnp.float32), jnp.zeros((1, bq), jnp.float32), jnp.zeros((HEAD_DIM, bq), jnp.float32)) for _ in range(heads))
    full = i * bq // bk
    carry = lax.fori_loop(0, full, lambda j, c: block(j, c, False), init)
    for d in range(max(1, bq // bk)):
        carry = block(full + d, carry, True)
    for h in range(heads):
        m, l, acc = carry[h]
        o = acc / l
        o_ref[:, head(h)] = o.T.astype(jnp.bfloat16)
        ot_ref[head(h), :] = o.astype(jnp.bfloat16)
        lse_ref[h:h + 1, :] = m * SCALE2 + jnp.log2(l)

    @pl.when(i == last)
    def _():
        carry_over.cube.start(2)
        carry_over.end()


def flash_fwd(q, k, vt, ws, cid, bq=1024, bk=512):
    seq, width = q.shape
    heads = width // HEAD_DIM
    vm = pl.BlockSpec(memory_space=pltpu.VMEM)
    an = pl.BlockSpec(memory_space=pl.ANY)
    return pl.pallas_call(
        functools.partial(fwd_kernel, bq, bk),
        grid=(seq // bq,),
        in_specs=[pl.BlockSpec((bq, width), by_rows),
                  pl.BlockSpec((seq, HEAD_DIM), whole),
                  pl.BlockSpec((HEAD_DIM, seq), whole)] + [vm] * 4,
        out_specs=[pl.BlockSpec((bq, width), by_rows), pl.BlockSpec((width, bq), by_cols),
                   pl.BlockSpec((heads, bq), by_cols)] + [an] * 4,
        out_shape=[jax.ShapeDtypeStruct((seq, width), jnp.bfloat16), jax.ShapeDtypeStruct((width, seq), jnp.bfloat16), jax.ShapeDtypeStruct((heads, seq), jnp.float32)] + gathered(ws),
        scratch_shapes=[pltpu.SemaphoreType.DMA((NW,)), pltpu.SemaphoreType.DMA((NW,)), pltpu.SemaphoreType.DMA((4,))],
        cost_estimate=pl.CostEstimate(flops=2 * seq * seq * width * 2, bytes_accessed=8 << 20, transcendentals=seq * seq),
        compiler_params=comm_params(cid, vmem_limit_bytes=56 << 20),
        name="flash_fwd",
    )(q, k, vt, *ws)


def bwd_kernel(bq, bk, q_ref, o_ref, d_ref, k_ref, kt_ref, v_ref, lse_ref, cos_ref, sin_ref, g1, g3, g2, out_ref, r1, r3, r2, dqt, dka, dva, rd, send_sem, recv_sem):
    j = pl.program_id(0)
    nk = pl.num_programs(0)
    seq, width = q_ref.shape
    heads = width // HEAD_DIM
    nq = seq // bq
    k = k_ref[...]
    v = v_ref[...]
    kt = kt_ref[...]
    here = Spot()
    wires = Wires(send_sem, recv_sem)
    carry_over = halve_copies(here, wires, 3, (g1, g3, g2), (r1, r3, r2))

    half = HEAD_DIM // 2

    @pl.when(j == 0)
    def _():
        greet([here.peer(d) for d in 'xyz'])
        for cp in carry_over:
            cp.start()
        dqt[...] = jnp.zeros_like(dqt)

        def prep(i, c):
            rows = pl.ds(pl.multiple_of(i * bq, bq), bq)
            for h in range(heads):
                cols = head(h)
                prod = o_ref[rows, cols].astype(jnp.float32) * d_ref[rows, cols].astype(jnp.float32)
                rd[h:h + 1, rows] = jnp.sum(prod.T, axis=0, keepdims=True)
            return c
        lax.fori_loop(0, nq, prep, 0)

    dka[...] = jnp.zeros_like(dka)
    dva[...] = jnp.zeros_like(dva)

    def block(i, masked):
        rows = pl.ds(pl.multiple_of(i * bq, bq), bq)
        for h in range(heads):
            cols = head(h)
            q = q_ref[rows, cols]
            d = d_ref[rows, cols]
            s = lax.dot_general(k, q, NT, preferred_element_type=jnp.float32)
            dp = lax.dot_general(v, d, NT, preferred_element_type=jnp.float32)
            p = jnp.exp2(s * SCALE2 - lse_ref[h:h + 1, rows])
            if masked:
                kpos = j * bk + lax.broadcasted_iota(jnp.int32, (bk, bq), 0)
                qpos = i * bq + lax.broadcasted_iota(jnp.int32, (bk, bq), 1)
                p = jnp.where(qpos >= kpos, p, 0.0)
            ds = (p * (dp - rd[h:h + 1, rows]) * ATTN_SCALE).astype(jnp.bfloat16)
            dva[...] += lax.dot_general(p.astype(jnp.bfloat16), d, NN, preferred_element_type=jnp.float32)
            dka[...] += lax.dot_general(ds, q, NN, preferred_element_type=jnp.float32)
            dqt[cols, rows] += lax.dot_general(kt, ds, NN, preferred_element_type=jnp.float32)

    first = j * bk // bq
    ndiag = max(1, bk // bq)
    for t in range(ndiag):
        block(first + t, True)
    lax.fori_loop(first + ndiag, nq, lambda i, c: (block(i, False), c)[1], 0)
    own = pl.ds(pl.multiple_of(j * bk, bk), bk)
    cosw, sinw = wide_tables(cos_ref[:, own], sin_ref[:, own])
    dk = dka[...].astype(jnp.bfloat16).astype(jnp.float32)
    out_ref[own, width:width + HEAD_DIM] = (dk * cosw - pltpu.roll(dk, half, 1) * sinw).astype(jnp.bfloat16)
    out_ref[own, width + HEAD_DIM:] = dva[...].astype(jnp.bfloat16)

    @pl.when(j == nk - 1)
    def _():
        def fin(i, c):
            rows = pl.ds(pl.multiple_of(i * bq, bq), bq)
            cos, sin = cos_ref[:, rows], sin_ref[:, rows]
            for h in range(heads):
                cols = head(h)
                t = dqt[cols, rows].astype(jnp.bfloat16).astype(jnp.float32)
                lo, hi = t[:half], t[half:]
                out_ref[rows, cols] = jnp.concatenate([lo * cos + hi * sin, hi * cos - lo * sin], axis=0).T.astype(jnp.bfloat16)
            return c
        lax.fori_loop(0, nq, fin, 0)
        for cp in carry_over:
            cp.wait()


def flash_bwd(q, o, d, k, kt, v, lse, cos_t, sin_t, gs, cid, bq=512, bk=512):
    seq, width = q.shape
    heads = width // HEAD_DIM
    an = pl.BlockSpec(memory_space=pl.ANY)
    return pl.pallas_call(
        functools.partial(bwd_kernel, bq, bk),
        grid=(seq // bk,),
        in_specs=[pl.BlockSpec((seq, width), whole), pl.BlockSpec((seq, width), whole), pl.BlockSpec((seq, width), whole),
                  pl.BlockSpec((bk, HEAD_DIM), by_rows), pl.BlockSpec((HEAD_DIM, bk), by_cols),
                  pl.BlockSpec((bk, HEAD_DIM), by_rows),
                  pl.BlockSpec((heads, seq), whole), pl.BlockSpec(cos_t.shape, whole), pl.BlockSpec(cos_t.shape, whole)] + [an] * 3,
        out_specs=[pl.BlockSpec((seq, width + 2 * HEAD_DIM), whole)] + [an] * 3,
        out_shape=[jax.ShapeDtypeStruct((seq, width + 2 * HEAD_DIM), jnp.bfloat16)] + halve_shapes(gs, 3),
        scratch_shapes=[pltpu.VMEM((width, seq), jnp.float32), pltpu.VMEM((bk, HEAD_DIM), jnp.float32), pltpu.VMEM((bk, HEAD_DIM), jnp.float32),
                        pltpu.VMEM((heads, seq), jnp.float32), pltpu.SemaphoreType.DMA((3,)), pltpu.SemaphoreType.DMA((3,))],
        cost_estimate=pl.CostEstimate(flops=5 * seq * seq * width * 2 // 2, bytes_accessed=16 << 20, transcendentals=seq * seq),
        compiler_params=comm_params(cid, vmem_limit_bytes=58 << 20),
        name="flash_bwd",
    )(q, o, d, k, kt, v, lse, cos_t, sin_t, *gs)


class PlaneGather:
    N = 13

    def __init__(self, here, wires, src, out, local_sem):
        h = src.shape[0] // 2
        A, B = slice(h), slice(h, None)
        s = here.s
        sx, sy, sc = here.peer('x')[1], here.peer('y')[1], here.peer('c')[1]
        sd = here.s + 2 - 4 * here.x + 4 - 8 * here.y
        nx, ny, nc = here.peer('x'), here.peer('y'), here.peer('c')
        self.local = pltpu.make_async_copy(src, out.at[s], local_sem)
        mk = wires.copy
        self.x1 = {k: mk(src.at[r], out.at[s, r], nx) for k, r in (('A', A), ('B', B))}
        self.y1 = {k: mk(src.at[r], out.at[s, r], ny) for k, r in (('B', B), ('A', A))}
        self.c1 = mk(src, out.at[s], nc)
        self.fy = mk(out.at[sx, A], out.at[sx, A], ny)
        self.fx = mk(out.at[sy, B], out.at[sy, B], nx)
        self.cc = {}
        for name, idx in (('x', sx), ('y', sy), ('d', sd)):
            for k, r in (('A', A), ('B', B)):
                self.cc[name + k] = mk(out.at[idx, r], out.at[idx, r], nc)

    def start_first(self):
        self.x1['A'].start()
        self.y1['B'].start()
        self.c1.start()
        self.local.start()

    def start_second(self):
        self.x1['B'].start()
        self.y1['A'].start()

    def relay(self):
        self.x1['A'].wait_recv()
        self.fy.start()
        self.cc['xA'].start()
        self.y1['B'].wait_recv()
        self.fx.start()
        self.cc['yB'].start()
        self.x1['B'].wait_recv()
        self.cc['xB'].start()
        self.y1['A'].wait_recv()
        self.cc['yA'].start()

    def finish(self):
        self.fy.wait_recv()
        self.cc['dA'].start()
        self.fx.wait_recv()
        self.cc['dB'].start()
        self.c1.wait_recv()
        for k in self.cc:
            self.cc[k].wait_recv()
        for c in (*self.x1.values(), *self.y1.values(), self.c1, self.fy, self.fx, *self.cc.values()):
            c.wait_send()
        self.local.wait()


def dh_kernel(src, out, send_sem, recv_sem, local_sem):
    here = Spot()
    greet([here.peer(d) for d in 'xyc'])
    g = PlaneGather(here, Wires(send_sem, recv_sem), src, out, local_sem)
    g.start_first()
    g.start_second()
    g.relay()
    g.finish()


def gather_dh(src, cid):
    rows, cols = src.shape
    n = PlaneGather.N
    return pl.pallas_call(
        dh_kernel, in_specs=[pl.BlockSpec(memory_space=pltpu.VMEM)], out_specs=pl.BlockSpec(memory_space=pl.ANY),
        out_shape=jax.ShapeDtypeStruct((8, rows, cols), src.dtype),
        scratch_shapes=[pltpu.SemaphoreType.DMA((n,)), pltpu.SemaphoreType.DMA((n,)), pltpu.SemaphoreType.DMA],
        cost_estimate=busy(40), compiler_params=comm_params(cid), name="gather_dh",
    )(src)


def mlp_kernel(u_ref, d_ref, w1_ref, w3_ref, w2_ref, wg, y_ref, yp_ref, dx_ref, dxp_ref, g1_ref, g3_ref, g2_ref, og, ut, send_sem, recv_sem, local_sem):
    j = pl.program_id(0)
    last = pl.num_programs(0) - 1
    here = Spot()
    c = here.c
    wires = Wires(send_sem, recv_sem)
    loc = pltpu.make_async_copy(wg, og.at[here.region('') + (c,)], local_sem)
    jobs = [(og, (c, slice(None), slice(off, off + n)), order) for (off, n), order in zip(col_chunks(wg.shape[1], 3), ORDERS)]
    cube = CubeGather(here, wires, jobs)
    post = wires.copy(og.at[:, :, :, c], og.at[:, :, :, c], here.peer('c'))
    toks = u_ref.shape[0]

    @pl.when(j == 0)
    def _():
        greet(cube_targets(here))
        loc.start()
        loc.wait()
        cube.start(0)
        for r in (y_ref, yp_ref, dx_ref, dxp_ref):
            r[...] = jnp.zeros_like(r)

        def flip(i, carry):
            part = pl.ds(pl.multiple_of(i * 128, 128), 128)
            ut[:, part] = u_ref[part, :].astype(jnp.float32).T.astype(jnp.bfloat16)
            return carry
        lax.fori_loop(0, toks // 128, flip, 0)

    @pl.when(j == 1)
    def _():
        cube.start(1)

    @pl.when(j == 3)
    def _():
        cube.start(2)

    @pl.when(j == last)
    def _():
        cube.arrive()
        post.start()

    f32 = jnp.float32
    u, d = u_ref[...], d_ref[...]
    w1, w3, w2 = w1_ref[...], w3_ref[...], w2_ref[...]
    gate = jnp.dot(u, w1, preferred_element_type=f32)
    up = jnp.dot(u, w3, preferred_element_type=f32)
    act = lax.dot_general(d, w2, NT, preferred_element_type=f32)
    sig = jax.nn.sigmoid(gate)
    silu = gate * sig
    z = (silu * up).astype(jnp.bfloat16)
    da = (act * up * sig * (1.0 + gate * (1.0 - sig))).astype(jnp.bfloat16)
    dc = (act * silu).astype(jnp.bfloat16)
    y = jnp.dot(z, w2, preferred_element_type=f32)
    dx = lax.dot_general(da, w1, NT, preferred_element_type=f32) + lax.dot_general(dc, w3, NT, preferred_element_type=f32)
    mine = y_ref.shape[0]
    y_ref[...] += y[:mine]
    yp_ref[...] += y[mine:]
    dx_ref[...] += dx[:mine]
    dxp_ref[...] += dx[mine:]
    g1_ref[...] = jnp.dot(ut[...], da, preferred_element_type=f32)
    g3_ref[...] = jnp.dot(ut[...], dc, preferred_element_type=f32)
    g2_ref[...] = lax.dot_general(z, d, (((0,), (0,)), ((), ())), preferred_element_type=f32)

    @pl.when(j == last)
    def _():
        post.wait()
        cube.drain()


def mlp(u, d, w1, w3, w2, wg, cid, bh=256):
    toks, dim = u.shape
    half = w1.shape[1]
    f32 = jnp.float32
    vm = pl.BlockSpec(memory_space=pltpu.VMEM)
    an = pl.BlockSpec(memory_space=pl.ANY)
    return pl.pallas_call(
        mlp_kernel, grid=(half // bh,),
        in_specs=[vm, vm, pl.BlockSpec((dim, bh), by_cols), pl.BlockSpec((dim, bh), by_cols), pl.BlockSpec((bh, dim), by_rows), vm],
        out_specs=[pl.BlockSpec((toks // 2, dim), whole)] * 4 + [pl.BlockSpec((dim, bh), by_cols), pl.BlockSpec((dim, bh), by_cols),
                   pl.BlockSpec((bh, dim), by_rows), an],
        out_shape=[jax.ShapeDtypeStruct((toks // 2, dim), f32)] * 4 + [jax.ShapeDtypeStruct((dim, half), f32),
                   jax.ShapeDtypeStruct((dim, half), f32), jax.ShapeDtypeStruct((half, dim), f32),
                   jax.ShapeDtypeStruct((2, 2, 2, 2, *wg.shape), wg.dtype)],
        scratch_shapes=[pltpu.VMEM((dim, toks), jnp.bfloat16), pltpu.SemaphoreType.DMA((19,)), pltpu.SemaphoreType.DMA((19,)), pltpu.SemaphoreType.DMA],
        cost_estimate=pl.CostEstimate(flops=18 * toks * dim * half, bytes_accessed=48 << 20, transcendentals=toks * half),
        compiler_params=comm_params(cid, vmem_limit_bytes=58 << 20), name="mlp",
    )(u, d, w1, w3, w2, wg)


def entry_kernel(x_ref, w_ref, meta_ref, pos_ref, xa, wa, ma, pa, send_sem, recv_sem, local_sem):
    here = Spot()
    z, s = here.z, here.s
    peers = here.others()
    nz = here.peer('z')
    greet(peers + [nz])
    wires = Wires(send_sem, recv_sem)
    first = []
    for t in peers:
        for src, dst in ((w_ref.at[t[1]], wa.at[z, s]), (meta_ref, ma.at[z, s]), (pos_ref, pa.at[s])):
            first.append(wires.copy(src, dst, t))
    locals_ = [pltpu.make_async_copy(w_ref.at[s], wa.at[z, s], local_sem.at[1]),
               pltpu.make_async_copy(meta_ref, ma.at[z, s], local_sem.at[2]),
               pltpu.make_async_copy(pos_ref, pa.at[s], local_sem.at[3])]
    g = PlaneGather(here, wires, x_ref, xa, local_sem.at[0])
    cross = [wires.copy(wa.at[z], wa.at[z], nz), wires.copy(ma.at[z], ma.at[z], nz)]
    for c in first:
        c.start()
    for c in locals_:
        c.start()
    g.start_first()
    g.start_second()
    for c in first:
        c.wait_recv()
    for c in locals_:
        c.wait()
    for c in cross:
        c.start()
    g.relay()
    g.finish()
    for c in cross:
        c.wait()
    for c in first:
        c.wait_send()


def entry(x, w, meta, pos, cid):
    n = PlaneGather.N + 21 + 2
    vm = pl.BlockSpec(memory_space=pltpu.VMEM)
    an = pl.BlockSpec(memory_space=pl.ANY)
    return pl.pallas_call(
        entry_kernel,
        in_specs=[vm] * 4, out_specs=[an] * 4,
        out_shape=[jax.ShapeDtypeStruct((8, *x.shape), x.dtype), jax.ShapeDtypeStruct((2, 8, *w.shape[1:]), w.dtype),
                   jax.ShapeDtypeStruct((2, 8, *meta.shape), meta.dtype), jax.ShapeDtypeStruct((8, *pos.shape), pos.dtype)],
        scratch_shapes=[pltpu.SemaphoreType.DMA((n,)), pltpu.SemaphoreType.DMA((n,)), pltpu.SemaphoreType.DMA((4,))],
        cost_estimate=busy(45), compiler_params=comm_params(cid),
        name="entry",
    )(x, w, meta, pos)


def regroup_kernel(n, *refs):
    src, gs, out, rs = refs[0], refs[1:1 + n], refs[1 + n], refs[2 + n:2 + 2 * n]
    send_sem, recv_sem, local_sem, stage = refs[2 + 2 * n:]
    here = Spot()
    s = here.s
    rows, width = out.shape[0], src.shape[1]
    peers = here.others()
    greet(peers + ([here.peer('z')] if n else []))
    wires = Wires(send_sem, recv_sem)
    piece = lambda i: pl.ds(pl.multiple_of(i * rows, rows), rows)
    mine = pl.ds(pl.multiple_of(s * width, width), width)
    cs = [wires.copy(src.at[piece(t[1])], out.at[:, mine], t) for t in peers]
    cs += [wires.copy(g, r, here.peer(order[1])) for g, r, order in zip(gs[:3], rs, ORDERS)]
    cs += [wires.copy(g.at[1 - here.z], r, here.peer('z')) for g, r in zip(gs[3:], rs[3:])]
    for c in cs:
        c.start()
    a = pltpu.make_async_copy(src.at[piece(s)], stage, local_sem.at[0])
    a.start()
    a.wait()
    b = pltpu.make_async_copy(stage, out.at[:, mine], local_sem.at[1])
    b.start()
    b.wait()
    for c in cs:
        c.wait()


def regroup(src, gs, cid, name):
    seq, width = src.shape
    rows, n = seq // 8, len(gs)
    an = pl.BlockSpec(memory_space=pl.ANY)
    back = [jax.ShapeDtypeStruct(g.shape if i < 3 else g.shape[1:], g.dtype) for i, g in enumerate(gs)]
    out = pl.pallas_call(
        functools.partial(regroup_kernel, n), in_specs=[an] * (1 + n), out_specs=[an] * (1 + n),
        out_shape=[jax.ShapeDtypeStruct((rows, 8 * width), src.dtype)] + back,
        scratch_shapes=[pltpu.SemaphoreType.DMA((7 + n,)), pltpu.SemaphoreType.DMA((7 + n,)), pltpu.SemaphoreType.DMA((2,)), pltpu.VMEM((rows, width), src.dtype)],
        cost_estimate=busy(70 if n else 25), compiler_params=comm_params(cid), name=name,
    )(src, *gs)
    return out[0], out[1:]


def back_kernel(t_ref, w_ref, x_ref, gain_ref, res_ref, a, g1, g3, g2, dx_ref, gg_ref, oa, r1, r3, r2, acc, send_sem, recv_sem, local_sem):
    j = pl.program_id(0)
    bn = w_ref.shape[0]
    here = Spot()
    peers = here.others()
    wires = Wires(send_sem, recv_sem)
    s = here.s
    cs = [wires.copy(g, r, here.peer(order[0])) for g, r, order in zip((g1, g3, g2), (r1, r3, r2), ORDERS)]
    cs += [wires.copy(a.at[t[1]], oa.at[s], t) for t in peers]
    loc = pltpu.make_async_copy(a.at[s], oa.at[s], local_sem)

    @pl.when(j == 0)
    def _():
        greet(peers + [here.peer('z')])
        for c in cs:
            c.start()
        loc.start()

    acc[:, pl.ds(pl.multiple_of(j * bn, bn), bn)] = lax.dot_general(t_ref[...], w_ref[...], NT, preferred_element_type=jnp.float32)

    @pl.when(j == pl.num_programs(0) - 1)
    def _():
        gg_ref[...] = jnp.zeros_like(gg_ref)
        gain = gain_ref[0:1, :].astype(jnp.float32)

        def rows_of(i, carry):
            part = pl.ds(pl.multiple_of(i * HEAD_DIM, HEAD_DIM), HEAD_DIM)
            x = x_ref[part, :].astype(jnp.float32)
            inv = lax.rsqrt(jnp.mean(x * x, axis=-1, keepdims=True) + NORM_EPS)
            normed = x * inv
            d_out = acc[part, :]
            d_normed = d_out * gain
            gg_ref[...] += jnp.sum(d_out * normed, axis=0, keepdims=True)
            grad_in = inv * (d_normed - normed * jnp.mean(d_normed * normed, axis=-1, keepdims=True))
            dx_ref[part, :] = (res_ref[part, :] + grad_in).astype(jnp.bfloat16)
            return carry
        lax.fori_loop(0, x_ref.shape[0] // HEAD_DIM, rows_of, 0)
        for c in cs:
            c.wait()
        loc.wait()


def back_project(t, w, x, gain, res, a, gs, cid, bn=256):
    toks, inner = t.shape
    dim = w.shape[0]
    vm = pl.BlockSpec(memory_space=pltpu.VMEM)
    an = pl.BlockSpec(memory_space=pl.ANY)
    out = pl.pallas_call(
        back_kernel, grid=(dim // bn,),
        in_specs=[vm, pl.BlockSpec((bn, inner), by_rows)] + [vm] * 4 + [an] * 3,
        out_specs=[pl.BlockSpec((toks, dim), whole), pl.BlockSpec((1, dim), whole)] + [an] * 4,
        out_shape=[jax.ShapeDtypeStruct((toks, dim), jnp.bfloat16), jax.ShapeDtypeStruct((1, dim), jnp.float32), jax.ShapeDtypeStruct(a.shape, a.dtype)]
        + [jax.ShapeDtypeStruct(g.shape, g.dtype) for g in gs],
        scratch_shapes=[pltpu.VMEM((toks, dim), jnp.float32), pltpu.SemaphoreType.DMA((10,)), pltpu.SemaphoreType.DMA((10,)), pltpu.SemaphoreType.DMA],
        cost_estimate=busy(35), compiler_params=comm_params(cid, vmem_limit_bytes=62 << 20), name="back_project",
    )(t, w, x, gain, res, a, *gs)
    return out[0], out[1], out[2], out[3:]


def last_kernel(b, p1, p3, ob, q1, q3, send_sem, recv_sem, local_sem):
    here = Spot()
    peers = here.others()
    greet(peers)
    wires = Wires(send_sem, recv_sem)
    s, nc = here.s, here.peer('c')
    cs = [wires.copy(p.at[1 - here.c], q, nc) for p, q in ((p1, q1), (p3, q3))]
    cs += [wires.copy(b.at[t[1]], ob.at[s], t) for t in peers]
    loc = pltpu.make_async_copy(b.at[s], ob.at[s], local_sem)
    for c in cs + [loc]:
        c.start()
    for c in cs + [loc]:
        c.wait()


def last_exchange(b, p1, p3, cid):
    vm = pl.BlockSpec(memory_space=pltpu.VMEM)
    return pl.pallas_call(
        last_kernel, in_specs=[vm] * 3, out_specs=[vm] * 3,
        out_shape=[jax.ShapeDtypeStruct(b.shape, b.dtype)] + [jax.ShapeDtypeStruct(p.shape[1:], p.dtype) for p in (p1, p3)],
        scratch_shapes=[pltpu.SemaphoreType.DMA((9,)), pltpu.SemaphoreType.DMA((9,)), pltpu.SemaphoreType.DMA],
        cost_estimate=busy(5), compiler_params=comm_params(cid), name="last_exchange",
    )(b, p1, p3)


def dot_tokens(left_op, right_op):
    return lax.dot_general(left_op, right_op, (((0,), (0,)), ((), ())), preferred_element_type=jnp.float32)


def dot_back(left_op, weight):
    return lax.dot_general(left_op, weight, (((1,), (1,)), ((), ())), preferred_element_type=jnp.float32)


def dot_on(left_op, weight):
    return jnp.dot(left_op, weight, preferred_element_type=jnp.float32)


def swap_core(t):
    return lax.ppermute(t, 'sp', [(i, i ^ 1) for i in range(8)])


def swap_z(t):
    return lax.ppermute(t, 'dp', [(0, 1), (1, 0)])


def split_cols(w):
    rows, cols = w.shape
    return w.reshape(rows, 8, 2, cols // 16).transpose(2, 0, 1, 3).reshape(2, rows, cols // 2)


def join_cols(mine, other, c):
    rows, half = mine.shape
    m, o = mine.reshape(rows, 8, 1, half // 8), other.reshape(rows, 8, 1, half // 8)
    first = jnp.where(c == 0, m, o)
    second = jnp.where(c == 0, o, m)
    return jnp.concatenate([first, second], axis=2).reshape(rows, 2 * half)


def layer_step(hidden, positions, grad_out, gain_attn, gain_mlp, w_query, w_key, w_value, w_out, w_gate, w_up, w_down):
    tokens = hidden[0]
    d_layer = grad_out[0]
    tok, dim = tokens.shape
    here = Spot()
    z, s, c = here.z, here.s, here.c
    rows = w_query.shape[0]
    grp_q = w_query.shape[1] // 8
    grp_k = w_key.shape[1] // 8
    grp = grp_q + 2 * grp_k
    seq = 8 * tok

    w_grp = jnp.concatenate([w_query.reshape(rows, 8, grp_q), w_key.reshape(rows, 8, grp_k), w_value.reshape(rows, 8, grp_k)], axis=2)
    w_flat = w_grp.reshape(rows, 8 * grp)
    pad = HEAD_DIM - gain_attn.shape[0]
    meta = jnp.pad(jnp.stack([gain_attn, gain_mlp]), ((0, 14), (0, pad)))
    x_all, w_own, meta_all, pos_all = entry(tokens, w_grp.transpose(1, 0, 2), meta, positions[0].reshape(-1, 128), 1)
    x_all = x_all.reshape(seq, dim)
    w_own = w_own.reshape(dim, grp)
    gain1 = meta_all[:, :, 0, :rows].reshape(dim)
    gain2 = meta_all[:, :, 1, :rows].reshape(dim)
    cos_t, sin_t = rope_tables(pos_all.reshape(seq))

    gain1_rows = jnp.broadcast_to(gain1[None], (16, dim))
    u_all, q_own, k_own, v_own, k_t, v_t = project(x_all, gain1_rows, w_own, cos_t, sin_t)
    o_own, o_t, lse, w1, w3, w2, wo = flash_fwd(q_own, k_own, v_t, (split_cols(w_gate), split_cols(w_up), w_down, w_out), 2)
    ffn_half = w1.shape[-1]
    w1, w3 = w1.reshape(dim, ffn_half), w3.reshape(dim, ffn_half)
    w2 = w2.reshape(ffn_half, dim)
    wo = wo.reshape(-1, dim)
    attn_out, _ = regroup(o_own, (), 3, 'regroup_o')
    residual = (tokens.astype(jnp.float32) + dot_on(attn_out, wo)).astype(jnp.bfloat16)
    u_mlp, normed2, inv_rms2 = rms_norm(residual, gain2)
    u_pair = jnp.concatenate([u_mlp, swap_core(u_mlp)], axis=0)
    d_pair = jnp.concatenate([d_layer, swap_core(d_layer)], axis=0)
    y_part, y_peer, d_part, d_peer, g1, g3, g2, wg = mlp(u_pair, d_pair, w1, w3, w2, w_flat, 7)
    layer_out = (residual.astype(jnp.float32) + (y_part + swap_core(y_peer))).astype(jnp.bfloat16)

    d_umlp = d_part + swap_core(d_peer)
    d_res_norm, d_gain2 = rms_norm_grad(d_umlp, normed2, inv_rms2, gain2)
    d_resid = d_layer.astype(jnp.float32) + d_res_norm
    d_resid_bf = d_resid.astype(jnp.bfloat16)
    g1 = g1.reshape(2, 2, 2, dim // 8, ffn_half)
    g3 = g3.reshape(2, 2, 2, dim // 8, ffn_half)
    g2 = g2.reshape(2, 2, 2, ffn_half // 8, dim)

    dh_all = gather_dh(d_resid_bf, 4).reshape(seq, dim)
    wg = wg.reshape(dim, 8 * grp)
    wo_own = lax.dynamic_slice_in_dim(wo, s * grp_q, grp_q, 0)
    d_own = dot_back(dh_all, wo_own).astype(jnp.bfloat16)
    go = dot_on(o_t, dh_all).reshape(2, grp_q // 2, dim)
    dqkv_pre, *got = flash_bwd(q_own, o_own, d_own, k_own, k_t, v_own, lse, cos_t, sin_t, (g1, g3, g2), 6)
    gq = dot_tokens(u_all, dqkv_pre).reshape(2, dim // 2, grp)
    terms = after(here, [[g1], [g3], [g2]], got, 3)
    dqkv_tok, (*got, gq_got, go_got) = regroup(dqkv_pre, (*to_send(here, terms, 2), gq, go), 5, 'regroup_dqkv')
    go_mine = pick(go, z) + go_got
    stay = dim // HEAD_DIM - 1
    moved = lax.ppermute(go_mine, ALL_AXES, [(zz * 8 + ss, 2 * ss + zz) for zz in range(2) for ss in range(8) if ss != zz * stay])
    grad_w_out = jnp.where(s == z * stay, go_mine, moved)
    terms = after(here, terms, got, 2)
    gq_mine = pick(gq, z) + gq_got
    grad_hidden, d_gain1, got_q, got = back_project(dqkv_tok, wg, tokens, gain1_rows, d_resid, gq_mine.reshape(8, rows, grp), to_send(here, terms, 1), 8)
    m1, m3, grad_w_down = [total(ts) for ts in after(here, terms, got, 1)]

    gains = jnp.concatenate([d_gain1.reshape(2, 8, rows), d_gain2.reshape(2, 8, rows)], axis=2)
    gains_mine = pick(gains, z) + swap_z(pick(gains, 1 - z))
    gains_mine = jnp.broadcast_to(gains_mine[:, None, :], (8, 8, 2 * rows))
    pair1, pair3 = m1.reshape(2, rows, ffn_half), m3.reshape(2, rows, ffn_half)
    got_g, other1, other3 = last_exchange(gains_mine, pair1, pair3, 10)
    got_q = got_q.transpose(1, 0, 2)
    grad_w_query = got_q[:, :, :grp_q].reshape(rows, 8 * grp_q)
    grad_w_key = got_q[:, :, grp_q:grp_q + grp_k].reshape(rows, 8 * grp_k)
    grad_w_value = got_q[:, :, grp_q + grp_k:].reshape(rows, 8 * grp_k)
    grad_gains = jnp.sum(got_g[:, 0, :], axis=0)
    grad_gain_attn, grad_gain_mlp = grad_gains[:rows], grad_gains[rows:]

    grad_w_gate = join_cols(pick(pair1, c), other1, c)
    grad_w_up = join_cols(pick(pair3, c), other3, c)
    return (layer_out[None], grad_hidden[None], grad_gain_attn, grad_gain_mlp, grad_w_query, grad_w_key, grad_w_value, grad_w_out, grad_w_gate, grad_w_up, grad_w_down)


def solution(mesh):
    act_spec = P('dp', 'sp', None)
    pos_spec = P('dp', 'sp')
    vec_spec = P(ALL_AXES)
    mat_spec = P(ALL_AXES, None)
    in_specs = (act_spec, pos_spec, act_spec, vec_spec, vec_spec) + (mat_spec,) * 7
    out_specs = (act_spec, act_spec, vec_spec, vec_spec) + (mat_spec,) * 7
    return jax.shard_map(layer_step, mesh=mesh, in_specs=in_specs, out_specs=out_specs, check_vma=False)
```

```python
import functools
import math

import jax
import jax.numpy as jnp
from jax import lax
from jax.experimental import pallas as pl
from jax.experimental.pallas import tpu as pltpu
from jax.sharding import PartitionSpec as P

HEAD_DIM = 128
ROPE_BASE = 10000.0
NORM_EPS = 1e-5
ATTN_SCALE = HEAD_DIM ** -0.5
ALL_AXES = ('dp', 'sp')


def rope_tables(pos_ids):
    inv_freq = ROPE_BASE ** (-(jnp.arange(HEAD_DIM // 2, dtype=jnp.float32) * (2.0 / HEAD_DIM)))
    angles = pos_ids.astype(jnp.float32)[None, :] * inv_freq[:, None]
    return jnp.cos(angles), jnp.sin(angles)


def rms_norm(values, gain_vec):
    vals32 = values.astype(jnp.float32)
    inv_rms = lax.rsqrt(jnp.mean(vals32 * vals32, axis=-1, keepdims=True) + NORM_EPS)
    normed = vals32 * inv_rms
    return (normed * gain_vec.astype(jnp.float32)).astype(jnp.bfloat16), normed, inv_rms


def rms_norm_grad(d_out, normed, inv_rms, gain_vec):
    d_normed = d_out * gain_vec.astype(jnp.float32)
    grad_gain = jnp.sum(d_out * normed, axis=0)
    grad_in = inv_rms * (d_normed - normed * jnp.mean(d_normed * normed, axis=-1, keepdims=True))
    return grad_in, grad_gain


MESH = pl.DeviceIdType.MESH


def by_rows(i):
    return i, 0


def by_cols(i):
    return 0, i


def whole(i):
    return 0, 0


def head(h):
    return slice(h * HEAD_DIM, (h + 1) * HEAD_DIM)


def pick(t, i):
    return lax.dynamic_index_in_dim(t, i, 0, False)


ORDERS = ('xyz', 'yzx', 'zxy')


class Spot:
    def __init__(self):
        self.z = lax.axis_index('dp')
        self.s = lax.axis_index('sp')
        self.y = self.s // 4
        self.x = (self.s // 2) % 2
        self.c = self.s % 2
        self.bits = {'z': self.z, 'y': self.y, 'x': self.x}

    def peer(self, dim):
        if dim == 'z':
            return (1 - self.z, self.s)
        if dim == 'y':
            return (self.z, self.s + 4 - 8 * self.y)
        if dim == 'x':
            return (self.z, self.s + 2 - 4 * self.x)
        return (self.z, self.s + 1 - 2 * self.c)

    def others(self):
        return [(self.z, (self.s + t) % 8) for t in range(1, 8)]

    def region(self, freed, flipped=''):
        return tuple(slice(None) if d in freed else (1 - self.bits[d] if d in flipped else self.bits[d]) for d in 'zyx')


def greet(targets):
    bar = pltpu.get_barrier_semaphore()
    for t in targets:
        pl.semaphore_signal(bar, inc=1, device_id=t, device_id_type=MESH)
    pl.semaphore_wait(bar, len(targets))


class Wires:
    def __init__(self, send_sem, recv_sem):
        self.send_sem, self.recv_sem, self.n = send_sem, recv_sem, 0

    def copy(self, src, dst, target):
        i = self.n
        self.n += 1
        return pltpu.make_async_remote_copy(src_ref=src, dst_ref=dst, send_sem=self.send_sem.at[i], recv_sem=self.recv_sem.at[i], device_id=target, device_id_type=MESH)


class CubeGather:
    def __init__(self, here, wires, jobs):
        firsts, seconds, thirds = [], [], []
        for out, suffix, (a, b, e) in jobs:
            def mk(freed, flipped, d):
                reg = here.region(freed, flipped) + suffix
                return wires.copy(out.at[reg], out.at[reg], here.peer(d))
            firsts.append([mk('', '', d) for d in (a, b, e)])
            seconds.append([mk('', a, d) for d in (b, e)])
            thirds.append(mk(a, b, e))
        self.stages = [[f[i] for i in range(3) for f in firsts], [t[i] for i in range(2) for t in seconds], thirds]
        self.need = [[f[0] for f in firsts], [f[1] for f in firsts] + [t[0] for t in seconds]]
        self.rest = [[f[2], t[1], e] for f, t, e in zip(firsts, seconds, thirds)]

    def start(self, i):
        for c in self.need[i - 1] if i else ():
            c.wait_recv()
        for c in self.stages[i]:
            c.start()

    def arrive(self, lo=0, hi=None):
        for job in self.rest[lo:hi]:
            for c in job:
                c.wait_recv()

    def drain(self):
        for st in self.stages:
            for c in st:
                c.wait_send()


def col_chunks(cols, parts):
    n, out, off = cols // 128, [], 0
    for p in range(parts, 0, -1):
        w = -(-n // p)
        out.append((off, w * 128))
        off += w * 128
        n -= w
    return out


def cube_targets(here):
    return [here.peer(d) for d in 'xyzc']


def comm_params(cid, **kw):
    return pltpu.CompilerParams(collective_id=cid, has_side_effects=True, **kw)


def busy(us):
    return pl.CostEstimate(flops=int(us * 1e8), bytes_accessed=1 << 20, transcendentals=0)


NW = 2 + 6 * 6 + 1


class WeightGather:
    def __init__(self, here, wires, local_sem, ins, outs):
        w1, w3, w2, wo = ins
        o1, o3, o2, oo = outs
        c, zyx, nc = here.c, here.region(''), here.peer('c')
        self.pre = [wires.copy(w1.at[1 - c], o1.at[zyx + (c,)], nc), wires.copy(w3.at[1 - c], o3.at[zyx + (c,)], nc)]
        self.loc = [pltpu.make_async_copy(w1.at[c], o1.at[zyx + (c,)], local_sem.at[0]),
                    pltpu.make_async_copy(w3.at[c], o3.at[zyx + (c,)], local_sem.at[1]),
                    pltpu.make_async_copy(w2, o2.at[zyx], local_sem.at[2]),
                    pltpu.make_async_copy(wo, oo.at[zyx + (c,)], local_sem.at[3])]
        jobs = [(oo, (c, slice(None), slice(off, off + n)), order) for (off, n), order in zip(col_chunks(wo.shape[1], 3), ORDERS)]
        jobs += [(o1, (), ORDERS[0]), (o3, (), ORDERS[1]), (o2, (), ORDERS[2])]
        self.cube = CubeGather(here, wires, jobs)
        self.post = wires.copy(oo.at[:, :, :, c], oo.at[:, :, :, c], nc)

    def begin(self):
        for c in self.pre + self.loc:
            c.start()
        for c in self.loc:
            c.wait()
        for c in self.pre:
            c.wait()
        self.cube.start(0)

    def end(self):
        self.cube.arrive(0, 3)
        self.post.start()
        self.cube.arrive(3)
        self.post.wait()
        self.cube.drain()


def gathered(ws):
    return [jax.ShapeDtypeStruct((2, 2, 2, *w.shape), w.dtype) if k < 3 else jax.ShapeDtypeStruct((2, 2, 2, 2, *w.shape), w.dtype) for k, w in enumerate(ws)]


def halve_copies(here, wires, nd, ins, outs):
    cs = []
    for i, (a, o) in enumerate(zip(ins, outs)):
        order = ORDERS[i % 3]
        d = order[nd - 1]
        reg = tuple(1 - here.bits[d] if e == d else slice(None) for e in 'zyx' if e in order[:nd])
        cs.append(wires.copy(a.at[reg], o, here.peer(d)))
    return cs


def halve_shapes(arrs, nd):
    return [jax.ShapeDtypeStruct((*((2,) * (nd - 1)), *a.shape[nd:]), a.dtype) for a in arrs]


def part_of(here, t, order, nd, flip):
    live = [d for d in 'zyx' if d in order[:nd]]
    d = order[nd - 1]
    bit = here.bits[d]
    return lax.dynamic_index_in_dim(t, 1 - bit if flip else bit, live.index(d), False)


def total(terms):
    out = terms[0]
    for t in terms[1:]:
        out = out + t
    return out


def to_send(here, terms, nd):
    return [total([part_of(here, t, ORDERS[i % 3], nd, True) for t in ts]) for i, ts in enumerate(terms)]


def after(here, terms, got, nd):
    return [[part_of(here, t, ORDERS[i % 3], nd, False) for t in ts] + [r] for i, (ts, r) in enumerate(zip(terms, got))]


def wide_tables(cos_t, sin_t):
    return jnp.concatenate([cos_t, cos_t], axis=0).T, jnp.concatenate([-sin_t, sin_t], axis=0).T


def proj_kernel(nrot, x_ref, g_ref, w_ref, cos_ref, sin_ref, u_ref, q_ref, k_ref, v_ref, kt_ref, vt_ref):
    x = x_ref[...].astype(jnp.float32)
    inv = lax.rsqrt(jnp.mean(x * x, axis=-1, keepdims=True) + NORM_EPS)
    u = (x * inv * g_ref[0:1, :].astype(jnp.float32)).astype(jnp.bfloat16)
    u_ref[...] = u
    cos, sin = wide_tables(cos_ref[...], sin_ref[...])
    full = jnp.dot(u, w_ref[...], preferred_element_type=jnp.float32)
    for h in range(nrot + 2):
        t = full[:, head(h)]
        if h <= nrot:
            t = t * cos + pltpu.roll(t, HEAD_DIM // 2, 1) * sin
        if h < nrot:
            q_ref[:, head(h)] = t.astype(jnp.bfloat16)
        else:
            n_ref, t_ref = (k_ref, kt_ref) if h == nrot else (v_ref, vt_ref)
            n_ref[...] = t.astype(jnp.bfloat16)
            t_ref[...] = t.T.astype(jnp.bfloat16)


def project(x, gain, w, cos_t, sin_t, bt=512):
    seq, dim = x.shape
    grp = w.shape[1]
    nq = grp // HEAD_DIM - 2
    bf = jnp.bfloat16
    return pl.pallas_call(
        functools.partial(proj_kernel, nq), grid=(seq // bt,),
        in_specs=[pl.BlockSpec((bt, dim), by_rows), pl.BlockSpec((16, dim), whole), pl.BlockSpec((dim, grp), whole),
                  pl.BlockSpec((cos_t.shape[0], bt), by_cols), pl.BlockSpec((cos_t.shape[0], bt), by_cols)],
        out_specs=[pl.BlockSpec((bt, dim), by_rows), pl.BlockSpec((bt, nq * HEAD_DIM), by_rows), pl.BlockSpec((bt, HEAD_DIM), by_rows), pl.BlockSpec((bt, HEAD_DIM), by_rows),
                   pl.BlockSpec((HEAD_DIM, bt), by_cols), pl.BlockSpec((HEAD_DIM, bt), by_cols)],
        out_shape=[jax.ShapeDtypeStruct((seq, dim), bf), jax.ShapeDtypeStruct((seq, nq * HEAD_DIM), bf), jax.ShapeDtypeStruct((seq, HEAD_DIM), bf),
                   jax.ShapeDtypeStruct((seq, HEAD_DIM), bf), jax.ShapeDtypeStruct((HEAD_DIM, seq), bf), jax.ShapeDtypeStruct((HEAD_DIM, seq), bf)],
        cost_estimate=pl.CostEstimate(flops=2 * seq * dim * grp, bytes_accessed=32 << 20, transcendentals=0),
        compiler_params=pltpu.CompilerParams(vmem_limit_bytes=62 << 20), name="project",
    )(x, gain, w, cos_t, sin_t)


LOG2E = math.log2(math.e)
SCALE2 = ATTN_SCALE * LOG2E
NT = (((1,), (1,)), ((), ()))
NN = (((1,), (0,)), ((), ()))
BIG = -1e30


def fwd_kernel(bq, bk, q_ref, k_ref, vt_ref, w1, w3, w2, wo, o_ref, ot_ref, lse_ref, o1, o3, o2, oo, send_sem, recv_sem, local_sem):
    i = pl.program_id(0)
    last = pl.num_programs(0) - 1
    here = Spot()
    carry_over = WeightGather(here, Wires(send_sem, recv_sem), local_sem, (w1, w3, w2, wo), (o1, o3, o2, oo))

    @pl.when(i == 0)
    def _():
        greet(cube_targets(here))
        carry_over.begin()

    @pl.when(i == 2)
    def _():
        carry_over.cube.start(1)

    heads = q_ref.shape[1] // HEAD_DIM
    qs = [q_ref[:, head(h)] for h in range(heads)]

    def block(j, carry, masked):
        rows = pl.ds(pl.multiple_of(j * bk, bk), bk)
        k = k_ref[rows, :]
        vt = vt_ref[:, rows]
        out = []
        for h in range(heads):
            m, l, acc = carry[h]
            s = lax.dot_general(k, qs[h], NT, preferred_element_type=jnp.float32)
            if masked:
                kpos = j * bk + lax.broadcasted_iota(jnp.int32, (bk, bq), 0)
                qpos = i * bq + lax.broadcasted_iota(jnp.int32, (bk, bq), 1)
                s = jnp.where(qpos >= kpos, s, BIG)
            m_new = jnp.maximum(m, jnp.max(s, axis=0, keepdims=True))
            p = jnp.exp2((s - m_new) * SCALE2)
            alpha = jnp.exp2((m - m_new) * SCALE2)
            l = l * alpha + jnp.sum(p, axis=0, keepdims=True)
            acc = acc * alpha + lax.dot_general(vt, p.astype(jnp.bfloat16), NN, preferred_element_type=jnp.float32)
            out.append((m_new, l, acc))
        return tuple(out)

    init = tuple((jnp.full((1, bq), BIG, jnp.float32), jnp.zeros((1, bq), jnp.float32), jnp.zeros((HEAD_DIM, bq), jnp.float32)) for _ in range(heads))
    full = i * bq // bk
    carry = lax.fori_loop(0, full, lambda j, c: block(j, c, False), init)
    carry = lax.fori_loop(full, full + bq // bk, lambda j, c: block(j, c, True), carry)
    for h in range(heads):
        m, l, acc = carry[h]
        o = acc / l
        o_ref[:, head(h)] = o.T.astype(jnp.bfloat16)
        ot_ref[head(h), :] = o.astype(jnp.bfloat16)
        lse_ref[h:h + 1, :] = m * SCALE2 + jnp.log2(l)

    @pl.when(i == last)
    def _():
        carry_over.cube.start(2)
        carry_over.end()


def flash_fwd(q, k, vt, ws, cid, bq=1024, bk=512):
    seq, width = q.shape
    heads = width // HEAD_DIM
    vm = pl.BlockSpec(memory_space=pltpu.VMEM)
    an = pl.BlockSpec(memory_space=pl.ANY)
    return pl.pallas_call(
        functools.partial(fwd_kernel, bq, bk),
        grid=(seq // bq,),
        in_specs=[pl.BlockSpec((bq, width), by_rows),
                  pl.BlockSpec((seq, HEAD_DIM), whole),
                  pl.BlockSpec((HEAD_DIM, seq), whole)] + [vm] * 4,
        out_specs=[pl.BlockSpec((bq, width), by_rows), pl.BlockSpec((width, bq), by_cols),
                   pl.BlockSpec((heads, bq), by_cols)] + [an] * 4,
        out_shape=[jax.ShapeDtypeStruct((seq, width), jnp.bfloat16), jax.ShapeDtypeStruct((width, seq), jnp.bfloat16), jax.ShapeDtypeStruct((heads, seq), jnp.float32)] + gathered(ws),
        scratch_shapes=[pltpu.SemaphoreType.DMA((NW,)), pltpu.SemaphoreType.DMA((NW,)), pltpu.SemaphoreType.DMA((4,))],
        cost_estimate=pl.CostEstimate(flops=2 * seq * seq * width * 2, bytes_accessed=8 << 20, transcendentals=seq * seq),
        compiler_params=comm_params(cid, vmem_limit_bytes=56 << 20),
        name="flash_fwd",
    )(q, k, vt, *ws)


def bwd_kernel(bq, bk, q_ref, o_ref, d_ref, k_ref, kt_ref, v_ref, lse_ref, cos_ref, sin_ref, g1, g3, g2, out_ref, r1, r3, r2, dqt, dka, dva, rd, send_sem, recv_sem):
    j = pl.program_id(0)
    nk = pl.num_programs(0)
    seq, width = q_ref.shape
    heads = width // HEAD_DIM
    nq = seq // bq
    k = k_ref[...]
    v = v_ref[...]
    kt = kt_ref[...]
    here = Spot()
    wires = Wires(send_sem, recv_sem)
    carry_over = halve_copies(here, wires, 3, (g1, g3, g2), (r1, r3, r2))

    half = HEAD_DIM // 2

    @pl.when(j == 0)
    def _():
        greet([here.peer(d) for d in 'xyz'])
        for cp in carry_over:
            cp.start()
        dqt[...] = jnp.zeros_like(dqt)

        def prep(i, c):
            rows = pl.ds(pl.multiple_of(i * bq, bq), bq)
            for h in range(heads):
                cols = head(h)
                prod = o_ref[rows, cols].astype(jnp.float32) * d_ref[rows, cols].astype(jnp.float32)
                rd[h:h + 1, rows] = jnp.sum(prod.T, axis=0, keepdims=True)
            return c
        lax.fori_loop(0, nq, prep, 0)

    dka[...] = jnp.zeros_like(dka)
    dva[...] = jnp.zeros_like(dva)

    def block(i, masked):
        rows = pl.ds(pl.multiple_of(i * bq, bq), bq)
        for h in range(heads):
            cols = head(h)
            q = q_ref[rows, cols]
            d = d_ref[rows, cols]
            s = lax.dot_general(k, q, NT, preferred_element_type=jnp.float32)
            dp = lax.dot_general(v, d, NT, preferred_element_type=jnp.float32)
            p = jnp.exp2(s * SCALE2 - lse_ref[h:h + 1, rows])
            if masked:
                kpos = j * bk + lax.broadcasted_iota(jnp.int32, (bk, bq), 0)
                qpos = i * bq + lax.broadcasted_iota(jnp.int32, (bk, bq), 1)
                p = jnp.where(qpos >= kpos, p, 0.0)
            ds = (p * (dp - rd[h:h + 1, rows]) * ATTN_SCALE).astype(jnp.bfloat16)
            dva[...] += lax.dot_general(p.astype(jnp.bfloat16), d, NN, preferred_element_type=jnp.float32)
            dka[...] += lax.dot_general(ds, q, NN, preferred_element_type=jnp.float32)
            dqt[cols, rows] += lax.dot_general(kt, ds, NN, preferred_element_type=jnp.float32)

    first = j * bk // bq
    ndiag = max(1, bk // bq)
    for t in range(ndiag):
        block(first + t, True)
    lax.fori_loop(first + ndiag, nq, lambda i, c: (block(i, False), c)[1], 0)
    own = pl.ds(pl.multiple_of(j * bk, bk), bk)
    cosw, sinw = wide_tables(cos_ref[:, own], sin_ref[:, own])
    dk = dka[...].astype(jnp.bfloat16).astype(jnp.float32)
    out_ref[own, width:width + HEAD_DIM] = (dk * cosw - pltpu.roll(dk, half, 1) * sinw).astype(jnp.bfloat16)
    out_ref[own, width + HEAD_DIM:] = dva[...].astype(jnp.bfloat16)

    @pl.when(j == nk - 1)
    def _():
        def fin(i, c):
            rows = pl.ds(pl.multiple_of(i * bq, bq), bq)
            cos, sin = cos_ref[:, rows], sin_ref[:, rows]
            for h in range(heads):
                cols = head(h)
                t = dqt[cols, rows].astype(jnp.bfloat16).astype(jnp.float32)
                lo, hi = t[:half], t[half:]
                out_ref[rows, cols] = jnp.concatenate([lo * cos + hi * sin, hi * cos - lo * sin], axis=0).T.astype(jnp.bfloat16)
            return c
        lax.fori_loop(0, nq, fin, 0)
        for cp in carry_over:
            cp.wait()


def flash_bwd(q, o, d, k, kt, v, lse, cos_t, sin_t, gs, cid, bq=512, bk=512):
    seq, width = q.shape
    heads = width // HEAD_DIM
    an = pl.BlockSpec(memory_space=pl.ANY)
    return pl.pallas_call(
        functools.partial(bwd_kernel, bq, bk),
        grid=(seq // bk,),
        in_specs=[pl.BlockSpec((seq, width), whole), pl.BlockSpec((seq, width), whole), pl.BlockSpec((seq, width), whole),
                  pl.BlockSpec((bk, HEAD_DIM), by_rows), pl.BlockSpec((HEAD_DIM, bk), by_cols),
                  pl.BlockSpec((bk, HEAD_DIM), by_rows),
                  pl.BlockSpec((heads, seq), whole), pl.BlockSpec(cos_t.shape, whole), pl.BlockSpec(cos_t.shape, whole)] + [an] * 3,
        out_specs=[pl.BlockSpec((seq, width + 2 * HEAD_DIM), whole)] + [an] * 3,
        out_shape=[jax.ShapeDtypeStruct((seq, width + 2 * HEAD_DIM), jnp.bfloat16)] + halve_shapes(gs, 3),
        scratch_shapes=[pltpu.VMEM((width, seq), jnp.float32), pltpu.VMEM((bk, HEAD_DIM), jnp.float32), pltpu.VMEM((bk, HEAD_DIM), jnp.float32),
                        pltpu.VMEM((heads, seq), jnp.float32), pltpu.SemaphoreType.DMA((3,)), pltpu.SemaphoreType.DMA((3,))],
        cost_estimate=pl.CostEstimate(flops=5 * seq * seq * width * 2 // 2, bytes_accessed=16 << 20, transcendentals=seq * seq),
        compiler_params=comm_params(cid, vmem_limit_bytes=58 << 20),
        name="flash_bwd",
    )(q, o, d, k, kt, v, lse, cos_t, sin_t, *gs)


class PlaneGather:
    N = 13

    def __init__(self, here, wires, src, out, local_sem):
        h = src.shape[0] // 2
        A, B = slice(h), slice(h, None)
        s = here.s
        sx, sy, sc = here.peer('x')[1], here.peer('y')[1], here.peer('c')[1]
        sd = here.s + 2 - 4 * here.x + 4 - 8 * here.y
        nx, ny, nc = here.peer('x'), here.peer('y'), here.peer('c')
        self.local = pltpu.make_async_copy(src, out.at[s], local_sem)
        mk = wires.copy
        self.x1 = {k: mk(src.at[r], out.at[s, r], nx) for k, r in (('A', A), ('B', B))}
        self.y1 = {k: mk(src.at[r], out.at[s, r], ny) for k, r in (('B', B), ('A', A))}
        self.c1 = mk(src, out.at[s], nc)
        self.fy = mk(out.at[sx, A], out.at[sx, A], ny)
        self.fx = mk(out.at[sy, B], out.at[sy, B], nx)
        self.cc = {}
        for name, idx in (('x', sx), ('y', sy), ('d', sd)):
            for k, r in (('A', A), ('B', B)):
                self.cc[name + k] = mk(out.at[idx, r], out.at[idx, r], nc)

    def start_first(self):
        self.x1['A'].start()
        self.y1['B'].start()
        self.c1.start()
        self.local.start()

    def start_second(self):
        self.x1['B'].start()
        self.y1['A'].start()

    def relay(self):
        self.x1['A'].wait_recv()
        self.fy.start()
        self.cc['xA'].start()
        self.y1['B'].wait_recv()
        self.fx.start()
        self.cc['yB'].start()
        self.x1['B'].wait_recv()
        self.cc['xB'].start()
        self.y1['A'].wait_recv()
        self.cc['yA'].start()

    def finish(self):
        self.fy.wait_recv()
        self.cc['dA'].start()
        self.fx.wait_recv()
        self.cc['dB'].start()
        self.c1.wait_recv()
        for k in self.cc:
            self.cc[k].wait_recv()
        for c in (*self.x1.values(), *self.y1.values(), self.c1, self.fy, self.fx, *self.cc.values()):
            c.wait_send()
        self.local.wait()


def dh_kernel(src, out, send_sem, recv_sem, local_sem):
    here = Spot()
    greet([here.peer(d) for d in 'xyc'])
    g = PlaneGather(here, Wires(send_sem, recv_sem), src, out, local_sem)
    g.start_first()
    g.start_second()
    g.relay()
    g.finish()


def gather_dh(src, cid):
    rows, cols = src.shape
    n = PlaneGather.N
    return pl.pallas_call(
        dh_kernel, in_specs=[pl.BlockSpec(memory_space=pltpu.VMEM)], out_specs=pl.BlockSpec(memory_space=pl.ANY),
        out_shape=jax.ShapeDtypeStruct((8, rows, cols), src.dtype),
        scratch_shapes=[pltpu.SemaphoreType.DMA((n,)), pltpu.SemaphoreType.DMA((n,)), pltpu.SemaphoreType.DMA],
        cost_estimate=busy(40), compiler_params=comm_params(cid), name="gather_dh",
    )(src)


def mlp_kernel(own_u, peer_u, own_d, peer_d, w1_ref, w3_ref, w2_ref, wg, y_ref, yp_ref, dx_ref, dxp_ref, g1_ref, g3_ref, g2_ref, og, u_ref, d_ref, ut, send_sem, recv_sem, local_sem):
    j = pl.program_id(0)
    last = pl.num_programs(0) - 1
    here = Spot()
    c = here.c
    wires = Wires(send_sem, recv_sem)
    loc = pltpu.make_async_copy(wg, og.at[here.region('') + (c,)], local_sem)
    jobs = [(og, (c, slice(None), slice(off, off + n)), order) for (off, n), order in zip(col_chunks(wg.shape[1], 3), ORDERS)]
    cube = CubeGather(here, wires, jobs)
    post = wires.copy(og.at[:, :, :, c], og.at[:, :, :, c], here.peer('c'))
    toks, mine = u_ref.shape[0], y_ref.shape[0]

    @pl.when(j == 0)
    def _():
        greet(cube_targets(here))
        loc.start()
        loc.wait()
        cube.start(0)
        for r in (y_ref, yp_ref, dx_ref, dxp_ref):
            r[...] = jnp.zeros_like(r)
        for pair, own, peer in ((u_ref, own_u, peer_u), (d_ref, own_d, peer_d)):
            pair[:mine] = own[...]
            pair[mine:] = peer[...]

        def flip(i, carry):
            part = pl.ds(pl.multiple_of(i * 128, 128), 128)
            ut[:, part] = u_ref[part, :].astype(jnp.float32).T.astype(jnp.bfloat16)
            return carry
        lax.fori_loop(0, toks // 128, flip, 0)

    @pl.when(j == 1)
    def _():
        cube.start(1)

    @pl.when(j == 3)
    def _():
        cube.start(2)

    @pl.when(j == last)
    def _():
        cube.arrive()
        post.start()

    f32 = jnp.float32
    u, d = u_ref[...], d_ref[...]
    w1, w3, w2 = w1_ref[...], w3_ref[...], w2_ref[...]
    gate = jnp.dot(u, w1, preferred_element_type=f32)
    up = jnp.dot(u, w3, preferred_element_type=f32)
    act = lax.dot_general(d, w2, NT, preferred_element_type=f32)
    sig = jax.nn.sigmoid(gate)
    silu = gate * sig
    z = (silu * up).astype(jnp.bfloat16)
    da = (act * up * sig * (1.0 + gate * (1.0 - sig))).astype(jnp.bfloat16)
    dc = (act * silu).astype(jnp.bfloat16)
    y = jnp.dot(z, w2, preferred_element_type=f32)
    dx = lax.dot_general(da, w1, NT, preferred_element_type=f32) + lax.dot_general(dc, w3, NT, preferred_element_type=f32)
    y_ref[...] += y[:mine]
    yp_ref[...] += y[mine:]
    dx_ref[...] += dx[:mine]
    dxp_ref[...] += dx[mine:]
    g1_ref[...] = jnp.dot(ut[...], da, preferred_element_type=f32)
    g3_ref[...] = jnp.dot(ut[...], dc, preferred_element_type=f32)
    g2_ref[...] = lax.dot_general(z, d, (((0,), (0,)), ((), ())), preferred_element_type=f32)

    @pl.when(j == last)
    def _():
        post.wait()
        cube.drain()


def mlp(us, ds, w1, w3, w2, wg, cid, bh=256):
    mine, dim = us[0].shape
    toks = mine + mine
    half = w1.shape[1]
    f32 = jnp.float32
    vm = pl.BlockSpec(memory_space=pltpu.VMEM)
    an = pl.BlockSpec(memory_space=pl.ANY)
    return pl.pallas_call(
        mlp_kernel, grid=(half // bh,),
        in_specs=[vm] * 4 + [pl.BlockSpec((dim, bh), by_cols), pl.BlockSpec((dim, bh), by_cols), pl.BlockSpec((bh, dim), by_rows), vm],
        out_specs=[pl.BlockSpec((mine, dim), whole)] * 4 + [pl.BlockSpec((dim, bh), by_cols), pl.BlockSpec((dim, bh), by_cols),
                   pl.BlockSpec((bh, dim), by_rows), an],
        out_shape=[jax.ShapeDtypeStruct((mine, dim), f32)] * 4 + [jax.ShapeDtypeStruct((dim, half), f32),
                   jax.ShapeDtypeStruct((dim, half), f32), jax.ShapeDtypeStruct((half, dim), f32),
                   jax.ShapeDtypeStruct((2, 2, 2, 2, *wg.shape), wg.dtype)],
        scratch_shapes=[pltpu.VMEM((toks, dim), jnp.bfloat16)] * 2 + [pltpu.VMEM((dim, toks), jnp.bfloat16), pltpu.SemaphoreType.DMA((19,)), pltpu.SemaphoreType.DMA((19,)), pltpu.SemaphoreType.DMA],
        cost_estimate=pl.CostEstimate(flops=18 * toks * dim * half, bytes_accessed=48 << 20, transcendentals=toks * half),
        compiler_params=comm_params(cid, vmem_limit_bytes=58 << 20), name="mlp",
    )(*us, *ds, w1, w3, w2, wg)


def entry_kernel(x_ref, w_ref, meta_ref, pos_ref, xa, wa, ma, pa, send_sem, recv_sem, local_sem):
    here = Spot()
    z, s = here.z, here.s
    peers = here.others()
    nz = here.peer('z')
    greet(peers + [nz])
    wires = Wires(send_sem, recv_sem)
    first = []
    for t in peers:
        for src, dst in ((w_ref.at[t[1]], wa.at[z, s]), (meta_ref, ma.at[z, s]), (pos_ref, pa.at[s])):
            first.append(wires.copy(src, dst, t))
    locals_ = [pltpu.make_async_copy(w_ref.at[s], wa.at[z, s], local_sem.at[1]),
               pltpu.make_async_copy(meta_ref, ma.at[z, s], local_sem.at[2]),
               pltpu.make_async_copy(pos_ref, pa.at[s], local_sem.at[3])]
    g = PlaneGather(here, wires, x_ref, xa, local_sem.at[0])
    cross = [wires.copy(wa.at[z], wa.at[z], nz), wires.copy(ma.at[z], ma.at[z], nz)]
    for c in first:
        c.start()
    for c in locals_:
        c.start()
    g.start_first()
    g.start_second()
    for c in first:
        c.wait_recv()
    for c in locals_:
        c.wait()
    for c in cross:
        c.start()
    g.relay()
    g.finish()
    for c in cross:
        c.wait()
    for c in first:
        c.wait_send()


def entry(x, w, meta, pos, cid):
    n = PlaneGather.N + 21 + 2
    vm = pl.BlockSpec(memory_space=pltpu.VMEM)
    an = pl.BlockSpec(memory_space=pl.ANY)
    return pl.pallas_call(
        entry_kernel,
        in_specs=[vm] * 4, out_specs=[an] * 4,
        out_shape=[jax.ShapeDtypeStruct((8, *x.shape), x.dtype), jax.ShapeDtypeStruct((2, 8, *w.shape[1:]), w.dtype),
                   jax.ShapeDtypeStruct((2, 8, *meta.shape), meta.dtype), jax.ShapeDtypeStruct((8, *pos.shape), pos.dtype)],
        scratch_shapes=[pltpu.SemaphoreType.DMA((n,)), pltpu.SemaphoreType.DMA((n,)), pltpu.SemaphoreType.DMA((4,))],
        cost_estimate=busy(45), compiler_params=comm_params(cid),
        name="entry",
    )(x, w, meta, pos)


def regroup_kernel(n, *refs):
    src, gs, out, rs = refs[0], refs[1:1 + n], refs[1 + n], refs[2 + n:2 + 2 * n]
    send_sem, recv_sem, local_sem, stage = refs[2 + 2 * n:]
    here = Spot()
    s = here.s
    rows, width = out.shape[0], src.shape[1]
    peers = here.others()
    greet(peers + ([here.peer('z')] if n else []))
    wires = Wires(send_sem, recv_sem)
    piece = lambda i: pl.ds(pl.multiple_of(i * rows, rows), rows)
    mine = pl.ds(pl.multiple_of(s * width, width), width)
    cs = [wires.copy(src.at[piece(t[1])], out.at[:, mine], t) for t in peers]
    cs += [wires.copy(g, r, here.peer(order[1])) for g, r, order in zip(gs[:3], rs, ORDERS)]
    cs += [wires.copy(g.at[1 - here.z], r, here.peer('z')) for g, r in zip(gs[3:], rs[3:])]
    for c in cs:
        c.start()
    a = pltpu.make_async_copy(src.at[piece(s)], stage, local_sem.at[0])
    a.start()
    a.wait()
    b = pltpu.make_async_copy(stage, out.at[:, mine], local_sem.at[1])
    b.start()
    b.wait()
    for c in cs:
        c.wait()


def regroup(src, gs, cid, name):
    seq, width = src.shape
    rows, n = seq // 8, len(gs)
    an = pl.BlockSpec(memory_space=pl.ANY)
    back = [jax.ShapeDtypeStruct(g.shape if i < 3 else g.shape[1:], g.dtype) for i, g in enumerate(gs)]
    out = pl.pallas_call(
        functools.partial(regroup_kernel, n), in_specs=[an] * (1 + n), out_specs=[an] * (1 + n),
        out_shape=[jax.ShapeDtypeStruct((rows, 8 * width), src.dtype)] + back,
        scratch_shapes=[pltpu.SemaphoreType.DMA((7 + n,)), pltpu.SemaphoreType.DMA((7 + n,)), pltpu.SemaphoreType.DMA((2,)), pltpu.VMEM((rows, width), src.dtype)],
        cost_estimate=busy(70 if n else 25), compiler_params=comm_params(cid), name=name,
    )(src, *gs)
    return out[0], out[1:]


def back_kernel(t_ref, w_ref, x_ref, gain_ref, res_ref, a, g1, g3, g2, dx_ref, gg_ref, oa, r1, r3, r2, acc, send_sem, recv_sem, local_sem):
    j = pl.program_id(0)
    bn = w_ref.shape[0]
    here = Spot()
    peers = here.others()
    wires = Wires(send_sem, recv_sem)
    s = here.s
    cs = [wires.copy(g, r, here.peer(order[0])) for g, r, order in zip((g1, g3, g2), (r1, r3, r2), ORDERS)]
    cs += [wires.copy(a.at[t[1]], oa.at[s], t) for t in peers]
    loc = pltpu.make_async_copy(a.at[s], oa.at[s], local_sem)

    @pl.when(j == 0)
    def _():
        greet(peers + [here.peer('z')])
        for c in cs:
            c.start()
        loc.start()

    acc[:, pl.ds(pl.multiple_of(j * bn, bn), bn)] = lax.dot_general(t_ref[...], w_ref[...], NT, preferred_element_type=jnp.float32)

    @pl.when(j == pl.num_programs(0) - 1)
    def _():
        gg_ref[...] = jnp.zeros_like(gg_ref)
        gain = gain_ref[0:1, :].astype(jnp.float32)

        def rows_of(i, carry):
            part = pl.ds(pl.multiple_of(i * HEAD_DIM, HEAD_DIM), HEAD_DIM)
            x = x_ref[part, :].astype(jnp.float32)
            inv = lax.rsqrt(jnp.mean(x * x, axis=-1, keepdims=True) + NORM_EPS)
            normed = x * inv
            d_out = acc[part, :]
            d_normed = d_out * gain
            gg_ref[...] += jnp.sum(d_out * normed, axis=0, keepdims=True)
            grad_in = inv * (d_normed - normed * jnp.mean(d_normed * normed, axis=-1, keepdims=True))
            dx_ref[part, :] = (res_ref[part, :] + grad_in).astype(jnp.bfloat16)
            return carry
        lax.fori_loop(0, x_ref.shape[0] // HEAD_DIM, rows_of, 0)
        for c in cs:
            c.wait()
        loc.wait()


def back_project(t, w, x, gain, res, a, gs, cid, bn=256):
    toks, inner = t.shape
    dim = w.shape[0]
    vm = pl.BlockSpec(memory_space=pltpu.VMEM)
    an = pl.BlockSpec(memory_space=pl.ANY)
    out = pl.pallas_call(
        back_kernel, grid=(dim // bn,),
        in_specs=[vm, pl.BlockSpec((bn, inner), by_rows)] + [vm] * 4 + [an] * 3,
        out_specs=[pl.BlockSpec((toks, dim), whole), pl.BlockSpec((1, dim), whole)] + [an] * 4,
        out_shape=[jax.ShapeDtypeStruct((toks, dim), jnp.bfloat16), jax.ShapeDtypeStruct((1, dim), jnp.float32), jax.ShapeDtypeStruct(a.shape, a.dtype)]
        + [jax.ShapeDtypeStruct(g.shape, g.dtype) for g in gs],
        scratch_shapes=[pltpu.VMEM((toks, dim), jnp.float32), pltpu.SemaphoreType.DMA((10,)), pltpu.SemaphoreType.DMA((10,)), pltpu.SemaphoreType.DMA],
        cost_estimate=busy(35), compiler_params=comm_params(cid, vmem_limit_bytes=62 << 20), name="back_project",
    )(t, w, x, gain, res, a, *gs)
    return out[0], out[1], out[2], out[3:]


def last_kernel(b, p1, p3, ob, q1, q3, send_sem, recv_sem, local_sem):
    here = Spot()
    peers = here.others()
    greet(peers)
    wires = Wires(send_sem, recv_sem)
    s, nc = here.s, here.peer('c')
    cs = [wires.copy(p.at[1 - here.c], q, nc) for p, q in ((p1, q1), (p3, q3))]
    cs += [wires.copy(b.at[t[1]], ob.at[s], t) for t in peers]
    loc = pltpu.make_async_copy(b.at[s], ob.at[s], local_sem)
    for c in cs + [loc]:
        c.start()
    for c in cs + [loc]:
        c.wait()


def last_exchange(b, p1, p3, cid):
    vm = pl.BlockSpec(memory_space=pltpu.VMEM)
    return pl.pallas_call(
        last_kernel, in_specs=[vm] * 3, out_specs=[vm] * 3,
        out_shape=[jax.ShapeDtypeStruct(b.shape, b.dtype)] + [jax.ShapeDtypeStruct(p.shape[1:], p.dtype) for p in (p1, p3)],
        scratch_shapes=[pltpu.SemaphoreType.DMA((9,)), pltpu.SemaphoreType.DMA((9,)), pltpu.SemaphoreType.DMA],
        cost_estimate=busy(5), compiler_params=comm_params(cid), name="last_exchange",
    )(b, p1, p3)


def dot_tokens(left_op, right_op):
    return lax.dot_general(left_op, right_op, (((0,), (0,)), ((), ())), preferred_element_type=jnp.float32)


def dot_back(left_op, weight):
    return lax.dot_general(left_op, weight, (((1,), (1,)), ((), ())), preferred_element_type=jnp.float32)


def dot_on(left_op, weight):
    return jnp.dot(left_op, weight, preferred_element_type=jnp.float32)


def swap_core(t):
    return lax.ppermute(t, 'sp', [(i, i ^ 1) for i in range(8)])


def swap_z(t):
    return lax.ppermute(t, 'dp', [(0, 1), (1, 0)])


def split_cols(w):
    rows, cols = w.shape
    return w.reshape(rows, 8, 2, cols // 16).transpose(2, 0, 1, 3).reshape(2, rows, cols // 2)


def join_cols(mine, other, c):
    rows, half = mine.shape
    m, o = mine.reshape(rows, 8, 1, half // 8), other.reshape(rows, 8, 1, half // 8)
    first = jnp.where(c == 0, m, o)
    second = jnp.where(c == 0, o, m)
    return jnp.concatenate([first, second], axis=2).reshape(rows, 2 * half)


def layer_step(hidden, positions, grad_out, gain_attn, gain_mlp, w_query, w_key, w_value, w_out, w_gate, w_up, w_down):
    tokens = hidden[0]
    d_layer = grad_out[0]
    tok, dim = tokens.shape
    here = Spot()
    z, s, c = here.z, here.s, here.c
    rows = w_query.shape[0]
    grp_q = w_query.shape[1] // 8
    grp_k = w_key.shape[1] // 8
    grp = grp_q + 2 * grp_k
    seq = 8 * tok

    w_grp = jnp.concatenate([w_query.reshape(rows, 8, grp_q), w_key.reshape(rows, 8, grp_k), w_value.reshape(rows, 8, grp_k)], axis=2)
    w_flat = w_grp.reshape(rows, 8 * grp)
    pad = HEAD_DIM - gain_attn.shape[0]
    meta = jnp.pad(jnp.stack([gain_attn, gain_mlp]), ((0, 14), (0, pad)))
    x_all, w_own, meta_all, pos_all = entry(tokens, w_grp.transpose(1, 0, 2), meta, positions[0].reshape(-1, 128), 1)
    x_all = x_all.reshape(seq, dim)
    w_own = w_own.reshape(dim, grp)
    gain1 = meta_all[:, :, 0, :rows].reshape(dim)
    gain2 = meta_all[:, :, 1, :rows].reshape(dim)
    cos_t, sin_t = rope_tables(pos_all.reshape(seq))

    gain1_rows = jnp.broadcast_to(gain1[None], (16, dim))
    u_all, q_own, k_own, v_own, k_t, v_t = project(x_all, gain1_rows, w_own, cos_t, sin_t)
    o_own, o_t, lse, w1, w3, w2, wo = flash_fwd(q_own, k_own, v_t, (split_cols(w_gate), split_cols(w_up), w_down, w_out), 2)
    ffn_half = w1.shape[-1]
    w1, w3 = w1.reshape(dim, ffn_half), w3.reshape(dim, ffn_half)
    w2 = w2.reshape(ffn_half, dim)
    wo = wo.reshape(-1, dim)
    attn_out, _ = regroup(o_own, (), 3, 'regroup_o')
    residual = (tokens.astype(jnp.float32) + dot_on(attn_out, wo)).astype(jnp.bfloat16)
    u_mlp, normed2, inv_rms2 = rms_norm(residual, gain2)
    y_part, y_peer, d_part, d_peer, g1, g3, g2, wg = mlp((u_mlp, swap_core(u_mlp)), (d_layer, swap_core(d_layer)), w1, w3, w2, w_flat, 7)
    layer_out = (residual.astype(jnp.float32) + (y_part + swap_core(y_peer))).astype(jnp.bfloat16)

    d_umlp = d_part + swap_core(d_peer)
    d_res_norm, d_gain2 = rms_norm_grad(d_umlp, normed2, inv_rms2, gain2)
    d_resid = d_layer.astype(jnp.float32) + d_res_norm
    d_resid_bf = d_resid.astype(jnp.bfloat16)
    g1 = g1.reshape(2, 2, 2, dim // 8, ffn_half)
    g3 = g3.reshape(2, 2, 2, dim // 8, ffn_half)
    g2 = g2.reshape(2, 2, 2, ffn_half // 8, dim)

    dh_all = gather_dh(d_resid_bf, 4).reshape(seq, dim)
    wg = wg.reshape(dim, 8 * grp)
    wo_own = lax.dynamic_slice_in_dim(wo, s * grp_q, grp_q, 0)
    d_own = dot_back(dh_all, wo_own).astype(jnp.bfloat16)
    go = dot_on(o_t, dh_all).reshape(2, grp_q // 2, dim)
    dqkv_pre, *got = flash_bwd(q_own, o_own, d_own, k_own, k_t, v_own, lse, cos_t, sin_t, (g1, g3, g2), 6)
    gq = dot_tokens(u_all, dqkv_pre).reshape(2, dim // 2, grp)
    terms = after(here, [[g1], [g3], [g2]], got, 3)
    dqkv_tok, (*got, gq_got, go_got) = regroup(dqkv_pre, (*to_send(here, terms, 2), gq, go), 5, 'regroup_dqkv')
    go_mine = pick(go, z) + go_got
    stay = dim // HEAD_DIM - 1
    moved = lax.ppermute(go_mine, ALL_AXES, [(zz * 8 + ss, 2 * ss + zz) for zz in range(2) for ss in range(8) if ss != zz * stay])
    grad_w_out = jnp.where(s == z * stay, go_mine, moved)
    terms = after(here, terms, got, 2)
    gq_mine = pick(gq, z) + gq_got
    grad_hidden, d_gain1, got_q, got = back_project(dqkv_tok, wg, tokens, gain1_rows, d_resid, gq_mine.reshape(8, rows, grp), to_send(here, terms, 1), 8)
    m1, m3, grad_w_down = [total(ts) for ts in after(here, terms, got, 1)]

    gains = jnp.concatenate([d_gain1.reshape(2, 8, rows), d_gain2.reshape(2, 8, rows)], axis=2)
    gains_mine = pick(gains, z) + swap_z(pick(gains, 1 - z))
    gains_mine = jnp.broadcast_to(gains_mine[:, None, :], (8, 8, 2 * rows))
    pair1, pair3 = m1.reshape(2, rows, ffn_half), m3.reshape(2, rows, ffn_half)
    got_g, other1, other3 = last_exchange(gains_mine, pair1, pair3, 10)
    got_q = got_q.transpose(1, 0, 2)
    grad_w_query = got_q[:, :, :grp_q].reshape(rows, 8 * grp_q)
    grad_w_key = got_q[:, :, grp_q:grp_q + grp_k].reshape(rows, 8 * grp_k)
    grad_w_value = got_q[:, :, grp_q + grp_k:].reshape(rows, 8 * grp_k)
    grad_gains = jnp.sum(got_g[:, 0, :], axis=0)
    grad_gain_attn, grad_gain_mlp = grad_gains[:rows], grad_gains[rows:]

    grad_w_gate = join_cols(pick(pair1, c), other1, c)
    grad_w_up = join_cols(pick(pair3, c), other3, c)
    return (layer_out[None], grad_hidden[None], grad_gain_attn, grad_gain_mlp, grad_w_query, grad_w_key, grad_w_value, grad_w_out, grad_w_gate, grad_w_up, grad_w_down)


def solution(mesh):
    act_spec = P('dp', 'sp', None)
    pos_spec = P('dp', 'sp')
    vec_spec = P(ALL_AXES)
    mat_spec = P(ALL_AXES, None)
    in_specs = (act_spec, pos_spec, act_spec, vec_spec, vec_spec) + (mat_spec,) * 7
    out_specs = (act_spec, act_spec, vec_spec, vec_spec) + (mat_spec,) * 7
    return jax.shard_map(layer_step, mesh=mesh, in_specs=in_specs, out_specs=out_specs, check_vma=False)
```
